8 devices in a mesh: rep: 1 (over z), model: 2 (over y), vocab: 4 (over x, core).
Axes of the slice: x: 2, y: 2, z: 1, core: 2. Of those that a mesh axis runs over, the one named last changes fastest.
Arguments:
- hidden: bfloat16 [256, 5120], P(('rep', 'model', 'vocab'))
- head_rows: bfloat16 [131072, 5120], P(('model', 'vocab'))
- allowed_ids: int32 [256, 64], P(('rep', 'model', 'vocab'))
- valid_mask: int32 [256, 64], P(('rep', 'model', 'vocab'))
- target_pos: int32 [256], P(('rep', 'model', 'vocab'))
Outputs:
- output 1: float32 [256, 64], P(('rep', 'model', 'vocab'))
- output 2: float32 [256], P(('rep', 'model', 'vocab'))
All inputs are finite; a program needn't handle non-finite values.
Results may differ from the reference program's by a relative error of at most 0.001.
Values are sent between devices in bfloat16 or wider.
A program may use at most 1 GiB of HBM per device.

```python
import jax
import jax.numpy as jnp
from jax import lax

VOCAB_SIZE = 131072
MODEL_WIDTH = 5120
NUM_ROWS = 256
LIST_LEN = 64
NUM_SHARDS = 8
OWNER_RUNS = 4
TEMPERATURE = 0.5


def draw_lists(idx_key):
    shard_len = VOCAB_SIZE // NUM_SHARDS
    run_len = LIST_LEN // OWNER_RUNS
    key_rot, key_step, key_start, key_count, key_target = jax.random.split(idx_key, 5)
    rotation = jax.random.randint(key_rot, (NUM_ROWS, 1), 0, NUM_SHARDS - 1)
    run_index = jnp.arange(OWNER_RUNS)[None, :]
    owners = jnp.where(run_index == 0, 0, 1 + (rotation + run_index - 1) % (NUM_SHARDS - 1))
    stride = jax.random.randint(key_step, (NUM_ROWS, OWNER_RUNS), 1, shard_len // run_len + 1)
    run_start = jax.random.randint(key_start, (NUM_ROWS, OWNER_RUNS), 0, shard_len - stride * (run_len - 1))
    offsets = run_start[:, :, None] + stride[:, :, None] * jnp.arange(run_len)[None, None, :]
    allowed_ids = (owners[:, :, None] * shard_len + offsets).reshape(NUM_ROWS, LIST_LEN).astype(jnp.int32)
    counts = LIST_LEN - jax.random.randint(key_count, (NUM_ROWS,), 0, LIST_LEN // 2)
    counts = jnp.where(jnp.arange(NUM_ROWS) == 0, LIST_LEN, counts)
    valid_mask = (jnp.arange(LIST_LEN)[None, :] < counts[:, None]).astype(jnp.int32)
    target_pos = jax.random.randint(key_target, (NUM_ROWS,), 0, counts).astype(jnp.int32)
    return allowed_ids, valid_mask, target_pos


def setup_inputs(seed: int = 0, part: int = 0) -> dict:
    base_key = jax.random.key(seed)
    part_key = jax.random.fold_in(base_key, part)
    key_hidden, key_lists = jax.random.split(part_key, 2)
    hidden = jax.random.normal(key_hidden, (NUM_ROWS, MODEL_WIDTH), jnp.float32).astype(jnp.bfloat16)
    head_rows = (jax.random.normal(jax.random.key(seed + 1), (VOCAB_SIZE, MODEL_WIDTH), jnp.float32) * MODEL_WIDTH ** -0.5).astype(jnp.bfloat16)
    allowed_ids, valid_mask, target_pos = draw_lists(key_lists)
    return {'hidden': hidden, 'head_rows': head_rows, 'allowed_ids': allowed_ids, 'valid_mask': valid_mask, 'target_pos': target_pos}


def reference(hidden, head_rows, allowed_ids, valid_mask, target_pos):
    def row_scores(row_args):
        h_row, row_ids = row_args
        return jnp.dot(head_rows[row_ids], h_row, preferred_element_type=jnp.float32)

    scores = lax.map(row_scores, (hidden, allowed_ids)) / TEMPERATURE
    is_valid = valid_mask > 0
    scores = jnp.where(is_valid, scores, -jnp.inf)
    top_score = jnp.max(scores, axis=1, keepdims=True)
    log_norm = top_score[:, 0] + jnp.log(jnp.sum(jnp.exp(scores - top_score), axis=1))
    probs = jnp.where(is_valid, jnp.exp(scores - log_norm[:, None]), 0.0)
    picked_score = jnp.take_along_axis(scores, target_pos[:, None], axis=1)[:, 0]
    return probs, picked_score - log_norm
```

```python
import functools

import jax
import jax.numpy as jnp
from jax import lax
from jax.experimental import pallas as pl
from jax.experimental.pallas import tpu as pltpu
from jax.sharding import PartitionSpec as P

MESH = pl.DeviceIdType.MESH
TEMP = 0.5
CAP = 16
GROUP = 8
DEPTH = 6


def entry_barrier(n_model, n_vocab, m, v):
    barrier = pltpu.get_barrier_semaphore()
    for dm in range(n_model):
        for dv in range(n_vocab):
            if dm or dv:
                pl.semaphore_signal(
                    barrier, inc=1,
                    device_id={"model": lax.rem(m + dm, n_model), "vocab": lax.rem(v + dv, n_vocab)},
                    device_id_type=MESH,
                )
    return barrier


def route_kernel(shard_len, n_model, n_vocab, h_ref, ids_ref, valid_ref, tgt_ref, tbl_ref, hall_ref, meta_ref,
                 t_ref, send_ref, tin_ref, hbuf, tsend, trecv, hsend, hrecv, lsem):
    n = n_model * n_vocab
    rows, length = ids_ref.shape
    m, v = lax.axis_index("model"), lax.axis_index("vocab")
    me = m * n_vocab + v
    barrier = entry_barrier(n_model, n_vocab, m, v)

    ids = ids_ref[...]
    ok = valid_ref[...] > 0
    owner = jnp.where(ok, lax.div(ids, shard_len), n)
    off = lax.rem(ids, shard_len)
    tri = (lax.broadcasted_iota(jnp.int32, (length, length), 0)
           < lax.broadcasted_iota(jnp.int32, (length, length), 1)).astype(jnp.bfloat16)
    rank = jnp.zeros((rows, length), jnp.float32)
    for s in range(n):
        hit = owner == s
        count = jnp.dot(jnp.where(hit, 1.0, 0.0).astype(jnp.bfloat16), tri, preferred_element_type=jnp.float32)
        rank = rank + jnp.where(hit, count, 0.0)
    rank = rank.astype(jnp.int32)
    slot = jnp.where(ok, owner * CAP + rank, n * CAP)
    pair = off - lax.rem(off, 2)

    lane = lax.broadcasted_iota(jnp.int32, (rows, n * CAP), 1)
    row = lax.broadcasted_iota(jnp.int32, (rows, n * CAP), 0)
    spread = lax.rem(((me * rows + row) * CAP + lax.rem(lane, CAP)) * 4, shard_len)
    table = spread
    for j in range(length):
        table = jnp.where(lane == slot[:, j:j + 1], pair[:, j:j + 1], table)
    t_ref[...] = table

    code = jnp.where(ok, owner * (2 * CAP) + rank * 2 + lax.rem(off, 2), -1)
    diag = (lax.broadcasted_iota(jnp.int32, (rows, rows), 0) == lax.broadcasted_iota(jnp.int32, (rows, rows), 1))
    tcol = jnp.sum(jnp.where(diag, tgt_ref[...].reshape(1, rows), 0).astype(jnp.float32), axis=1, keepdims=True)
    meta_ref[:, :length] = code
    meta_ref[:, length:] = jnp.broadcast_to(tcol.astype(jnp.int32), (rows, length))

    groups = 128 // CAP
    per = rows // groups
    lane4 = lax.broadcasted_iota(jnp.int32, (per, 128), 1)
    parts = [jnp.zeros((per, 128), jnp.int32) for _ in range(n)]
    for q in range(groups):
        tq = t_ref[pl.ds(q, per, stride=groups), :]
        inside = lax.div(lane4, CAP) == q
        for s in range(n):
            moved = tq if q == s else pltpu.roll(tq, ((q - s) * CAP) % 128, axis=1)
            parts[s] = jnp.where(inside, moved, parts[s])
    for s in range(n):
        send_ref[s] = parts[s]

    pl.semaphore_wait(barrier, n - 1)

    def remote(src, dst, k, to):
        return pltpu.make_async_remote_copy(src_ref=src, dst_ref=dst, send_sem=hsend.at[k], recv_sem=hrecv.at[k],
                                            device_id=to, device_id_type=MESH)

    def at(mm, vv):
        return {"model": mm, "vocab": vv}

    tcopies = []
    for k in range(1, n):
        dm, dv = k // n_vocab, k % n_vocab
        om, ov = lax.rem(m + dm, n_model), lax.rem(v + dv, n_vocab)
        c = pltpu.make_async_remote_copy(
            src_ref=send_ref.at[om * n_vocab + ov], dst_ref=tin_ref.at[me], send_sem=tsend.at[k], recv_sem=trecv.at[k],
            device_id=at(om, ov), device_id_type=MESH)
        c.start()
        tcopies.append(c)

    core = lax.rem(v, 2)
    xpos = lax.div(v, 2)
    vp = xpos * 2 + (1 - core)
    vx = (1 - xpos) * 2 + core
    my = 1 - m
    partner, xpeer, ypeer = at(m, vp), at(m, vx), at(my, v)
    ix, iy, idg = m * n_vocab + vx, my * n_vocab + v, my * n_vocab + vx
    half = rows // 2
    lo, hi = pl.ds(0, half), pl.ds(half, half)

    own_x = [remote(h_ref.at[lo], hbuf.at[me, lo], 0, xpeer), remote(h_ref.at[hi], hbuf.at[me, hi], 1, xpeer)]
    own_y = [remote(h_ref.at[lo], hbuf.at[me, lo], 2, ypeer), remote(h_ref.at[hi], hbuf.at[me, hi], 3, ypeer)]
    own_p = remote(h_ref, hbuf.at[me], 4, partner)
    x_to_y = remote(hbuf.at[ix, lo], hbuf.at[ix, lo], 5, ypeer)
    y_to_x = remote(hbuf.at[iy, hi], hbuf.at[iy, hi], 6, xpeer)
    x_p = [remote(hbuf.at[ix, lo], hbuf.at[ix, lo], 7, partner), remote(hbuf.at[ix, hi], hbuf.at[ix, hi], 8, partner)]
    y_p = [remote(hbuf.at[iy, lo], hbuf.at[iy, lo], 9, partner), remote(hbuf.at[iy, hi], hbuf.at[iy, hi], 10, partner)]
    d_p = [remote(hbuf.at[idg, lo], hbuf.at[idg, lo], 11, partner), remote(hbuf.at[idg, hi], hbuf.at[idg, hi], 12, partner)]

    own_x[0].start()
    own_y[1].start()
    own_x[1].start()
    own_y[0].start()
    own_p.start()
    keep = pltpu.make_async_copy(h_ref, hall_ref.at[me], lsem.at[0])
    keep.start()
    tbl_ref[me] = send_ref[me]

    own_x[0].wait_recv()
    x_to_y.start()
    x_p[0].start()
    own_y[1].wait_recv()
    y_to_x.start()
    y_p[1].start()
    own_p.wait_recv()
    out = [pltpu.make_async_copy(hbuf.at[m * n_vocab + vp], hall_ref.at[m * n_vocab + vp], lsem.at[1])]
    out[0].start()
    own_x[1].wait_recv()
    x_p[1].start()
    own_y[0].wait_recv()
    y_p[0].start()
    for k in range(1, n):
        tcopies[k - 1].wait_recv()
    for s in range(n):
        @pl.when(s != me)
        def _():
            tbl_ref[s] = tin_ref[s]

    def keep_block(slot, sem):
        c = pltpu.make_async_copy(hbuf.at[slot], hall_ref.at[slot], lsem.at[sem])
        c.start()
        out.append(c)

    keep_block(ix, 2)
    keep_block(iy, 3)
    x_to_y.wait_recv()
    d_p[0].start()
    y_to_x.wait_recv()
    d_p[1].start()
    keep_block(idg, 4)
    for c in x_p:
        c.wait_recv()
    keep_block(m * n_vocab + (1 - xpos) * 2 + (1 - core), 5)
    for c in y_p:
        c.wait_recv()
    keep_block(my * n_vocab + vp, 6)
    for c in d_p:
        c.wait_recv()
    keep_block(my * n_vocab + (1 - xpos) * 2 + (1 - core), 7)
    for c in tcopies + own_x + own_y + [own_p, x_to_y, y_to_x] + x_p + y_p + d_p:
        c.wait_send()
    keep.wait()
    for c in out:
        c.wait()


def score_kernel(chunks, tbl_ref, h_hbm, w_hbm, out_ref, buf, h_ref, sems, hsem):
    slots = 128

    hcopy = pltpu.make_async_copy(h_hbm, h_ref, hsem)
    hcopy.start()

    def issue(c, b):
        def body(g, _):
            for u in range(16):
                k = g * 16 + u
                at = pl.multiple_of(tbl_ref[c, k], 2)
                pltpu.make_async_copy(
                    w_hbm.at[pl.ds(at, 2), :], buf.at[b, pl.ds(pl.multiple_of(2 * k, 2), 2), :], sems.at[b]
                ).start(priority=u % 2)
            return 0
        lax.fori_loop(0, slots // 16, body, 0)

    for c in range(DEPTH - 1):
        issue(c, c)
    hcopy.wait()

    lane = lax.broadcasted_iota(jnp.int32, (GROUP, 2 * slots), 1)
    row = lax.broadcasted_iota(jnp.int32, (GROUP, 2 * slots), 0)
    mine = lax.div(lane, 2 * CAP) == row

    def step(c, _):
        b = lax.rem(c, DEPTH)

        @pl.when(c + DEPTH - 1 < chunks)
        def _():
            issue(c + DEPTH - 1, lax.rem(c + DEPTH - 1, DEPTH))

        pltpu.make_async_copy(w_hbm.at[pl.ds(0, 2 * slots), :], buf.at[b], sems.at[b]).wait()
        hs = h_ref[c]
        part = lax.dot_general(hs, buf[b], (((1,), (1,)), ((), ())), preferred_element_type=jnp.float32)
        out_ref[pl.ds(c, 1), :] = jnp.sum(jnp.where(mine, part, 0.0), axis=0, keepdims=True)
        return 0

    lax.fori_loop(0, chunks, step, 0)


def finish_kernel(n_model, n_vocab, sc_ref, meta_ref, p_ref, lp_ref, inb, wide0, wide1, ssend, srecv):
    n = n_model * n_vocab
    wide = (wide0, wide1)
    rows, length = p_ref.shape
    m, v = lax.axis_index("model"), lax.axis_index("vocab")
    me = m * n_vocab + v
    barrier = entry_barrier(n_model, n_vocab, m, v)
    pl.semaphore_wait(barrier, n - 1)
    copies = []
    for k in range(1, n):
        om, ov = lax.rem(m + k // n_vocab, n_model), lax.rem(v + k % n_vocab, n_vocab)
        c = pltpu.make_async_remote_copy(
            src_ref=sc_ref.at[om * n_vocab + ov], dst_ref=inb.at[me], send_sem=ssend.at[k], recv_sem=srecv.at[k],
            device_id={"model": om, "vocab": ov}, device_id_type=MESH)
        c.start()
        copies.append(c)
    inb[me] = sc_ref[me]
    for c in copies:
        c.wait_recv()
    width = 2 * CAP
    groups = rows // GROUP
    lane = lax.broadcasted_iota(jnp.int32, (groups, 128), 1)
    per = 128 // width
    for q in range(GROUP):
        for hb in range(2):
            acc = jnp.zeros((groups, 128), jnp.float32)
            for sl in range(per):
                s = hb * per + sl
                src = inb[s][:, (q // per) * 128:(q // per + 1) * 128]
                shift = ((sl - q % per) * width) % 128
                moved = pltpu.roll(src, shift, axis=1) if shift else src
                acc = jnp.where(lax.div(lane, width) == sl, moved, acc)
            wide[hb][pl.ds(q, groups, stride=GROUP), :] = acc
    meta = meta_ref[...]
    code = meta[:, :length]
    ok = code >= 0
    full = jnp.concatenate([jnp.where(ok, code, 0), jnp.zeros((rows, 128 - length), jnp.int32)], axis=1)
    low = jnp.take_along_axis(wide0[...], lax.rem(full, 128), axis=1)
    high = jnp.take_along_axis(wide1[...], lax.rem(full, 128), axis=1)
    scores = jnp.where(full < 128, low, high)[:, :length] / TEMP
    scores = jnp.where(ok, scores, -jnp.inf)
    top = jnp.max(scores, axis=1, keepdims=True)
    log_norm = top + jnp.log(jnp.sum(jnp.exp(scores - top), axis=1, keepdims=True))
    p_ref[...] = jnp.where(ok, jnp.exp(scores - log_norm), 0.0)
    at = lax.broadcasted_iota(jnp.int32, (rows, length), 1)
    picked = jnp.sum(jnp.where(at == meta[:, length:], scores, 0.0), axis=1, keepdims=True)
    diag = (lax.broadcasted_iota(jnp.int32, (rows, rows), 0) == lax.broadcasted_iota(jnp.int32, (rows, rows), 1))
    lp_ref[...] = jnp.sum(jnp.where(diag, picked - log_norm, 0.0), axis=0)
    for c in copies:
        c.wait_send()


def solution(mesh):
    axes = ("model", "vocab")
    n_model, n_vocab = mesh.shape["model"], mesh.shape["vocab"]
    n = n_model * n_vocab
    row_spec = P(("rep",) + axes, None)
    vec_spec = P(("rep",) + axes)
    vmem = pl.BlockSpec(memory_space=pltpu.VMEM)
    hbm = pl.BlockSpec(memory_space=pl.ANY)
    smem = pl.BlockSpec(memory_space=pltpu.SMEM)

    def local_step(hidden, head_rows, allowed_ids, valid_mask, target_pos):
        rows, length = allowed_ids.shape
        shard_len, width = head_rows.shape
        per = rows * CAP // 128
        tbl, hall, meta = pl.pallas_call(
            functools.partial(route_kernel, shard_len, n_model, n_vocab),
            out_shape=(jax.ShapeDtypeStruct((n, per, 128), jnp.int32),
                       jax.ShapeDtypeStruct((n, rows, width), jnp.bfloat16),
                       jax.ShapeDtypeStruct((rows, 2 * length), jnp.int32)),
            in_specs=[vmem, vmem, vmem, vmem],
            out_specs=(vmem, hbm, vmem),
            scratch_shapes=[
                pltpu.VMEM((rows, n * CAP), jnp.int32),
                pltpu.VMEM((n, per, 128), jnp.int32),
                pltpu.VMEM((n, per, 128), jnp.int32),
                pltpu.VMEM((n, rows, width), jnp.bfloat16),
                pltpu.SemaphoreType.DMA((n,)),
                pltpu.SemaphoreType.DMA((n,)),
                pltpu.SemaphoreType.DMA((13,)),
                pltpu.SemaphoreType.DMA((13,)),
                pltpu.SemaphoreType.DMA((n,)),
            ],
            compiler_params=pltpu.CompilerParams(collective_id=0, has_side_effects=True),
            name="route",
        )(hidden, allowed_ids, valid_mask, target_pos)
        chunks = n * rows // GROUP
        scores = pl.pallas_call(
            functools.partial(score_kernel, chunks),
            out_shape=jax.ShapeDtypeStruct((chunks, 256), jnp.float32),
            in_specs=[smem, hbm, hbm],
            out_specs=vmem,
            scratch_shapes=[
                pltpu.VMEM((DEPTH, 256, width), jnp.bfloat16),
                pltpu.VMEM((chunks, GROUP, width), jnp.bfloat16),
                pltpu.SemaphoreType.DMA((DEPTH,)),
                pltpu.SemaphoreType.DMA,
            ],
            compiler_params=pltpu.CompilerParams(vmem_limit_bytes=48 * 1024 * 1024),
            name="score",
        )(tbl.reshape(n * per, 128), hall.reshape(chunks, GROUP, width), head_rows)
        probs, lp = pl.pallas_call(
            functools.partial(finish_kernel, n_model, n_vocab),
            out_shape=(jax.ShapeDtypeStruct((rows, length), jnp.float32), jax.ShapeDtypeStruct((rows,), jnp.float32)),
            in_specs=[vmem, vmem],
            out_specs=(vmem, vmem),
            scratch_shapes=[
                pltpu.VMEM((n, rows // GROUP, 256), jnp.float32),
                pltpu.VMEM((rows, 128), jnp.float32),
                pltpu.VMEM((rows, 128), jnp.float32),
                pltpu.SemaphoreType.DMA((n,)),
                pltpu.SemaphoreType.DMA((n,)),
            ],
            compiler_params=pltpu.CompilerParams(collective_id=1, has_side_effects=True),
            name="finish",
        )(scores.reshape(n, rows // GROUP, 256), meta)
        return probs, lp

    return jax.shard_map(local_step, mesh=mesh, in_specs=(row_spec, P(axes, None), row_spec, row_spec, vec_spec),
                         out_specs=(row_spec, vec_spec), check_vma=False)
```

```python
import functools

import jax
import jax.numpy as jnp
from jax import lax
from jax.experimental import pallas as pl
from jax.experimental.pallas import tpu as pltpu
from jax.sharding import PartitionSpec as P

MESH = pl.DeviceIdType.MESH
TEMP = 0.5
CAP = 16
GROUP = 8
DEPTH = 4
PIECES = 4


def entry_barrier(n_model, n_vocab, m, v):
    barrier = pltpu.get_barrier_semaphore()
    for dm in range(n_model):
        for dv in range(n_vocab):
            if dm or dv:
                pl.semaphore_signal(
                    barrier, inc=1,
                    device_id={"model": lax.rem(m + dm, n_model), "vocab": lax.rem(v + dv, n_vocab)},
                    device_id_type=MESH,
                )
    return barrier


def route_kernel(shard_len, n_model, n_vocab, h_ref, ids_ref, valid_ref, tgt_ref, tbl_ref, hall_ref, meta_ref,
                 t_ref, send_ref, tin_ref, hbuf, tsend, trecv, hsend, hrecv, lsem):
    n = n_model * n_vocab
    rows, length = ids_ref.shape
    m, v = lax.axis_index("model"), lax.axis_index("vocab")
    me = m * n_vocab + v
    barrier = entry_barrier(n_model, n_vocab, m, v)

    ids = ids_ref[...]
    ok = valid_ref[...] > 0
    owner = jnp.where(ok, lax.div(ids, shard_len), n)
    off = lax.rem(ids, shard_len)
    tri = (lax.broadcasted_iota(jnp.int32, (length, length), 0)
           < lax.broadcasted_iota(jnp.int32, (length, length), 1)).astype(jnp.bfloat16)
    rank = jnp.zeros((rows, length), jnp.float32)
    for s in range(n):
        hit = owner == s
        count = jnp.dot(jnp.where(hit, 1.0, 0.0).astype(jnp.bfloat16), tri, preferred_element_type=jnp.float32)
        rank = rank + jnp.where(hit, count, 0.0)
    rank = rank.astype(jnp.int32)
    slot = jnp.where(ok, owner * CAP + rank, n * CAP)
    pair = off - lax.rem(off, 2)

    lane = lax.broadcasted_iota(jnp.int32, (rows, n * CAP), 1)
    row = lax.broadcasted_iota(jnp.int32, (rows, n * CAP), 0)
    spread = lax.rem(((me * rows + row) * CAP + lax.rem(lane, CAP)) * 4, shard_len)
    table = spread
    for j in range(length):
        table = jnp.where(lane == slot[:, j:j + 1], pair[:, j:j + 1], table)
    t_ref[...] = table

    code = jnp.where(ok, owner * (2 * CAP) + rank * 2 + lax.rem(off, 2), -1)
    diag = (lax.broadcasted_iota(jnp.int32, (rows, rows), 0) == lax.broadcasted_iota(jnp.int32, (rows, rows), 1))
    tcol = jnp.sum(jnp.where(diag, tgt_ref[...].reshape(1, rows), 0).astype(jnp.float32), axis=1, keepdims=True)
    meta_ref[:, :length] = code
    meta_ref[:, length:] = jnp.broadcast_to(tcol.astype(jnp.int32), (rows, length))

    groups = 128 // CAP
    per = rows // groups
    lane4 = lax.broadcasted_iota(jnp.int32, (per, 128), 1)
    parts = [jnp.zeros((per, 128), jnp.int32) for _ in range(n)]
    for q in range(groups):
        tq = t_ref[pl.ds(q, per, stride=groups), :]
        inside = lax.div(lane4, CAP) == q
        for s in range(n):
            moved = tq if q == s else pltpu.roll(tq, ((q - s) * CAP) % 128, axis=1)
            parts[s] = jnp.where(inside, moved, parts[s])
    for s in range(n):
        send_ref[s] = parts[s]

    pl.semaphore_wait(barrier, n - 1)

    def remote(src, dst, k, to):
        return pltpu.make_async_remote_copy(src_ref=src, dst_ref=dst, send_sem=hsend.at[k], recv_sem=hrecv.at[k],
                                            device_id=to, device_id_type=MESH)

    def at(mm, vv):
        return {"model": mm, "vocab": vv}

    tcopies = []
    for k in range(1, n):
        dm, dv = k // n_vocab, k % n_vocab
        om, ov = lax.rem(m + dm, n_model), lax.rem(v + dv, n_vocab)
        c = pltpu.make_async_remote_copy(
            src_ref=send_ref.at[om * n_vocab + ov], dst_ref=tin_ref.at[me], send_sem=tsend.at[k], recv_sem=trecv.at[k],
            device_id=at(om, ov), device_id_type=MESH)
        c.start()
        tcopies.append(c)

    core = lax.rem(v, 2)
    xpos = lax.div(v, 2)
    vp = xpos * 2 + (1 - core)
    vx = (1 - xpos) * 2 + core
    my = 1 - m
    partner, xpeer, ypeer = at(m, vp), at(m, vx), at(my, v)
    ix, iy, idg = m * n_vocab + vx, my * n_vocab + v, my * n_vocab + vx
    half = rows // 2
    lo, hi = pl.ds(0, half), pl.ds(half, half)

    own_x = [remote(h_ref.at[lo], hbuf.at[me, lo], 0, xpeer), remote(h_ref.at[hi], hbuf.at[me, hi], 1, xpeer)]
    own_y = [remote(h_ref.at[lo], hbuf.at[me, lo], 2, ypeer), remote(h_ref.at[hi], hbuf.at[me, hi], 3, ypeer)]
    own_p = remote(h_ref, hbuf.at[me], 4, partner)
    x_to_y = remote(hbuf.at[ix, lo], hbuf.at[ix, lo], 5, ypeer)
    y_to_x = remote(hbuf.at[iy, hi], hbuf.at[iy, hi], 6, xpeer)
    x_p = [remote(hbuf.at[ix, lo], hbuf.at[ix, lo], 7, partner), remote(hbuf.at[ix, hi], hbuf.at[ix, hi], 8, partner)]
    y_p = [remote(hbuf.at[iy, lo], hbuf.at[iy, lo], 9, partner), remote(hbuf.at[iy, hi], hbuf.at[iy, hi], 10, partner)]
    d_p = [remote(hbuf.at[idg, lo], hbuf.at[idg, lo], 11, partner), remote(hbuf.at[idg, hi], hbuf.at[idg, hi], 12, partner)]

    own_x[0].start()
    own_y[1].start()
    own_x[1].start()
    own_y[0].start()
    own_p.start()
    keep = pltpu.make_async_copy(h_ref, hall_ref.at[me], lsem.at[0])
    keep.start()
    tbl_ref[me] = send_ref[me]

    own_x[0].wait_recv()
    x_to_y.start()
    x_p[0].start()
    own_y[1].wait_recv()
    y_to_x.start()
    y_p[1].start()
    own_p.wait_recv()
    out = [pltpu.make_async_copy(hbuf.at[m * n_vocab + vp], hall_ref.at[m * n_vocab + vp], lsem.at[1])]
    out[0].start()
    own_x[1].wait_recv()
    x_p[1].start()
    own_y[0].wait_recv()
    y_p[0].start()
    for k in range(1, n):
        tcopies[k - 1].wait_recv()
    for s in range(n):
        @pl.when(s != me)
        def _():
            tbl_ref[s] = tin_ref[s]

    def keep_block(slot, sem):
        c = pltpu.make_async_copy(hbuf.at[slot], hall_ref.at[slot], lsem.at[sem])
        c.start()
        out.append(c)

    keep_block(ix, 2)
    keep_block(iy, 3)
    x_to_y.wait_recv()
    d_p[0].start()
    y_to_x.wait_recv()
    d_p[1].start()
    keep_block(idg, 4)
    for c in x_p:
        c.wait_recv()
    keep_block(m * n_vocab + (1 - xpos) * 2 + (1 - core), 5)
    for c in y_p:
        c.wait_recv()
    keep_block(my * n_vocab + vp, 6)
    for c in d_p:
        c.wait_recv()
    keep_block(my * n_vocab + (1 - xpos) * 2 + (1 - core), 7)
    for c in tcopies + own_x + own_y + [own_p, x_to_y, y_to_x] + x_p + y_p + d_p:
        c.wait_send()
    keep.wait()
    for c in out:
        c.wait()


def score_kernel(chunks, pieces, tbl_ref, h_hbm, w_hbm, out_ref, *scratch):
    bufs, (h_ref, sems, hsem) = scratch[:DEPTH], scratch[DEPTH:]
    slots = 128
    width = w_hbm.shape[1]

    hcopy = pltpu.make_async_copy(h_hbm, h_ref, hsem)
    hcopy.start()

    def issue(c, b, lo=0, hi=slots):
        for k in range(lo, hi):
            at = pl.multiple_of(tbl_ref[c, k], 2)
            pltpu.make_async_copy(
                w_hbm.at[pl.ds(at, 2), :], bufs[b].at[pl.ds(2 * k, 2), :], sems.at[b]
            ).start(priority=k % 2)

    lane = lax.broadcasted_iota(jnp.int32, (GROUP, 2 * slots), 1)
    row = lax.broadcasted_iota(jnp.int32, (GROUP, 2 * slots), 0)
    mine = lax.div(lane, 2 * CAP) == row

    def work(c, b, more):
        pltpu.make_async_copy(w_hbm.at[pl.ds(0, 2 * slots), :], bufs[b], sems.at[b]).wait()
        part = jnp.zeros((GROUP, 2 * slots), jnp.float32)
        for q in range(pieces):
            if more:
                issue(c + DEPTH - 1, (b + DEPTH - 1) % DEPTH, q * slots // pieces, (q + 1) * slots // pieces)
            ks = slice(q * width // pieces, (q + 1) * width // pieces)
            part = part + lax.dot_general(h_ref[c, :, ks], bufs[b][:, ks], (((1,), (1,)), ((), ())),
                                          preferred_element_type=jnp.float32)
        out_ref[pl.ds(c, 1), :] = jnp.sum(jnp.where(mine, part, 0.0), axis=0, keepdims=True)

    for c in range(DEPTH - 1):
        issue(c, c)
    hcopy.wait()

    def step(g, _):
        for b in range(DEPTH):
            work(g * DEPTH + b, b, True)
        return 0

    lax.fori_loop(0, chunks // DEPTH - 1, step, 0)
    for b in range(DEPTH):
        work(chunks - DEPTH + b, b, b == 0)


def finish_kernel(n_model, n_vocab, sc_ref, meta_ref, p_ref, lp_ref, inb, wide0, wide1, ssend, srecv):
    n = n_model * n_vocab
    wide = (wide0, wide1)
    rows, length = p_ref.shape
    m, v = lax.axis_index("model"), lax.axis_index("vocab")
    me = m * n_vocab + v
    barrier = entry_barrier(n_model, n_vocab, m, v)
    pl.semaphore_wait(barrier, n - 1)
    copies = []
    for k in range(1, n):
        om, ov = lax.rem(m + k // n_vocab, n_model), lax.rem(v + k % n_vocab, n_vocab)
        c = pltpu.make_async_remote_copy(
            src_ref=sc_ref.at[om * n_vocab + ov], dst_ref=inb.at[me], send_sem=ssend.at[k], recv_sem=srecv.at[k],
            device_id={"model": om, "vocab": ov}, device_id_type=MESH)
        c.start()
        copies.append(c)
    inb[me] = sc_ref[me]
    for c in copies:
        c.wait_recv()
    width = 2 * CAP
    groups = rows // GROUP
    lane = lax.broadcasted_iota(jnp.int32, (groups, 128), 1)
    per = 128 // width
    for q in range(GROUP):
        for hb in range(2):
            acc = jnp.zeros((groups, 128), jnp.float32)
            for sl in range(per):
                s = hb * per + sl
                src = inb[s][:, (q // per) * 128:(q // per + 1) * 128]
                shift = ((sl - q % per) * width) % 128
                moved = pltpu.roll(src, shift, axis=1) if shift else src
                acc = jnp.where(lax.div(lane, width) == sl, moved, acc)
            wide[hb][pl.ds(q, groups, stride=GROUP), :] = acc
    meta = meta_ref[...]
    code = meta[:, :length]
    ok = code >= 0
    full = jnp.concatenate([jnp.where(ok, code, 0), jnp.zeros((rows, 128 - length), jnp.int32)], axis=1)
    low = jnp.take_along_axis(wide0[...], lax.rem(full, 128), axis=1)
    high = jnp.take_along_axis(wide1[...], lax.rem(full, 128), axis=1)
    scores = jnp.where(full < 128, low, high)[:, :length] / TEMP
    scores = jnp.where(ok, scores, -jnp.inf)
    top = jnp.max(scores, axis=1, keepdims=True)
    log_norm = top + jnp.log(jnp.sum(jnp.exp(scores - top), axis=1, keepdims=True))
    p_ref[...] = jnp.where(ok, jnp.exp(scores - log_norm), 0.0)
    at = lax.broadcasted_iota(jnp.int32, (rows, length), 1)
    picked = jnp.sum(jnp.where(at == meta[:, length:], scores, 0.0), axis=1, keepdims=True)
    diag = (lax.broadcasted_iota(jnp.int32, (rows, rows), 0) == lax.broadcasted_iota(jnp.int32, (rows, rows), 1))
    lp_ref[...] = jnp.sum(jnp.where(diag, picked - log_norm, 0.0), axis=0)
    for c in copies:
        c.wait_send()


def solution(mesh):
    axes = ("model", "vocab")
    n_model, n_vocab = mesh.shape["model"], mesh.shape["vocab"]
    n = n_model * n_vocab
    row_spec = P(("rep",) + axes, None)
    vec_spec = P(("rep",) + axes)
    vmem = pl.BlockSpec(memory_space=pltpu.VMEM)
    hbm = pl.BlockSpec(memory_space=pl.ANY)
    smem = pl.BlockSpec(memory_space=pltpu.SMEM)

    def local_step(hidden, head_rows, allowed_ids, valid_mask, target_pos):
        rows, length = allowed_ids.shape
        shard_len, width = head_rows.shape
        per = rows * CAP // 128
        tbl, hall, meta = pl.pallas_call(
            functools.partial(route_kernel, shard_len, n_model, n_vocab),
            out_shape=(jax.ShapeDtypeStruct((n, per, 128), jnp.int32),
                       jax.ShapeDtypeStruct((n, rows, width), jnp.bfloat16),
                       jax.ShapeDtypeStruct((rows, 2 * length), jnp.int32)),
            in_specs=[vmem, vmem, vmem, vmem],
            out_specs=(vmem, hbm, vmem),
            scratch_shapes=[
                pltpu.VMEM((rows, n * CAP), jnp.int32),
                pltpu.VMEM((n, per, 128), jnp.int32),
                pltpu.VMEM((n, per, 128), jnp.int32),
                pltpu.VMEM((n, rows, width), jnp.bfloat16),
                pltpu.SemaphoreType.DMA((n,)),
                pltpu.SemaphoreType.DMA((n,)),
                pltpu.SemaphoreType.DMA((13,)),
                pltpu.SemaphoreType.DMA((13,)),
                pltpu.SemaphoreType.DMA((n,)),
            ],
            compiler_params=pltpu.CompilerParams(collective_id=0, has_side_effects=True),
            name="route",
        )(hidden, allowed_ids, valid_mask, target_pos)
        chunks = n * rows // GROUP
        scores = pl.pallas_call(
            functools.partial(score_kernel, chunks, PIECES),
            out_shape=jax.ShapeDtypeStruct((chunks, 256), jnp.float32),
            in_specs=[smem, hbm, hbm],
            out_specs=vmem,
            scratch_shapes=[
                *[pltpu.VMEM((256, width), jnp.bfloat16)] * DEPTH,
                pltpu.VMEM((chunks, GROUP, width), jnp.bfloat16),
                pltpu.SemaphoreType.DMA((DEPTH,)),
                pltpu.SemaphoreType.DMA,
            ],
            compiler_params=pltpu.CompilerParams(vmem_limit_bytes=48 * 1024 * 1024),
            name="score",
        )(tbl.reshape(n * per, 128), hall.reshape(chunks, GROUP, width), head_rows)
        probs, lp = pl.pallas_call(
            functools.partial(finish_kernel, n_model, n_vocab),
            out_shape=(jax.ShapeDtypeStruct((rows, length), jnp.float32), jax.ShapeDtypeStruct((rows,), jnp.float32)),
            in_specs=[vmem, vmem],
            out_specs=(vmem, vmem),
            scratch_shapes=[
                pltpu.VMEM((n, rows // GROUP, 256), jnp.float32),
                pltpu.VMEM((rows, 128), jnp.float32),
                pltpu.VMEM((rows, 128), jnp.float32),
                pltpu.SemaphoreType.DMA((n,)),
                pltpu.SemaphoreType.DMA((n,)),
            ],
            compiler_params=pltpu.CompilerParams(collective_id=1, has_side_effects=True),
            name="finish",
        )(scores.reshape(n, rows // GROUP, 256), meta)
        return probs, lp

    return jax.shard_map(local_step, mesh=mesh, in_specs=(row_spec, P(axes, None), row_spec, row_spec, vec_spec),
                         out_specs=(row_spec, vec_spec), check_vma=False)
```

```python
import functools

import jax
import jax.numpy as jnp
from jax import lax
from jax.experimental import pallas as pl
from jax.experimental.pallas import tpu as pltpu
from jax.sharding import PartitionSpec as P

MESH = pl.DeviceIdType.MESH
TEMP = 0.5
CAP = 16
SLOTS = 128
DEPTH = 4


def entry_barrier(n_model, n_vocab, m, v):
    barrier = pltpu.get_barrier_semaphore()
    for dm in range(n_model):
        for dv in range(n_vocab):
            if dm or dv:
                pl.semaphore_signal(
                    barrier, inc=1,
                    device_id={"model": lax.rem(m + dm, n_model), "vocab": lax.rem(v + dv, n_vocab)},
                    device_id_type=MESH,
                )
    return barrier


def route_kernel(shard_len, n_model, n_vocab, h_ref, ids_ref, valid_ref, tgt_ref, tbl_ref, hall_ref, meta_ref,
                 t_ref, send_ref, tin_ref, hbuf, tsend, trecv, hsend, hrecv, lsem):
    n = n_model * n_vocab
    rows, length = ids_ref.shape
    m, v = lax.axis_index("model"), lax.axis_index("vocab")
    me = m * n_vocab + v
    barrier = entry_barrier(n_model, n_vocab, m, v)

    ids = ids_ref[...]
    ok = valid_ref[...] > 0
    owner = jnp.where(ok, lax.div(ids, shard_len), n)
    off = lax.rem(ids, shard_len)
    tri = (lax.broadcasted_iota(jnp.int32, (length, length), 0)
           < lax.broadcasted_iota(jnp.int32, (length, length), 1)).astype(jnp.bfloat16)
    rank = jnp.zeros((rows, length), jnp.float32)
    for s in range(n):
        hit = owner == s
        count = jnp.dot(jnp.where(hit, 1.0, 0.0).astype(jnp.bfloat16), tri, preferred_element_type=jnp.float32)
        rank = rank + jnp.where(hit, count, 0.0)
    rank = rank.astype(jnp.int32)
    slot = jnp.where(ok, owner * CAP + rank, n * CAP)
    pair = off - lax.rem(off, 2)

    lane = lax.broadcasted_iota(jnp.int32, (rows, n * CAP), 1)
    row = lax.broadcasted_iota(jnp.int32, (rows, n * CAP), 0)
    spread = lax.rem(((me * rows + row) * CAP + lax.rem(lane, CAP)) * 4, shard_len)
    table = spread
    for j in range(length):
        table = jnp.where(lane == slot[:, j:j + 1], pair[:, j:j + 1], table)
    t_ref[...] = table

    code = lax.div(rank, 4) * (n * 8) + owner * 8 + lax.rem(rank, 4) * 2 + lax.rem(off, 2)
    code = jnp.where(ok, code, -1)
    diag = (lax.broadcasted_iota(jnp.int32, (rows, rows), 0) == lax.broadcasted_iota(jnp.int32, (rows, rows), 1))
    tcol = jnp.sum(jnp.where(diag, tgt_ref[...].reshape(1, rows), 0).astype(jnp.float32), axis=1, keepdims=True)
    meta_ref[:, :length] = code
    meta_ref[:, length:] = jnp.broadcast_to(tcol.astype(jnp.int32), (rows, length))

    groups = 128 // CAP
    per = rows // groups
    lane4 = lax.broadcasted_iota(jnp.int32, (per, 128), 1)
    parts = [jnp.zeros((per, 128), jnp.int32) for _ in range(n)]
    for q in range(groups):
        tq = t_ref[pl.ds(q, per, stride=groups), :]
        inside = lax.div(lane4, CAP) == q
        for s in range(n):
            moved = tq if q == s else pltpu.roll(tq, ((q - s) * CAP) % 128, axis=1)
            parts[s] = jnp.where(inside, moved, parts[s])
    for s in range(n):
        send_ref[s] = parts[s]

    pl.semaphore_wait(barrier, n - 1)

    def remote(src, dst, k, to):
        return pltpu.make_async_remote_copy(src_ref=src, dst_ref=dst, send_sem=hsend.at[k], recv_sem=hrecv.at[k],
                                            device_id=to, device_id_type=MESH)

    def at(mm, vv):
        return {"model": mm, "vocab": vv}

    tcopies = []
    for k in range(1, n):
        dm, dv = k // n_vocab, k % n_vocab
        om, ov = lax.rem(m + dm, n_model), lax.rem(v + dv, n_vocab)
        c = pltpu.make_async_remote_copy(
            src_ref=send_ref.at[om * n_vocab + ov], dst_ref=tin_ref.at[me], send_sem=tsend.at[k], recv_sem=trecv.at[k],
            device_id=at(om, ov), device_id_type=MESH)
        c.start()
        tcopies.append(c)

    core = lax.rem(v, 2)
    xpos = lax.div(v, 2)
    vp = xpos * 2 + (1 - core)
    vx = (1 - xpos) * 2 + core
    my = 1 - m
    partner, xpeer, ypeer = at(m, vp), at(m, vx), at(my, v)
    ix, iy, idg = m * n_vocab + vx, my * n_vocab + v, my * n_vocab + vx
    half = rows // 2
    lo, hi = pl.ds(0, half), pl.ds(half, half)

    own_x = [remote(h_ref.at[lo], hbuf.at[me, lo], 0, xpeer), remote(h_ref.at[hi], hbuf.at[me, hi], 1, xpeer)]
    own_y = [remote(h_ref.at[lo], hbuf.at[me, lo], 2, ypeer), remote(h_ref.at[hi], hbuf.at[me, hi], 3, ypeer)]
    own_p = remote(h_ref, hbuf.at[me], 4, partner)
    x_to_y = remote(hbuf.at[ix, lo], hbuf.at[ix, lo], 5, ypeer)
    y_to_x = remote(hbuf.at[iy, hi], hbuf.at[iy, hi], 6, xpeer)
    x_p = [remote(hbuf.at[ix, lo], hbuf.at[ix, lo], 7, partner), remote(hbuf.at[ix, hi], hbuf.at[ix, hi], 8, partner)]
    y_p = [remote(hbuf.at[iy, lo], hbuf.at[iy, lo], 9, partner), remote(hbuf.at[iy, hi], hbuf.at[iy, hi], 10, partner)]
    d_p = [remote(hbuf.at[idg, lo], hbuf.at[idg, lo], 11, partner), remote(hbuf.at[idg, hi], hbuf.at[idg, hi], 12, partner)]

    own_x[0].start()
    own_y[1].start()
    own_x[1].start()
    own_y[0].start()
    own_p.start()
    keep = pltpu.make_async_copy(h_ref, hall_ref.at[me], lsem.at[0])
    keep.start()
    tbl_ref[me] = send_ref[me]

    own_x[0].wait_recv()
    x_to_y.start()
    x_p[0].start()
    own_y[1].wait_recv()
    y_to_x.start()
    y_p[1].start()
    own_p.wait_recv()
    out = [pltpu.make_async_copy(hbuf.at[m * n_vocab + vp], hall_ref.at[m * n_vocab + vp], lsem.at[1])]
    out[0].start()
    own_x[1].wait_recv()
    x_p[1].start()
    own_y[0].wait_recv()
    y_p[0].start()
    for k in range(1, n):
        tcopies[k - 1].wait_recv()
    for s in range(n):
        @pl.when(s != me)
        def _():
            tbl_ref[s] = tin_ref[s]

    def keep_block(slot, sem):
        c = pltpu.make_async_copy(hbuf.at[slot], hall_ref.at[slot], lsem.at[sem])
        c.start()
        out.append(c)

    keep_block(ix, 2)
    keep_block(iy, 3)
    x_to_y.wait_recv()
    d_p[0].start()
    y_to_x.wait_recv()
    d_p[1].start()
    keep_block(idg, 4)
    for c in x_p:
        c.wait_recv()
    keep_block(m * n_vocab + (1 - xpos) * 2 + (1 - core), 5)
    for c in y_p:
        c.wait_recv()
    keep_block(my * n_vocab + vp, 6)
    for c in d_p:
        c.wait_recv()
    keep_block(my * n_vocab + (1 - xpos) * 2 + (1 - core), 7)
    for c in tcopies + own_x + own_y + [own_p, x_to_y, y_to_x] + x_p + y_p + d_p:
        c.wait_send()
    keep.wait()
    for c in out:
        c.wait()


def score_kernel(chunks, tbl_ref, h_hbm, w_hbm, out_ref, *scratch):
    bufs, (h_ref, hf_ref, sems, hsem) = scratch[:DEPTH], scratch[DEPTH:]
    tiles = w_hbm.shape[1]
    nrow = SLOTS // CAP
    quads = CAP // 4

    hcopy = pltpu.make_async_copy(h_hbm, h_ref, hsem)
    hcopy.start()

    def issue(c, b, k):
        at = tbl_ref[c, k]
        t, p = lax.shift_right_logical(at, 3), lax.bitwise_and(lax.shift_right_logical(at, 1), 3)
        pltpu.make_async_copy(
            w_hbm.at[t, :, p], bufs[b].at[k // 4, :, pl.ds(2 * (k % 4), 2), :], sems.at[b]).start(priority=k % 2)

    lane = lax.broadcasted_iota(jnp.int32, (8, 128), 1)

    def work(c, b, more):
        pltpu.make_async_copy(bufs[b], bufs[b], sems.at[b]).wait()
        flat = bufs[b].reshape(SLOTS // 4 * tiles * 8, 128)
        hf_ref[...] = h_ref[c].astype(jnp.float32)
        got = jnp.zeros((8, 128), jnp.float32)
        base = lax.rem(c, 128 // (SLOTS // 4)) * (SLOTS // 4)
        for i in range(nrow):
            acc = [[jnp.zeros((8, 128), jnp.float32)] * 2 for _ in range(quads)]
            for kk in range(0, tiles, 2):
                if more:
                    for k in range(-(-kk * CAP // tiles), -(-(kk + 2) * CAP // tiles)):
                        issue(c + DEPTH - 1, (b + DEPTH - 1) % DEPTH, i * CAP + k)
                hb = [jnp.broadcast_to(hf_ref[i:i + 1, (kk + z) * 128:(kk + z + 1) * 128], (8, 128)) for z in (0, 1)]
                for g in range(quads):
                    at = ((i * quads + g) * tiles + kk) * 8
                    x = flat[at:at + 16, :].astype(jnp.float32)
                    acc[g] = [acc[g][0] + x[:8] * hb[0], acc[g][1] + x[8:] * hb[1]]
            for g in range(quads):
                total = jnp.sum(acc[g][0] + acc[g][1], axis=1, keepdims=True)
                got = jnp.where(lane == base + (i * quads + g), total, got)
        at = lax.div(c, 128 // (SLOTS // 4))
        fresh = (lane >= base) & (lane < base + SLOTS // 4)
        out_ref[at] = jnp.where(fresh, got, out_ref[at])

    for c in range(DEPTH - 1):
        for k in range(SLOTS):
            issue(c, c, k)
    hcopy.wait()

    def step(g, _):
        for b in range(DEPTH):
            work(g * DEPTH + b, b, True)
        return 0

    lax.fori_loop(0, chunks // DEPTH - 1, step, 0)
    for b in range(DEPTH):
        work(chunks - DEPTH + b, b, b == 0)


def finish_kernel(n_model, n_vocab, sc_ref, meta_ref, p_ref, lp_ref, inb, flip, ssend, srecv):
    n = n_model * n_vocab
    rows, length = p_ref.shape
    m, v = lax.axis_index("model"), lax.axis_index("vocab")
    me = m * n_vocab + v
    barrier = entry_barrier(n_model, n_vocab, m, v)
    pl.semaphore_wait(barrier, n - 1)
    copies = []
    for k in range(1, n):
        om, ov = lax.rem(m + k // n_vocab, n_model), lax.rem(v + k % n_vocab, n_vocab)
        c = pltpu.make_async_remote_copy(
            src_ref=sc_ref.at[om * n_vocab + ov], dst_ref=inb.at[me], send_sem=ssend.at[k], recv_sem=srecv.at[k],
            device_id={"model": om, "vocab": ov}, device_id_type=MESH)
        c.start()
        copies.append(c)
    inb[me] = sc_ref[me]
    for c in copies:
        c.wait_recv()
    flip[...] = inb[...].reshape(n * 8, 128).T
    wide = [jnp.concatenate([flip[pl.ds(q, rows, stride=4), :] for q in (2 * hb, 2 * hb + 1)], axis=1) for hb in (0, 1)]
    meta = meta_ref[...]
    code = meta[:, :length]
    ok = code >= 0
    full = jnp.concatenate([jnp.where(ok, code, 0), jnp.zeros((rows, 128 - length), jnp.int32)], axis=1)
    low = jnp.take_along_axis(wide[0], lax.rem(full, 128), axis=1)
    high = jnp.take_along_axis(wide[1], lax.rem(full, 128), axis=1)
    scores = jnp.where(full < 128, low, high)[:, :length] / TEMP
    scores = jnp.where(ok, scores, -jnp.inf)
    top = jnp.max(scores, axis=1, keepdims=True)
    log_norm = top + jnp.log(jnp.sum(jnp.exp(scores - top), axis=1, keepdims=True))
    p_ref[...] = jnp.where(ok, jnp.exp(scores - log_norm), 0.0)
    at = lax.broadcasted_iota(jnp.int32, (rows, length), 1)
    picked = jnp.sum(jnp.where(at == meta[:, length:], scores, 0.0), axis=1, keepdims=True)
    diag = (lax.broadcasted_iota(jnp.int32, (rows, rows), 0) == lax.broadcasted_iota(jnp.int32, (rows, rows), 1))
    lp_ref[...] = jnp.sum(jnp.where(diag, picked - log_norm, 0.0), axis=0)
    for c in copies:
        c.wait_send()


def solution(mesh):
    axes = ("model", "vocab")
    n_model, n_vocab = mesh.shape["model"], mesh.shape["vocab"]
    n = n_model * n_vocab
    row_spec = P(("rep",) + axes, None)
    vec_spec = P(("rep",) + axes)
    vmem = pl.BlockSpec(memory_space=pltpu.VMEM)
    hbm = pl.BlockSpec(memory_space=pl.ANY)
    smem = pl.BlockSpec(memory_space=pltpu.SMEM)

    def local_step(hidden, head_rows, allowed_ids, valid_mask, target_pos):
        rows, length = allowed_ids.shape
        shard_len, width = head_rows.shape
        per = rows * CAP // 128
        tiles = width // 128
        tbl, hall, meta = pl.pallas_call(
            functools.partial(route_kernel, shard_len, n_model, n_vocab),
            out_shape=(jax.ShapeDtypeStruct((n, per, 128), jnp.int32),
                       jax.ShapeDtypeStruct((n, rows, width), jnp.bfloat16),
                       jax.ShapeDtypeStruct((rows, 2 * length), jnp.int32)),
            in_specs=[vmem, vmem, vmem, vmem],
            out_specs=(vmem, hbm, vmem),
            scratch_shapes=[
                pltpu.VMEM((rows, n * CAP), jnp.int32),
                pltpu.VMEM((n, per, 128), jnp.int32),
                pltpu.VMEM((n, per, 128), jnp.int32),
                pltpu.VMEM((n, rows, width), jnp.bfloat16),
                pltpu.SemaphoreType.DMA((n,)),
                pltpu.SemaphoreType.DMA((n,)),
                pltpu.SemaphoreType.DMA((13,)),
                pltpu.SemaphoreType.DMA((13,)),
                pltpu.SemaphoreType.DMA((n,)),
            ],
            compiler_params=pltpu.CompilerParams(collective_id=0, has_side_effects=True),
            name="route",
        )(hidden, allowed_ids, valid_mask, target_pos)
        chunks = n * rows * CAP // SLOTS
        pairs = head_rows.reshape(shard_len // 8, 4, 2, tiles, 128).transpose(0, 3, 1, 2, 4)
        scores = pl.pallas_call(
            functools.partial(score_kernel, chunks),
            out_shape=jax.ShapeDtypeStruct((n, 8, 128), jnp.float32),
            in_specs=[smem, hbm, hbm],
            out_specs=vmem,
            scratch_shapes=[
                *[pltpu.VMEM((SLOTS // 4, tiles, 8, 128), jnp.bfloat16)] * DEPTH,
                pltpu.VMEM((chunks, SLOTS // CAP, width), jnp.bfloat16),
                pltpu.VMEM((SLOTS // CAP, width), jnp.float32),
                pltpu.SemaphoreType.DMA((DEPTH,)),
                pltpu.SemaphoreType.DMA,
            ],
            compiler_params=pltpu.CompilerParams(vmem_limit_bytes=48 * 1024 * 1024),
            name="score",
        )(tbl.reshape(chunks, SLOTS), hall.reshape(chunks, SLOTS // CAP, width), pairs)
        probs, lp = pl.pallas_call(
            functools.partial(finish_kernel, n_model, n_vocab),
            out_shape=(jax.ShapeDtypeStruct((rows, length), jnp.float32), jax.ShapeDtypeStruct((rows,), jnp.float32)),
            in_specs=[vmem, vmem],
            out_specs=(vmem, vmem),
            scratch_shapes=[
                pltpu.VMEM((n, 8, 128), jnp.float32),
                pltpu.VMEM((128, n * 8), jnp.float32),
                pltpu.SemaphoreType.DMA((n,)),
                pltpu.SemaphoreType.DMA((n,)),
            ],
            compiler_params=pltpu.CompilerParams(collective_id=1, has_side_effects=True),
            name="finish",
        )(scores, meta)
        return probs, lp

    return jax.shard_map(local_step, mesh=mesh, in_specs=(row_spec, P(axes, None), row_spec, row_spec, vec_spec),
                         out_specs=(row_spec, vec_spec), check_vma=False)
```

```python
import functools

import jax
import jax.numpy as jnp
from jax import lax
from jax.experimental import pallas as pl
from jax.experimental.pallas import tpu as pltpu
from jax.sharding import PartitionSpec as P

MESH = pl.DeviceIdType.MESH
TEMP = 0.5
CAP = 16
SLOTS = 128
DEPTH = 4
STAGES = ((0, 1), (2, 4, 6), (3, 5, 7))


def flip_bits(a, k):
    for bit in (1, 2):
        if k & bit:
            a = a + bit - 2 * bit * lax.rem(lax.div(a, bit), 2)
    return a


def peer(m, v, k, n_vocab):
    return flip_bits(m, k // n_vocab), flip_bits(v, k % n_vocab)


def entry_barrier(n, n_vocab, m, v):
    barrier = pltpu.get_barrier_semaphore()
    for k in range(1, n):
        pm, pv = peer(m, v, k, n_vocab)
        pl.semaphore_signal(barrier, inc=1, device_id={"model": pm, "vocab": pv}, device_id_type=MESH)
    return barrier


def route_kernel(shard_len, n, n_vocab, ids_ref, valid_ref, tgt_ref, tbl_ref, meta_ref, t_ref, send_ref, tin_ref, tsend, trecv):
    rows, length = ids_ref.shape
    m, v = lax.axis_index("model"), lax.axis_index("vocab")
    me = m * n_vocab + v
    barrier = entry_barrier(n, n_vocab, m, v)

    ids = ids_ref[...]
    ok = valid_ref[...] > 0
    owner = jnp.where(ok, lax.div(ids, shard_len), n)
    off = lax.rem(ids, shard_len)
    tri = (lax.broadcasted_iota(jnp.int32, (length, length), 0)
           < lax.broadcasted_iota(jnp.int32, (length, length), 1)).astype(jnp.bfloat16)
    rank = jnp.zeros((rows, length), jnp.float32)
    for s in range(n):
        hit = owner == s
        count = jnp.dot(jnp.where(hit, 1.0, 0.0).astype(jnp.bfloat16), tri, preferred_element_type=jnp.float32)
        rank = rank + jnp.where(hit, count, 0.0)
    rank = rank.astype(jnp.int32)
    slot = jnp.where(ok, owner * CAP + rank, n * CAP)
    pair = off - lax.rem(off, 2)

    lane = lax.broadcasted_iota(jnp.int32, (rows, n * CAP), 1)
    row = lax.broadcasted_iota(jnp.int32, (rows, n * CAP), 0)
    spread = lax.rem(((me * rows + row) * CAP + lax.rem(lane, CAP)) * 4, shard_len)
    table = spread
    for j in range(length):
        table = jnp.where(lane == slot[:, j:j + 1], pair[:, j:j + 1], table)
    t_ref[...] = table

    groups = 128 // CAP
    per = rows // groups
    lane4 = lax.broadcasted_iota(jnp.int32, (per, 128), 1)
    parts = [jnp.zeros((per, 128), jnp.int32) for _ in range(n)]
    for q in range(groups):
        tq = t_ref[pl.ds(q, per, stride=groups), :]
        inside = lax.div(lane4, CAP) == q
        for s in range(n):
            moved = tq if q == s else pltpu.roll(tq, ((q - s) * CAP) % 128, axis=1)
            parts[s] = jnp.where(inside, moved, parts[s])
    for s in range(n):
        send_ref[s] = parts[s]

    code = lax.div(rank, 4) * (n * 8) + owner * 8 + lax.rem(rank, 4) * 2 + lax.rem(off, 2)
    diag = (lax.broadcasted_iota(jnp.int32, (rows, rows), 0) == lax.broadcasted_iota(jnp.int32, (rows, rows), 1))
    tcol = jnp.sum(jnp.where(diag, tgt_ref[...].reshape(1, rows), 0).astype(jnp.float32), axis=1, keepdims=True)
    meta_ref[:, :length] = jnp.where(ok, code, -1)
    meta_ref[:, length:] = jnp.broadcast_to(tcol.astype(jnp.int32), (rows, length))

    pl.semaphore_wait(barrier, n - 1)
    copies = []
    for k in range(1, n):
        pm, pv = peer(m, v, k, n_vocab)
        c = pltpu.make_async_remote_copy(
            src_ref=send_ref.at[pm * n_vocab + pv], dst_ref=tin_ref.at[k], send_sem=tsend.at[k], recv_sem=trecv.at[k],
            device_id={"model": pm, "vocab": pv}, device_id_type=MESH)
        c.start()
        copies.append(c)
    tbl_ref[0] = send_ref[me]
    for k in range(1, n):
        copies[k - 1].wait_recv()
        tbl_ref[k] = tin_ref[k]
    for c in copies:
        c.wait_send()


def score_kernel(blocks, *refs):
    nb = len(blocks)
    tbl_ref, w_hbm, h_refs, out_ref = refs[0], refs[1], refs[2:2 + nb], refs[2 + nb]
    bufs = refs[3 + nb:3 + nb + DEPTH]
    hf_ref, sems = refs[3 + nb + DEPTH:]
    tiles = w_hbm.shape[1]
    nrow = SLOTS // CAP
    quads = CAP // 4
    per = h_refs[0].shape[0] // nrow
    chunks = nb * per

    def table_row(c):
        if isinstance(c, int):
            return blocks[c // per] * per + c % per
        i = lax.div(c, per)
        blk = jnp.int32(blocks[0])
        for z in range(1, nb):
            blk = jnp.where(i == z, blocks[z], blk)
        return blk * per + lax.rem(c, per)

    def issue(r, b, k):
        at = tbl_ref[r, k]
        t, p = lax.shift_right_logical(at, 3), lax.bitwise_and(lax.shift_right_logical(at, 1), 3)
        pltpu.make_async_copy(
            w_hbm.at[t, :, p], bufs[b].at[k // 4, :, pl.ds(2 * (k % 4), 2), :], sems.at[b]).start(priority=k % 2)

    lane = lax.broadcasted_iota(jnp.int32, (8, 128), 1)

    def work(c, b, more):
        ahead = table_row(c + DEPTH - 1) if more else None
        pltpu.make_async_copy(bufs[b], bufs[b], sems.at[b]).wait()
        flat = bufs[b].reshape(SLOTS // 4 * tiles * 8, 128)
        blk, part = lax.div(c, per), lax.rem(c, per)
        for z in range(nb):
            @pl.when(blk == z)
            def _():
                hf_ref[...] = h_refs[z][pl.ds(pl.multiple_of(part * nrow, nrow), nrow), :].astype(jnp.float32)
        got = jnp.zeros((8, 128), jnp.float32)
        base = part * (SLOTS // 4)
        for i in range(nrow):
            acc = [[jnp.zeros((8, 128), jnp.float32)] * 2 for _ in range(quads)]
            for kk in range(0, tiles, 2):
                if more:
                    for k in range(-(-kk * CAP // tiles), -(-(kk + 2) * CAP // tiles)):
                        issue(ahead, (b + DEPTH - 1) % DEPTH, i * CAP + k)
                hb = [jnp.broadcast_to(hf_ref[i:i + 1, (kk + z) * 128:(kk + z + 1) * 128], (8, 128)) for z in (0, 1)]
                for g in range(quads):
                    at = ((i * quads + g) * tiles + kk) * 8
                    x = flat[at:at + 16, :].astype(jnp.float32)
                    acc[g] = [acc[g][0] + x[:8] * hb[0], acc[g][1] + x[8:] * hb[1]]
            for g in range(quads):
                total = jnp.sum(acc[g][0] + acc[g][1], axis=1, keepdims=True)
                got = jnp.where(lane == base + (i * quads + g), total, got)
        fresh = (lane >= base) & (lane < base + SLOTS // 4)
        out_ref[blk] = jnp.where(fresh, got, out_ref[blk])

    for c in range(DEPTH - 1):
        for k in range(SLOTS):
            issue(table_row(c), c, k)

    def step(g, _):
        for b in range(DEPTH):
            work(g * DEPTH + b, b, True)
        return 0

    lax.fori_loop(0, chunks // DEPTH - 1, step, 0)
    for b in range(DEPTH):
        work(jnp.int32(chunks - DEPTH + b), b, b == 0)


def return_kernel(n, n_vocab, *refs):
    ns = len(STAGES)
    scs, out_ref, inb, ssend, srecv = refs[:ns], refs[ns], refs[ns + 1], refs[ns + 2], refs[ns + 3]
    m, v = lax.axis_index("model"), lax.axis_index("vocab")
    me = m * n_vocab + v
    barrier = entry_barrier(n, n_vocab, m, v)
    pl.semaphore_wait(barrier, n - 1)
    copies = []
    for sc, blocks in zip(scs, STAGES):
        for i, k in enumerate(blocks):
            if k == 0:
                out_ref[me] = sc[i]
                continue
            pm, pv = peer(m, v, k, n_vocab)
            c = pltpu.make_async_remote_copy(
                src_ref=sc.at[i], dst_ref=inb.at[k], send_sem=ssend.at[k], recv_sem=srecv.at[k],
                device_id={"model": pm, "vocab": pv}, device_id_type=MESH)
            c.start()
            copies.append((k, c))
    for k, c in copies:
        c.wait_recv()
        pm, pv = peer(m, v, k, n_vocab)
        out_ref[pm * n_vocab + pv] = inb[k]
    for k, c in copies:
        c.wait_send()


def softmax_kernel(sc_ref, meta_ref, p_ref, lp_ref, flip):
    n = sc_ref.shape[0]
    rows, length = p_ref.shape
    flip[...] = sc_ref[...].reshape(n * 8, 128).T
    wide = [jnp.concatenate([flip[pl.ds(q, rows, stride=4), :] for q in (2 * hb, 2 * hb + 1)], axis=1) for hb in (0, 1)]
    meta = meta_ref[...]
    code = meta[:, :length]
    ok = code >= 0
    full = jnp.concatenate([jnp.where(ok, code, 0), jnp.zeros((rows, 128 - length), jnp.int32)], axis=1)
    low = jnp.take_along_axis(wide[0], lax.rem(full, 128), axis=1)
    high = jnp.take_along_axis(wide[1], lax.rem(full, 128), axis=1)
    scores = jnp.where(full < 128, low, high)[:, :length] / TEMP
    scores = jnp.where(ok, scores, -jnp.inf)
    top = jnp.max(scores, axis=1, keepdims=True)
    log_norm = top + jnp.log(jnp.sum(jnp.exp(scores - top), axis=1, keepdims=True))
    p_ref[...] = jnp.where(ok, jnp.exp(scores - log_norm), 0.0)
    at = lax.broadcasted_iota(jnp.int32, (rows, length), 1)
    picked = jnp.sum(jnp.where(at == meta[:, length:], scores, 0.0), axis=1, keepdims=True)
    diag = (lax.broadcasted_iota(jnp.int32, (rows, rows), 0) == lax.broadcasted_iota(jnp.int32, (rows, rows), 1))
    lp_ref[...] = jnp.sum(jnp.where(diag, picked - log_norm, 0.0), axis=0)


def solution(mesh):
    axes = ("model", "vocab")
    n_model, n_vocab = mesh.shape["model"], mesh.shape["vocab"]
    n = n_model * n_vocab
    row_spec = P(("rep",) + axes, None)
    vec_spec = P(("rep",) + axes)
    vmem = pl.BlockSpec(memory_space=pltpu.VMEM)
    hbm = pl.BlockSpec(memory_space=pl.ANY)
    smem = pl.BlockSpec(memory_space=pltpu.SMEM)

    def local_step(hidden, head_rows, allowed_ids, valid_mask, target_pos):
        rows, length = allowed_ids.shape
        shard_len, width = head_rows.shape
        per = rows * CAP // 128
        tiles = width // 128

        def exchange(x, k):
            return lax.ppermute(x, axes, [(s, s ^ k) for s in range(n)])

        blocks = {0: hidden}
        for k in (1, 2, 4, 6):
            blocks[k] = exchange(hidden, k)
        tbl, meta = pl.pallas_call(
            functools.partial(route_kernel, shard_len, n, n_vocab),
            out_shape=(jax.ShapeDtypeStruct((n, per, 128), jnp.int32),
                       jax.ShapeDtypeStruct((rows, 2 * length), jnp.int32)),
            in_specs=[vmem, vmem, vmem],
            out_specs=(vmem, vmem),
            scratch_shapes=[
                pltpu.VMEM((rows, n * CAP), jnp.int32),
                pltpu.VMEM((n, per, 128), jnp.int32),
                pltpu.VMEM((n, per, 128), jnp.int32),
                pltpu.SemaphoreType.DMA((n,)),
                pltpu.SemaphoreType.DMA((n,)),
            ],
            compiler_params=pltpu.CompilerParams(collective_id=0, has_side_effects=True),
            cost_estimate=pl.CostEstimate(flops=10_000_000, bytes_accessed=10_000, transcendentals=0),
            name="route",
        )(allowed_ids, valid_mask, target_pos)
        pairs = head_rows.reshape(shard_len // 8, 4, 2, tiles, 128).transpose(0, 3, 1, 2, 4)
        scores = []
        for stage in STAGES:
            nb = len(stage)
            if len(scores) == 1:
                *far, scores[0] = lax.optimization_barrier((*[blocks[k] for k in (2, 4, 6)], scores[0]))
                for k, x in zip((2, 4, 6), far):
                    blocks[k], blocks[k + 1] = x, exchange(x, 1)
            scores.append(pl.pallas_call(
                functools.partial(score_kernel, stage),
                out_shape=jax.ShapeDtypeStruct((nb, 8, 128), jnp.float32),
                in_specs=[smem, hbm] + [vmem] * nb,
                out_specs=vmem,
                scratch_shapes=[
                    *[pltpu.VMEM((SLOTS // 4, tiles, 8, 128), jnp.bfloat16)] * DEPTH,
                    pltpu.VMEM((SLOTS // CAP, width), jnp.float32),
                    pltpu.SemaphoreType.DMA((DEPTH,)),
                ],
                compiler_params=pltpu.CompilerParams(vmem_limit_bytes=24 * 1024 * 1024),
                cost_estimate=pl.CostEstimate(flops=20_000_000 * nb, bytes_accessed=nb * 10_000_000, transcendentals=0),
                name=f"score{stage[0]}",
            )(tbl.reshape(n * per, 128), pairs, *[blocks[k] for k in stage]))
        back = pl.pallas_call(
            functools.partial(return_kernel, n, n_vocab),
            out_shape=jax.ShapeDtypeStruct((n, 8, 128), jnp.float32),
            in_specs=[vmem] * len(STAGES),
            out_specs=vmem,
            scratch_shapes=[
                pltpu.VMEM((n, 8, 128), jnp.float32),
                pltpu.SemaphoreType.DMA((n,)),
                pltpu.SemaphoreType.DMA((n,)),
            ],
            compiler_params=pltpu.CompilerParams(collective_id=1, has_side_effects=True),
            name="giveback",
        )(*scores)
        return pl.pallas_call(
            softmax_kernel,
            out_shape=(jax.ShapeDtypeStruct((rows, length), jnp.float32), jax.ShapeDtypeStruct((rows,), jnp.float32)),
            in_specs=[vmem, vmem],
            out_specs=(vmem, vmem),
            scratch_shapes=[pltpu.VMEM((128, n * 8), jnp.float32)],
            name="finish",
        )(back, meta)

    return jax.shard_map(local_step, mesh=mesh, in_specs=(row_spec, P(axes, None), row_spec, row_spec, vec_spec),
                         out_specs=(row_spec, vec_spec), check_vma=False)
```

```python
import functools

import jax
import jax.numpy as jnp
from jax import lax
from jax.experimental import pallas as pl
from jax.experimental.pallas import tpu as pltpu
from jax.sharding import PartitionSpec as P

MESH = pl.DeviceIdType.MESH
TEMP = 0.5
CAP = 16
SLOTS = 128
DEPTH = 4
STAGES = ((0, 1), (2, 4), (3, 5, 6, 7))


def flip_bits(a, k):
    for bit in (1, 2):
        if k & bit:
            a = a + bit - 2 * bit * lax.rem(lax.div(a, bit), 2)
    return a


def peer(m, v, k, n_vocab):
    return flip_bits(m, k // n_vocab), flip_bits(v, k % n_vocab)


def entry_barrier(n, n_vocab, m, v):
    barrier = pltpu.get_barrier_semaphore()
    for k in range(1, n):
        pm, pv = peer(m, v, k, n_vocab)
        pl.semaphore_signal(barrier, inc=1, device_id={"model": pm, "vocab": pv}, device_id_type=MESH)
    return barrier


def route_kernel(shard_len, n, n_vocab, ids_ref, valid_ref, tgt_ref, h_ref, tbl_ref, meta_ref, h1_ref, hin_ref, t_ref, send_ref, tin_ref, tsend, trecv, hsend, hrecv):
    rows, length = ids_ref.shape
    m, v = lax.axis_index("model"), lax.axis_index("vocab")
    me = m * n_vocab + v
    barrier = entry_barrier(n, n_vocab, m, v)

    ids = ids_ref[...]
    ok = valid_ref[...] > 0
    owner = jnp.where(ok, lax.div(ids, shard_len), n)
    off = lax.rem(ids, shard_len)
    tri = (lax.broadcasted_iota(jnp.int32, (length, length), 0)
           < lax.broadcasted_iota(jnp.int32, (length, length), 1)).astype(jnp.bfloat16)
    rank = jnp.zeros((rows, length), jnp.float32)
    for s in range(n):
        hit = owner == s
        count = jnp.dot(jnp.where(hit, 1.0, 0.0).astype(jnp.bfloat16), tri, preferred_element_type=jnp.float32)
        rank = rank + jnp.where(hit, count, 0.0)
    rank = rank.astype(jnp.int32)
    slot = jnp.where(ok, owner * CAP + rank, n * CAP)
    pair = off - lax.rem(off, 2)

    lane = lax.broadcasted_iota(jnp.int32, (rows, n * CAP), 1)
    row = lax.broadcasted_iota(jnp.int32, (rows, n * CAP), 0)
    spread = lax.rem(((me * rows + row) * CAP + lax.rem(lane, CAP)) * 4, shard_len)
    table = spread
    for j in range(length):
        table = jnp.where(lane == slot[:, j:j + 1], pair[:, j:j + 1], table)
    t_ref[...] = table

    groups = 128 // CAP
    per = rows // groups
    lane4 = lax.broadcasted_iota(jnp.int32, (per, 128), 1)
    parts = [jnp.zeros((per, 128), jnp.int32) for _ in range(n)]
    for q in range(groups):
        tq = t_ref[pl.ds(q, per, stride=groups), :]
        inside = lax.div(lane4, CAP) == q
        for s in range(n):
            moved = tq if q == s else pltpu.roll(tq, ((q - s) * CAP) % 128, axis=1)
            parts[s] = jnp.where(inside, moved, parts[s])
    for s in range(n):
        send_ref[s] = parts[s]

    code = lax.div(rank, 4) * (n * 8) + owner * 8 + lax.rem(rank, 4) * 2 + lax.rem(off, 2)
    diag = (lax.broadcasted_iota(jnp.int32, (rows, rows), 0) == lax.broadcasted_iota(jnp.int32, (rows, rows), 1))
    tcol = jnp.sum(jnp.where(diag, tgt_ref[...].reshape(1, rows), 0).astype(jnp.float32), axis=1, keepdims=True)
    meta_ref[:, :length] = jnp.where(ok, code, -1)
    meta_ref[:, length:] = jnp.broadcast_to(tcol.astype(jnp.int32), (rows, length))

    pl.semaphore_wait(barrier, n - 1)
    copies = []
    for k in range(1, n):
        pm, pv = peer(m, v, k, n_vocab)
        c = pltpu.make_async_remote_copy(
            src_ref=send_ref.at[pm * n_vocab + pv], dst_ref=tin_ref.at[k], send_sem=tsend.at[k], recv_sem=trecv.at[k],
            device_id={"model": pm, "vocab": pv}, device_id_type=MESH)
        c.start()
        copies.append(c)
    pm, pv = peer(m, v, 1, n_vocab)
    hcopy = pltpu.make_async_remote_copy(
        src_ref=h_ref, dst_ref=hin_ref, send_sem=hsend, recv_sem=hrecv,
        device_id={"model": pm, "vocab": pv}, device_id_type=MESH)
    hcopy.start()
    tbl_ref[0] = send_ref[me]
    for k in range(1, n):
        copies[k - 1].wait_recv()
        tbl_ref[k] = tin_ref[k]
    hcopy.wait_recv()
    h1_ref[...] = hin_ref[...]
    hcopy.wait_send()
    for c in copies:
        c.wait_send()


def score_kernel(blocks, *refs):
    nb = len(blocks)
    tbl_ref, w_hbm, h_refs, out_ref = refs[0], refs[1], refs[2:2 + nb], refs[2 + nb]
    bufs = refs[3 + nb:3 + nb + DEPTH]
    res_ref, hf_ref, sems, osem = refs[3 + nb + DEPTH:]
    tiles = w_hbm.shape[1]
    nrow = SLOTS // CAP
    quads = CAP // 4
    per = h_refs[0].shape[0] // nrow
    chunks = nb * per

    def table_row(c):
        if isinstance(c, int):
            return blocks[c // per] * per + c % per
        i = lax.div(c, per)
        blk = jnp.int32(blocks[0])
        for z in range(1, nb):
            blk = jnp.where(i == z, blocks[z], blk)
        return blk * per + lax.rem(c, per)

    def issue(r, b, k):
        at = tbl_ref[r, k]
        t, p = lax.shift_right_logical(at, 3), lax.bitwise_and(lax.shift_right_logical(at, 1), 3)
        pltpu.make_async_copy(
            w_hbm.at[t, :, p], bufs[b].at[k // 4, :, pl.ds(2 * (k % 4), 2), :], sems.at[b]).start(priority=k % 2)

    lane = lax.broadcasted_iota(jnp.int32, (8, 128), 1)

    def work(c, b, more):
        ahead = table_row(c + DEPTH - 1) if more else None
        pltpu.make_async_copy(bufs[b], bufs[b], sems.at[b]).wait()
        flat = bufs[b].reshape(SLOTS // 4 * tiles * 8, 128)
        blk, part = lax.div(c, per), lax.rem(c, per)
        for z in range(nb):
            @pl.when(blk == z)
            def _():
                hf_ref[...] = h_refs[z][pl.ds(pl.multiple_of(part * nrow, nrow), nrow), :].astype(jnp.float32)
        got = jnp.zeros((8, 128), jnp.float32)
        base = part * (SLOTS // 4)
        for i in range(nrow):
            acc = [[jnp.zeros((8, 128), jnp.float32)] * 2 for _ in range(quads)]
            for kk in range(0, tiles, 2):
                if more:
                    for k in range(-(-kk * CAP // tiles), -(-(kk + 2) * CAP // tiles)):
                        issue(ahead, (b + DEPTH - 1) % DEPTH, i * CAP + k)
                hb = [jnp.broadcast_to(hf_ref[i:i + 1, (kk + z) * 128:(kk + z + 1) * 128], (8, 128)) for z in (0, 1)]
                for g in range(quads):
                    at = ((i * quads + g) * tiles + kk) * 8
                    x = flat[at:at + 16, :].astype(jnp.float32)
                    acc[g] = [acc[g][0] + x[:8] * hb[0], acc[g][1] + x[8:] * hb[1]]
            for g in range(quads):
                total = jnp.sum(acc[g][0] + acc[g][1], axis=1, keepdims=True)
                got = jnp.where(lane == base + (i * quads + g), total, got)
        fresh = (lane >= base) & (lane < base + SLOTS // 4)
        res_ref[blk] = jnp.where(fresh, got, res_ref[blk])

    for c in range(DEPTH - 1):
        for k in range(SLOTS):
            issue(table_row(c), c, k)

    def step(g, _):
        for b in range(DEPTH):
            work(g * DEPTH + b, b, True)
        return 0

    lax.fori_loop(0, chunks // DEPTH - 1, step, 0)
    for b in range(DEPTH):
        work(jnp.int32(chunks - DEPTH + b), b, b == 0)
    done = pltpu.make_async_copy(res_ref, out_ref, osem)
    done.start()
    done.wait()


def return_kernel(n, n_vocab, *refs):
    ns = len(STAGES)
    scs, out_ref, inb, ssend, srecv = refs[:ns], refs[ns], refs[ns + 1], refs[ns + 2], refs[ns + 3]
    m, v = lax.axis_index("model"), lax.axis_index("vocab")
    me = m * n_vocab + v
    barrier = entry_barrier(n, n_vocab, m, v)
    pl.semaphore_wait(barrier, n - 1)
    copies = []
    for sc, blocks in zip(scs, STAGES):
        for i, k in enumerate(blocks):
            if k == 0:
                out_ref[me] = sc[i]
                continue
            pm, pv = peer(m, v, k, n_vocab)
            c = pltpu.make_async_remote_copy(
                src_ref=sc.at[i], dst_ref=inb.at[k], send_sem=ssend.at[k], recv_sem=srecv.at[k],
                device_id={"model": pm, "vocab": pv}, device_id_type=MESH)
            c.start()
            copies.append((k, c))
    for k, c in copies:
        c.wait_recv()
        pm, pv = peer(m, v, k, n_vocab)
        out_ref[pm * n_vocab + pv] = inb[k]
    for k, c in copies:
        c.wait_send()


def softmax_kernel(sc_ref, meta_ref, p_ref, lp_ref, flip):
    n = sc_ref.shape[0]
    rows, length = p_ref.shape
    flip[...] = sc_ref[...].reshape(n * 8, 128).T
    wide = [jnp.concatenate([flip[pl.ds(q, rows, stride=4), :] for q in (2 * hb, 2 * hb + 1)], axis=1) for hb in (0, 1)]
    meta = meta_ref[...]
    code = meta[:, :length]
    ok = code >= 0
    full = jnp.concatenate([jnp.where(ok, code, 0), jnp.zeros((rows, 128 - length), jnp.int32)], axis=1)
    low = jnp.take_along_axis(wide[0], lax.rem(full, 128), axis=1)
    high = jnp.take_along_axis(wide[1], lax.rem(full, 128), axis=1)
    scores = jnp.where(full < 128, low, high)[:, :length] / TEMP
    scores = jnp.where(ok, scores, -jnp.inf)
    top = jnp.max(scores, axis=1, keepdims=True)
    log_norm = top + jnp.log(jnp.sum(jnp.exp(scores - top), axis=1, keepdims=True))
    p_ref[...] = jnp.where(ok, jnp.exp(scores - log_norm), 0.0)
    at = lax.broadcasted_iota(jnp.int32, (rows, length), 1)
    picked = jnp.sum(jnp.where(at == meta[:, length:], scores, 0.0), axis=1, keepdims=True)
    diag = (lax.broadcasted_iota(jnp.int32, (rows, rows), 0) == lax.broadcasted_iota(jnp.int32, (rows, rows), 1))
    lp_ref[...] = jnp.sum(jnp.where(diag, picked - log_norm, 0.0), axis=0)


def solution(mesh):
    axes = ("model", "vocab")
    n_model, n_vocab = mesh.shape["model"], mesh.shape["vocab"]
    n = n_model * n_vocab
    row_spec = P(("rep",) + axes, None)
    vec_spec = P(("rep",) + axes)
    vmem = pl.BlockSpec(memory_space=pltpu.VMEM)
    hbm = pl.BlockSpec(memory_space=pl.ANY)
    smem = pl.BlockSpec(memory_space=pltpu.SMEM)

    def local_step(hidden, head_rows, allowed_ids, valid_mask, target_pos):
        rows, length = allowed_ids.shape
        shard_len, width = head_rows.shape
        per = rows * CAP // 128
        tiles = width // 128

        def exchange(x, k):
            return lax.ppermute(x, axes, [(s, s ^ k) for s in range(n)])

        tbl, meta, beside = pl.pallas_call(
            functools.partial(route_kernel, shard_len, n, n_vocab),
            out_shape=(jax.ShapeDtypeStruct((n, per, 128), jnp.int32),
                       jax.ShapeDtypeStruct((rows, 2 * length), jnp.int32),
                       jax.ShapeDtypeStruct((rows, width), jnp.bfloat16)),
            in_specs=[vmem, vmem, vmem, vmem],
            out_specs=(vmem, vmem, vmem),
            scratch_shapes=[
                pltpu.VMEM((rows, width), jnp.bfloat16),
                pltpu.VMEM((rows, n * CAP), jnp.int32),
                pltpu.VMEM((n, per, 128), jnp.int32),
                pltpu.VMEM((n, per, 128), jnp.int32),
                pltpu.SemaphoreType.DMA((n,)),
                pltpu.SemaphoreType.DMA((n,)),
                pltpu.SemaphoreType.DMA,
                pltpu.SemaphoreType.DMA,
            ],
            compiler_params=pltpu.CompilerParams(collective_id=0, has_side_effects=True),
            cost_estimate=pl.CostEstimate(flops=10_000_000, bytes_accessed=10_000, transcendentals=0),
            name="route",
        )(allowed_ids, valid_mask, target_pos, hidden)
        hidden_after, tbl = lax.optimization_barrier((hidden, tbl))
        blocks = {0: hidden, 1: beside, **{k: exchange(hidden_after, k) for k in (2, 4, 6)}}
        pairs = head_rows.reshape(shard_len // 8, 4, 2, tiles, 128).transpose(0, 3, 1, 2, 4)
        scores = []
        for stage in STAGES:
            nb = len(stage)
            if len(scores) == 1:
                blocks[2], blocks[4], scores[0] = lax.optimization_barrier((blocks[2], blocks[4], scores[0]))
                blocks[3], blocks[5] = exchange(blocks[2], 1), exchange(blocks[4], 1)
            if len(scores) == 2:
                blocks[6], scores[1] = lax.optimization_barrier((blocks[6], scores[1]))
                blocks[7] = exchange(blocks[6], 1)
            scores.append(pl.pallas_call(
                functools.partial(score_kernel, stage),
                out_shape=jax.ShapeDtypeStruct((nb, 8, 128), jnp.float32),
                in_specs=[smem, hbm] + [vmem] * nb,
                out_specs=pl.BlockSpec(memory_space=pltpu.HBM),
                scratch_shapes=[
                    *[pltpu.VMEM((SLOTS // 4, tiles, 8, 128), jnp.bfloat16)] * DEPTH,
                    pltpu.VMEM((nb, 8, 128), jnp.float32),
                    pltpu.VMEM((SLOTS // CAP, width), jnp.float32),
                    pltpu.SemaphoreType.DMA((DEPTH,)),
                    pltpu.SemaphoreType.DMA,
                ],
                compiler_params=pltpu.CompilerParams(vmem_limit_bytes=24 * 1024 * 1024),
                cost_estimate=pl.CostEstimate(flops=20_000_000 * nb, bytes_accessed=nb * 10_000_000, transcendentals=0),
                name=f"score{stage[0]}",
            )(tbl.reshape(n * per, 128), pairs, *[blocks[k] for k in stage]))
        back = pl.pallas_call(
            functools.partial(return_kernel, n, n_vocab),
            out_shape=jax.ShapeDtypeStruct((n, 8, 128), jnp.float32),
            in_specs=[vmem] * len(STAGES),
            out_specs=vmem,
            scratch_shapes=[
                pltpu.VMEM((n, 8, 128), jnp.float32),
                pltpu.SemaphoreType.DMA((n,)),
                pltpu.SemaphoreType.DMA((n,)),
            ],
            compiler_params=pltpu.CompilerParams(collective_id=1, has_side_effects=True),
            name="giveback",
        )(*scores)
        return pl.pallas_call(
            softmax_kernel,
            out_shape=(jax.ShapeDtypeStruct((rows, length), jnp.float32), jax.ShapeDtypeStruct((rows,), jnp.float32)),
            in_specs=[vmem, vmem],
            out_specs=(vmem, vmem),
            scratch_shapes=[pltpu.VMEM((128, n * 8), jnp.float32)],
            name="finish",
        )(back, meta)

    return jax.shard_map(local_step, mesh=mesh, in_specs=(row_spec, P(axes, None), row_spec, row_spec, vec_spec),
                         out_specs=(row_spec, vec_spec), check_vma=False)
```

```python
import functools

import jax
import jax.numpy as jnp
from jax import lax
from jax.experimental import pallas as pl
from jax.experimental.pallas import tpu as pltpu
from jax.sharding import PartitionSpec as P

MESH = pl.DeviceIdType.MESH
TEMP = 0.5
CAP = 16
SLOTS = 128
DEPTH = 4


def flip_bits(a, k):
    for bit in (1, 2):
        if k & bit:
            a = a + bit - 2 * bit * lax.rem(lax.div(a, bit), 2)
    return a


def peer(m, v, k, n_vocab):
    return flip_bits(m, k // n_vocab), flip_bits(v, k % n_vocab)


def entry_barrier(n, n_vocab, m, v):
    barrier = pltpu.get_barrier_semaphore()
    for k in range(1, n):
        pm, pv = peer(m, v, k, n_vocab)
        pl.semaphore_signal(barrier, inc=1, device_id={"model": pm, "vocab": pv}, device_id_type=MESH)
    return barrier


def route_kernel(shard_len, n, n_vocab, ids_hbm, valid_hbm, tgt_hbm, h_hbm, tbl_out, meta_out, hall_out,
                 ids_ref, valid_ref, tgt_ref, meta_ref, t_ref, send_ref, tin_ref, hbuf, tsend, trecv, hsend, hrecv, lsem, osem):
    rows, length = ids_ref.shape
    m, v = lax.axis_index("model"), lax.axis_index("vocab")
    me = m * n_vocab + v
    barrier = entry_barrier(n, n_vocab, m, v)
    loads = [pltpu.make_async_copy(src, dst, lsem.at[i]) for i, (src, dst) in enumerate(
        ((h_hbm, hbuf.at[0]), (ids_hbm, ids_ref), (valid_hbm, valid_ref), (tgt_hbm, tgt_ref)))]
    for c in loads:
        c.start()

    half = rows // 2
    lo, hi, every = pl.ds(0, half), pl.ds(half, half), pl.ds(0, rows)
    sends = []

    def send(src, dst, part, to):
        pm, pv = peer(m, v, to, n_vocab)
        i = len(sends)
        sends.append(pltpu.make_async_remote_copy(
            src_ref=hbuf.at[src, part], dst_ref=hbuf.at[dst, part], send_sem=hsend.at[i], recv_sem=hrecv.at[i],
            device_id={"model": pm, "vocab": pv}, device_id_type=MESH))
        return sends[-1]

    own_x = [send(0, 2, lo, 2), send(0, 2, hi, 2)]
    own_y = [send(0, 4, lo, 4), send(0, 4, hi, 4)]
    own_p = send(0, 1, every, 1)
    x_to_y, y_to_x = send(2, 6, lo, 4), send(4, 6, hi, 2)
    x_p = [send(2, 3, lo, 1), send(2, 3, hi, 1)]
    y_p = [send(4, 5, lo, 1), send(4, 5, hi, 1)]
    d_p = [send(6, 7, lo, 1), send(6, 7, hi, 1)]

    loads[0].wait()
    pl.semaphore_wait(barrier, n - 1)
    for c in (own_x[0], own_y[1], own_p, own_x[1], own_y[0]):
        c.start()
    outs = []

    def keep(src, dst):
        outs.append(pltpu.make_async_copy(src, dst, osem.at[len(outs)]))
        outs[-1].start()

    keep(hbuf.at[0], hall_out.at[0])
    for c in loads[1:]:
        c.wait()

    ids = ids_ref[...]
    ok = valid_ref[...] > 0
    owner = jnp.where(ok, lax.div(ids, shard_len), n)
    off = lax.rem(ids, shard_len)
    tri = (lax.broadcasted_iota(jnp.int32, (length, length), 0)
           < lax.broadcasted_iota(jnp.int32, (length, length), 1)).astype(jnp.bfloat16)
    rank = jnp.zeros((rows, length), jnp.float32)
    for s in range(n):
        hit = owner == s
        count = jnp.dot(jnp.where(hit, 1.0, 0.0).astype(jnp.bfloat16), tri, preferred_element_type=jnp.float32)
        rank = rank + jnp.where(hit, count, 0.0)
    rank = rank.astype(jnp.int32)
    slot = jnp.where(ok, owner * CAP + rank, n * CAP)
    pair = off - lax.rem(off, 2)

    lane = lax.broadcasted_iota(jnp.int32, (rows, n * CAP), 1)
    row = lax.broadcasted_iota(jnp.int32, (rows, n * CAP), 0)
    spread = lax.rem(((me * rows + row) * CAP + lax.rem(lane, CAP)) * 4, shard_len)
    table = spread
    for j in range(length):
        table = jnp.where(lane == slot[:, j:j + 1], pair[:, j:j + 1], table)
    t_ref[...] = table

    groups = 128 // CAP
    per = rows // groups
    lane4 = lax.broadcasted_iota(jnp.int32, (per, 128), 1)
    parts = [jnp.zeros((per, 128), jnp.int32) for _ in range(n)]
    for q in range(groups):
        tq = t_ref[pl.ds(q, per, stride=groups), :]
        inside = lax.div(lane4, CAP) == q
        for s in range(n):
            moved = tq if q == s else pltpu.roll(tq, ((q - s) * CAP) % 128, axis=1)
            parts[s] = jnp.where(inside, moved, parts[s])
    for s in range(n):
        send_ref[s] = parts[s]

    code = lax.div(rank, 4) * (n * 8) + owner * 8 + lax.rem(rank, 4) * 2 + lax.rem(off, 2)
    diag = (lax.broadcasted_iota(jnp.int32, (rows, rows), 0) == lax.broadcasted_iota(jnp.int32, (rows, rows), 1))
    tcol = jnp.sum(jnp.where(diag, tgt_ref[...].reshape(1, rows), 0).astype(jnp.float32), axis=1, keepdims=True)
    meta_ref[:, :length] = jnp.where(ok, code, -1)
    meta_ref[:, length:] = jnp.broadcast_to(tcol.astype(jnp.int32), (rows, length))

    tin_ref[0] = send_ref[me]
    copies = []
    for k in range(1, n):
        pm, pv = peer(m, v, k, n_vocab)
        c = pltpu.make_async_remote_copy(
            src_ref=send_ref.at[pm * n_vocab + pv], dst_ref=tin_ref.at[k], send_sem=tsend.at[k], recv_sem=trecv.at[k],
            device_id={"model": pm, "vocab": pv}, device_id_type=MESH)
        c.start()
        copies.append(c)

    own_x[0].wait_recv()
    x_to_y.start()
    x_p[0].start()
    own_y[1].wait_recv()
    y_to_x.start()
    y_p[1].start()
    keep(meta_ref, meta_out)
    own_p.wait_recv()
    keep(hbuf.at[1], hall_out.at[1])
    own_x[1].wait_recv()
    x_p[1].start()
    keep(hbuf.at[2], hall_out.at[2])
    own_y[0].wait_recv()
    y_p[0].start()
    keep(hbuf.at[4], hall_out.at[4])
    for c in copies:
        c.wait_recv()
    keep(tin_ref, tbl_out)
    for c in x_p:
        c.wait_recv()
    keep(hbuf.at[3], hall_out.at[3])
    for c in y_p:
        c.wait_recv()
    keep(hbuf.at[5], hall_out.at[5])
    x_to_y.wait_recv()
    d_p[0].start()
    keep(hbuf.at[6, lo], hall_out.at[6, lo])
    y_to_x.wait_recv()
    d_p[1].start()
    keep(hbuf.at[6, hi], hall_out.at[6, hi])
    d_p[0].wait_recv()
    keep(hbuf.at[7, lo], hall_out.at[7, lo])
    d_p[1].wait_recv()
    keep(hbuf.at[7, hi], hall_out.at[7, hi])
    for c in sends + copies:
        c.wait_send()
    for c in outs:
        c.wait()


def score_kernel(tbl_ref, w_hbm, h_hbm, out_ref, *scratch):
    bufs = scratch[:DEPTH]
    h_ref, hf_ref, sems, hsem = scratch[DEPTH:]
    tiles = w_hbm.shape[1]
    nrow = SLOTS // CAP
    quads = CAP // 4
    chunks = tbl_ref.shape[0]
    per = chunks // out_ref.shape[0]

    def issue(r, b, k):
        at = tbl_ref[r, k]
        t, p = lax.shift_right_logical(at, 3), lax.bitwise_and(lax.shift_right_logical(at, 1), 3)
        pltpu.make_async_copy(
            w_hbm.at[t, :, p], bufs[b].at[k // 4, :, pl.ds(2 * (k % 4), 2), :], sems.at[b]).start(priority=k % 2)

    lane = lax.broadcasted_iota(jnp.int32, (8, 128), 1)

    def work(c, b, more):
        ahead = c + DEPTH - 1
        pltpu.make_async_copy(bufs[b], bufs[b], sems.at[b]).wait()
        flat = bufs[b].reshape(SLOTS // 4 * tiles * 8, 128)
        blk, part = lax.div(c, per), lax.rem(c, per)
        hf_ref[...] = h_ref[c].astype(jnp.float32)
        got = jnp.zeros((8, 128), jnp.float32)
        base = part * (SLOTS // 4)
        for i in range(nrow):
            acc = [[jnp.zeros((8, 128), jnp.float32)] * 2 for _ in range(quads)]
            for kk in range(0, tiles, 2):
                if more:
                    for k in range(-(-kk * CAP // tiles), -(-(kk + 2) * CAP // tiles)):
                        issue(ahead, (b + DEPTH - 1) % DEPTH, i * CAP + k)
                hb = [jnp.broadcast_to(hf_ref[i:i + 1, (kk + z) * 128:(kk + z + 1) * 128], (8, 128)) for z in (0, 1)]
                for g in range(quads):
                    at = ((i * quads + g) * tiles + kk) * 8
                    x = flat[at:at + 16, :].astype(jnp.float32)
                    acc[g] = [acc[g][0] + x[:8] * hb[0], acc[g][1] + x[8:] * hb[1]]
            for g in range(quads):
                total = jnp.sum(acc[g][0] + acc[g][1], axis=1, keepdims=True)
                got = jnp.where(lane == base + (i * quads + g), total, got)
        fresh = (lane >= base) & (lane < base + SLOTS // 4)
        out_ref[blk] = jnp.where(fresh, got, out_ref[blk])

    for k in range(SLOTS):
        issue(0, 0, k)
    hcopy = pltpu.make_async_copy(h_hbm, h_ref, hsem)
    hcopy.start()
    for c in range(1, DEPTH - 1):
        for k in range(SLOTS):
            issue(c, c, k)
    hcopy.wait()

    def step(g, _):
        for b in range(DEPTH):
            work(g * DEPTH + b, b, True)
        return 0

    lax.fori_loop(0, chunks // DEPTH - 1, step, 0)
    for b in range(DEPTH):
        work(jnp.int32(chunks - DEPTH + b), b, b == 0)


def return_kernel(n, n_vocab, sc_hbm, out_hbm, sc_ref, lsem, ssend, srecv):
    m, v = lax.axis_index("model"), lax.axis_index("vocab")
    me = m * n_vocab + v
    barrier = entry_barrier(n, n_vocab, m, v)
    load = pltpu.make_async_copy(sc_hbm, sc_ref, lsem.at[0])
    load.start()
    load.wait()
    pl.semaphore_wait(barrier, n - 1)
    copies = []
    for k in range(1, n):
        pm, pv = peer(m, v, k, n_vocab)
        c = pltpu.make_async_remote_copy(
            src_ref=sc_ref.at[k], dst_ref=out_hbm.at[me], send_sem=ssend.at[k], recv_sem=srecv.at[k],
            device_id={"model": pm, "vocab": pv}, device_id_type=MESH)
        c.start()
        copies.append(c)
    own = pltpu.make_async_copy(sc_ref.at[0], out_hbm.at[me], lsem.at[1])
    own.start()
    for c in copies:
        c.wait_recv()
    for c in copies:
        c.wait_send()
    own.wait()


def softmax_kernel(sc_ref, meta_ref, p_ref, lp_ref, flip):
    n = sc_ref.shape[0]
    rows, length = p_ref.shape
    flip[...] = sc_ref[...].reshape(n * 8, 128).T
    wide = [jnp.concatenate([flip[pl.ds(q, rows, stride=4), :] for q in (2 * hb, 2 * hb + 1)], axis=1) for hb in (0, 1)]
    meta = meta_ref[...]
    code = meta[:, :length]
    ok = code >= 0
    full = jnp.concatenate([jnp.where(ok, code, 0), jnp.zeros((rows, 128 - length), jnp.int32)], axis=1)
    low = jnp.take_along_axis(wide[0], lax.rem(full, 128), axis=1)
    high = jnp.take_along_axis(wide[1], lax.rem(full, 128), axis=1)
    scores = jnp.where(full < 128, low, high)[:, :length] / TEMP
    scores = jnp.where(ok, scores, -jnp.inf)
    top = jnp.max(scores, axis=1, keepdims=True)
    log_norm = top + jnp.log(jnp.sum(jnp.exp(scores - top), axis=1, keepdims=True))
    p_ref[...] = jnp.where(ok, jnp.exp(scores - log_norm), 0.0)
    at = lax.broadcasted_iota(jnp.int32, (rows, length), 1)
    picked = jnp.sum(jnp.where(at == meta[:, length:], scores, 0.0), axis=1, keepdims=True)
    diag = (lax.broadcasted_iota(jnp.int32, (rows, rows), 0) == lax.broadcasted_iota(jnp.int32, (rows, rows), 1))
    lp_ref[...] = jnp.sum(jnp.where(diag, picked - log_norm, 0.0), axis=0)


def solution(mesh):
    axes = ("model", "vocab")
    n_model, n_vocab = mesh.shape["model"], mesh.shape["vocab"]
    n = n_model * n_vocab
    row_spec = P(("rep",) + axes, None)
    vec_spec = P(("rep",) + axes)
    vmem = pl.BlockSpec(memory_space=pltpu.VMEM)
    hbm = pl.BlockSpec(memory_space=pl.ANY)
    smem = pl.BlockSpec(memory_space=pltpu.SMEM)

    def local_step(hidden, head_rows, allowed_ids, valid_mask, target_pos):
        rows, length = allowed_ids.shape
        shard_len, width = head_rows.shape
        per = rows * CAP // 128
        tiles = width // 128

        chunks = n * rows * CAP // SLOTS
        tbl, meta, hall = pl.pallas_call(
            functools.partial(route_kernel, shard_len, n, n_vocab),
            out_shape=(jax.ShapeDtypeStruct((n, per, 128), jnp.int32),
                       jax.ShapeDtypeStruct((rows, 2 * length), jnp.int32),
                       jax.ShapeDtypeStruct((n, rows, width), jnp.bfloat16)),
            in_specs=[hbm] * 4,
            out_specs=(hbm, hbm, hbm),
            scratch_shapes=[
                pltpu.VMEM((rows, length), jnp.int32),
                pltpu.VMEM((rows, length), jnp.int32),
                pltpu.VMEM((rows,), jnp.int32),
                pltpu.VMEM((rows, 2 * length), jnp.int32),
                pltpu.VMEM((rows, n * CAP), jnp.int32),
                pltpu.VMEM((n, per, 128), jnp.int32),
                pltpu.VMEM((n, per, 128), jnp.int32),
                pltpu.VMEM((n, rows, width), jnp.bfloat16),
                pltpu.SemaphoreType.DMA((n,)),
                pltpu.SemaphoreType.DMA((n,)),
                pltpu.SemaphoreType.DMA((13,)),
                pltpu.SemaphoreType.DMA((13,)),
                pltpu.SemaphoreType.DMA((4,)),
                pltpu.SemaphoreType.DMA((12,)),
            ],
            compiler_params=pltpu.CompilerParams(collective_id=0, has_side_effects=True),
            name="route",
        )(allowed_ids, valid_mask, target_pos, hidden)
        pairs = head_rows.reshape(shard_len // 8, 4, 2, tiles, 128).transpose(0, 3, 1, 2, 4)
        scores = pl.pallas_call(
            score_kernel,
            out_shape=jax.ShapeDtypeStruct((n, 8, 128), jnp.float32),
            in_specs=[smem, hbm, hbm],
            out_specs=vmem,
            scratch_shapes=[
                *[pltpu.VMEM((SLOTS // 4, tiles, 8, 128), jnp.bfloat16)] * DEPTH,
                pltpu.VMEM((chunks, SLOTS // CAP, width), jnp.bfloat16),
                pltpu.VMEM((SLOTS // CAP, width), jnp.float32),
                pltpu.SemaphoreType.DMA((DEPTH,)),
                pltpu.SemaphoreType.DMA,
            ],
            compiler_params=pltpu.CompilerParams(vmem_limit_bytes=67_000_000),
            name="score",
        )(tbl.reshape(n * per, 128), pairs, hall.reshape(chunks, SLOTS // CAP, width))
        back = pl.pallas_call(
            functools.partial(return_kernel, n, n_vocab),
            out_shape=jax.ShapeDtypeStruct((n, 8, 128), jnp.float32),
            in_specs=[hbm],
            out_specs=hbm,
            scratch_shapes=[
                pltpu.VMEM((n, 8, 128), jnp.float32),
                pltpu.SemaphoreType.DMA((2,)),
                pltpu.SemaphoreType.DMA((n,)),
                pltpu.SemaphoreType.DMA((n,)),
            ],
            compiler_params=pltpu.CompilerParams(collective_id=1, has_side_effects=True),
            name="giveback",
        )(scores)
        return pl.pallas_call(
            softmax_kernel,
            out_shape=(jax.ShapeDtypeStruct((rows, length), jnp.float32), jax.ShapeDtypeStruct((rows,), jnp.float32)),
            in_specs=[vmem, vmem],
            out_specs=(vmem, vmem),
            scratch_shapes=[pltpu.VMEM((128, n * 8), jnp.float32)],
            name="finish",
        )(back, meta)

    return jax.shard_map(local_step, mesh=mesh, in_specs=(row_spec, P(axes, None), row_spec, row_spec, vec_spec),
                         out_specs=(row_spec, vec_spec), check_vma=False)
```

```python
import functools

import jax
import jax.numpy as jnp
from jax import lax
from jax.experimental import pallas as pl
from jax.experimental.pallas import tpu as pltpu
from jax.sharding import PartitionSpec as P

MESH = pl.DeviceIdType.MESH
TEMP = 0.5
CAP = 16
SLOTS = 128
DEPTH = 4
WAITS = 4


def flip_bits(a, k):
    for bit in (1, 2):
        if k & bit:
            a = a + bit - 2 * bit * lax.rem(lax.div(a, bit), 2)
    return a


def peer(m, v, k, n_vocab):
    return flip_bits(m, k // n_vocab), flip_bits(v, k % n_vocab)


def entry_barrier(n, n_vocab, m, v):
    barrier = pltpu.get_barrier_semaphore()
    for k in range(1, n):
        pm, pv = peer(m, v, k, n_vocab)
        pl.semaphore_signal(barrier, inc=1, device_id={"model": pm, "vocab": pv}, device_id_type=MESH)
    return barrier


def route_kernel(shard_len, n, n_vocab, ids_hbm, valid_hbm, tgt_hbm, h_hbm, tbl_out, meta_out, hall_out,
                 ids_ref, valid_ref, tgt_ref, meta_ref, t_ref, send_ref, tin_ref, hbuf, tsend, trecv, hsend, hrecv, lsem, osem):
    rows, length = ids_ref.shape
    m, v = lax.axis_index("model"), lax.axis_index("vocab")
    me = m * n_vocab + v
    barrier = entry_barrier(n, n_vocab, m, v)
    loads = [pltpu.make_async_copy(src, dst, lsem.at[i]) for i, (src, dst) in enumerate(
        ((h_hbm, hbuf.at[0]), (ids_hbm, ids_ref), (valid_hbm, valid_ref), (tgt_hbm, tgt_ref)))]
    for c in loads:
        c.start()

    half = rows // 2
    lo, hi, every = pl.ds(0, half), pl.ds(half, half), pl.ds(0, rows)
    sends = []

    def send(src, dst, part, to):
        pm, pv = peer(m, v, to, n_vocab)
        i = len(sends)
        sends.append(pltpu.make_async_remote_copy(
            src_ref=hbuf.at[src, part], dst_ref=(hall_out if to == 1 else hbuf).at[dst, part], send_sem=hsend.at[i], recv_sem=hrecv.at[i],
            device_id={"model": pm, "vocab": pv}, device_id_type=MESH))
        return sends[-1]

    own_x = [send(0, 2, lo, 2), send(0, 2, hi, 2)]
    own_y = [send(0, 4, lo, 4), send(0, 4, hi, 4)]
    own_p = send(0, 1, every, 1)
    x_to_y, y_to_x = send(2, 6, lo, 4), send(4, 6, hi, 2)
    x_p = [send(2, 3, lo, 1), send(2, 3, hi, 1)]
    y_p = [send(4, 5, lo, 1), send(4, 5, hi, 1)]
    d_p = [send(6, 7, lo, 1), send(6, 7, hi, 1)]

    loads[0].wait()
    pl.semaphore_wait(barrier, n - 1)
    for c in (own_x[0], own_y[1], own_p, own_x[1], own_y[0]):
        c.start()
    outs = []

    def keep(src, dst):
        outs.append(pltpu.make_async_copy(src, dst, osem.at[len(outs)]))
        outs[-1].start()

    keep(hbuf.at[0], hall_out.at[0])
    for c in loads[1:]:
        c.wait()

    ids = ids_ref[...]
    ok = valid_ref[...] > 0
    owner = jnp.where(ok, lax.div(ids, shard_len), n)
    off = lax.rem(ids, shard_len)
    tri = (lax.broadcasted_iota(jnp.int32, (length, length), 0)
           < lax.broadcasted_iota(jnp.int32, (length, length), 1)).astype(jnp.bfloat16)
    rank = jnp.zeros((rows, length), jnp.float32)
    for s in range(n):
        hit = owner == s
        count = jnp.dot(jnp.where(hit, 1.0, 0.0).astype(jnp.bfloat16), tri, preferred_element_type=jnp.float32)
        rank = rank + jnp.where(hit, count, 0.0)
    rank = rank.astype(jnp.int32)
    slot = jnp.where(ok, owner * CAP + rank, n * CAP)
    pair = off - lax.rem(off, 2)

    lane = lax.broadcasted_iota(jnp.int32, (rows, n * CAP), 1)
    row = lax.broadcasted_iota(jnp.int32, (rows, n * CAP), 0)
    spread = lax.rem(((me * rows + row) * CAP + lax.rem(lane, CAP)) * 4, shard_len)
    table = spread
    for j in range(length):
        table = jnp.where(lane == slot[:, j:j + 1], pair[:, j:j + 1], table)
    t_ref[...] = table

    groups = 128 // CAP
    per = rows // groups
    lane4 = lax.broadcasted_iota(jnp.int32, (per, 128), 1)
    parts = [jnp.zeros((per, 128), jnp.int32) for _ in range(n)]
    for q in range(groups):
        tq = t_ref[pl.ds(q, per, stride=groups), :]
        inside = lax.div(lane4, CAP) == q
        for s in range(n):
            moved = tq if q == s else pltpu.roll(tq, ((q - s) * CAP) % 128, axis=1)
            parts[s] = jnp.where(inside, moved, parts[s])
    for s in range(n):
        send_ref[s] = parts[s]

    code = lax.div(rank, 4) * (n * 8) + owner * 8 + lax.rem(rank, 4) * 2 + lax.rem(off, 2)
    diag = (lax.broadcasted_iota(jnp.int32, (rows, rows), 0) == lax.broadcasted_iota(jnp.int32, (rows, rows), 1))
    tcol = jnp.sum(jnp.where(diag, tgt_ref[...].reshape(1, rows), 0).astype(jnp.float32), axis=1, keepdims=True)
    meta_ref[:, :length] = jnp.where(ok, code, -1)
    meta_ref[:, length:] = jnp.broadcast_to(tcol.astype(jnp.int32), (rows, length))

    tin_ref[0] = send_ref[me]
    copies = []
    for k in range(1, n):
        pm, pv = peer(m, v, k, n_vocab)
        c = pltpu.make_async_remote_copy(
            src_ref=send_ref.at[pm * n_vocab + pv], dst_ref=tin_ref.at[k], send_sem=tsend.at[k], recv_sem=trecv.at[k],
            device_id={"model": pm, "vocab": pv}, device_id_type=MESH)
        c.start()
        copies.append(c)

    own_x[0].wait_recv()
    x_to_y.start()
    x_p[0].start()
    own_y[1].wait_recv()
    y_to_x.start()
    y_p[1].start()
    keep(meta_ref, meta_out)
    own_x[1].wait_recv()
    x_p[1].start()
    keep(hbuf.at[2], hall_out.at[2])
    own_y[0].wait_recv()
    y_p[0].start()
    keep(hbuf.at[4], hall_out.at[4])
    for c in copies:
        c.wait_recv()
    keep(tin_ref, tbl_out)
    x_to_y.wait_recv()
    d_p[0].start()
    keep(hbuf.at[6, lo], hall_out.at[6, lo])
    y_to_x.wait_recv()
    d_p[1].start()
    keep(hbuf.at[6, hi], hall_out.at[6, hi])
    for c in [own_p] + x_p + y_p + d_p:
        c.wait_recv()
    for c in sends + copies:
        c.wait_send()
    for c in outs:
        c.wait()


def score_kernel(tbl_hbm, w_hbm, h_hbm, out_ref, *scratch):
    bufs = scratch[:DEPTH]
    tbl_ref, h_ref, hf_ref, sems, lsem = scratch[DEPTH:]
    tiles = w_hbm.shape[1]
    nrow = SLOTS // CAP
    quads = CAP // 4
    blocks, per, _ = tbl_ref.shape
    chunks = blocks * per

    loads = [pltpu.make_async_copy(tbl_hbm.at[0], tbl_ref.at[0], lsem.at[0]),
             pltpu.make_async_copy(tbl_hbm.at[pl.ds(1, blocks - 1)], tbl_ref.at[pl.ds(1, blocks - 1)], lsem.at[1]),
             pltpu.make_async_copy(h_hbm, h_ref, lsem.at[2])]
    for c in loads:
        c.start()

    def issue(r, b, k):
        at = tbl_ref[r // per, r % per, k] if isinstance(r, int) else tbl_ref[lax.div(r, per), lax.rem(r, per), k]
        t, p = lax.shift_right_logical(at, 3), lax.bitwise_and(lax.shift_right_logical(at, 1), 3)
        pltpu.make_async_copy(
            w_hbm.at[t, :, p], bufs[b].at[k // 4, :, pl.ds(2 * (k % 4), 2), :], sems.at[b, k * WAITS // SLOTS]).start(priority=k % 2)

    lane = lax.broadcasted_iota(jnp.int32, (8, 128), 1)

    def work(c, b, more):
        ahead = c + DEPTH - 1
        flat = bufs[b].reshape(SLOTS // 4 * tiles * 8, 128)
        blk, part = lax.div(c, per), lax.rem(c, per)
        hf_ref[...] = h_ref[c].astype(jnp.float32)
        got = jnp.zeros((8, 128), jnp.float32)
        base = part * (SLOTS // 4)
        for i in range(nrow):
            if i % (nrow // WAITS) == 0:
                w = i // (nrow // WAITS)
                piece = bufs[b].at[pl.ds(w * (SLOTS // 4 // WAITS), SLOTS // 4 // WAITS)]
                pltpu.make_async_copy(piece, piece, sems.at[b, w]).wait()
            acc = [[jnp.zeros((8, 128), jnp.float32)] * 2 for _ in range(quads)]
            for kk in range(0, tiles, 2):
                if more:
                    for k in range(-(-kk * CAP // tiles), -(-(kk + 2) * CAP // tiles)):
                        issue(ahead, (b + DEPTH - 1) % DEPTH, i * CAP + k)
                hb = [jnp.broadcast_to(hf_ref[i:i + 1, (kk + z) * 128:(kk + z + 1) * 128], (8, 128)) for z in (0, 1)]
                for g in range(quads):
                    at = ((i * quads + g) * tiles + kk) * 8
                    x = flat[at:at + 16, :].astype(jnp.float32)
                    acc[g] = [acc[g][0] + x[:8] * hb[0], acc[g][1] + x[8:] * hb[1]]
            for g in range(quads):
                total = jnp.sum(acc[g][0] + acc[g][1], axis=1, keepdims=True)
                got = jnp.where(lane == base + (i * quads + g), total, got)
        fresh = (lane >= base) & (lane < base + SLOTS // 4)
        out_ref[blk] = jnp.where(fresh, got, out_ref[blk])

    loads[0].wait()
    for c in range(DEPTH - 1):
        for k in range(SLOTS):
            issue(c, c, k)
    loads[1].wait()
    loads[2].wait()

    def step(g, _):
        for b in range(DEPTH):
            work(g * DEPTH + b, b, True)
        return 0

    lax.fori_loop(0, chunks // DEPTH - 1, step, 0)
    for b in range(DEPTH):
        work(jnp.int32(chunks - DEPTH + b), b, b == 0)


def return_kernel(n, n_vocab, sc_hbm, out_hbm, sc_ref, lsem, ssend, srecv):
    m, v = lax.axis_index("model"), lax.axis_index("vocab")
    me = m * n_vocab + v
    barrier = entry_barrier(n, n_vocab, m, v)
    load = pltpu.make_async_copy(sc_hbm, sc_ref, lsem.at[0])
    load.start()
    load.wait()
    pl.semaphore_wait(barrier, n - 1)
    copies = []
    for k in range(1, n):
        pm, pv = peer(m, v, k, n_vocab)
        c = pltpu.make_async_remote_copy(
            src_ref=sc_ref.at[k], dst_ref=out_hbm.at[me], send_sem=ssend.at[k], recv_sem=srecv.at[k],
            device_id={"model": pm, "vocab": pv}, device_id_type=MESH)
        c.start()
        copies.append(c)
    own = pltpu.make_async_copy(sc_ref.at[0], out_hbm.at[me], lsem.at[1])
    own.start()
    for c in copies:
        c.wait_recv()
    for c in copies:
        c.wait_send()
    own.wait()


def softmax_kernel(sc_ref, meta_ref, p_ref, lp_ref, flip):
    n = sc_ref.shape[0]
    rows, length = p_ref.shape
    flip[...] = sc_ref[...].reshape(n * 8, 128).T
    wide = [jnp.concatenate([flip[pl.ds(q, rows, stride=4), :] for q in (2 * hb, 2 * hb + 1)], axis=1) for hb in (0, 1)]
    meta = meta_ref[...]
    code = meta[:, :length]
    ok = code >= 0
    full = jnp.concatenate([jnp.where(ok, code, 0), jnp.zeros((rows, 128 - length), jnp.int32)], axis=1)
    low = jnp.take_along_axis(wide[0], lax.rem(full, 128), axis=1)
    high = jnp.take_along_axis(wide[1], lax.rem(full, 128), axis=1)
    scores = jnp.where(full < 128, low, high)[:, :length] / TEMP
    scores = jnp.where(ok, scores, -jnp.inf)
    top = jnp.max(scores, axis=1, keepdims=True)
    log_norm = top + jnp.log(jnp.sum(jnp.exp(scores - top), axis=1, keepdims=True))
    p_ref[...] = jnp.where(ok, jnp.exp(scores - log_norm), 0.0)
    at = lax.broadcasted_iota(jnp.int32, (rows, length), 1)
    picked = jnp.sum(jnp.where(at == meta[:, length:], scores, 0.0), axis=1, keepdims=True)
    diag = (lax.broadcasted_iota(jnp.int32, (rows, rows), 0) == lax.broadcasted_iota(jnp.int32, (rows, rows), 1))
    lp_ref[...] = jnp.sum(jnp.where(diag, picked - log_norm, 0.0), axis=0)


def solution(mesh):
    axes = ("model", "vocab")
    n_model, n_vocab = mesh.shape["model"], mesh.shape["vocab"]
    n = n_model * n_vocab
    row_spec = P(("rep",) + axes, None)
    vec_spec = P(("rep",) + axes)
    vmem = pl.BlockSpec(memory_space=pltpu.VMEM)
    hbm = pl.BlockSpec(memory_space=pl.ANY)

    def local_step(hidden, head_rows, allowed_ids, valid_mask, target_pos):
        rows, length = allowed_ids.shape
        shard_len, width = head_rows.shape
        per = rows * CAP // 128
        tiles = width // 128

        chunks = n * rows * CAP // SLOTS
        tbl, meta, hall = pl.pallas_call(
            functools.partial(route_kernel, shard_len, n, n_vocab),
            out_shape=(jax.ShapeDtypeStruct((n, per, 128), jnp.int32),
                       jax.ShapeDtypeStruct((rows, 2 * length), jnp.int32),
                       jax.ShapeDtypeStruct((n, rows, width), jnp.bfloat16)),
            in_specs=[hbm] * 4,
            out_specs=(hbm, hbm, hbm),
            scratch_shapes=[
                pltpu.VMEM((rows, length), jnp.int32),
                pltpu.VMEM((rows, length), jnp.int32),
                pltpu.VMEM((rows,), jnp.int32),
                pltpu.VMEM((rows, 2 * length), jnp.int32),
                pltpu.VMEM((rows, n * CAP), jnp.int32),
                pltpu.VMEM((n, per, 128), jnp.int32),
                pltpu.VMEM((n, per, 128), jnp.int32),
                pltpu.VMEM((n, rows, width), jnp.bfloat16),
                pltpu.SemaphoreType.DMA((n,)),
                pltpu.SemaphoreType.DMA((n,)),
                pltpu.SemaphoreType.DMA((13,)),
                pltpu.SemaphoreType.DMA((13,)),
                pltpu.SemaphoreType.DMA((4,)),
                pltpu.SemaphoreType.DMA((12,)),
            ],
            compiler_params=pltpu.CompilerParams(collective_id=0, has_side_effects=True),
            name="route",
        )(allowed_ids, valid_mask, target_pos, hidden)
        pairs = head_rows.reshape(shard_len // 8, 4, 2, tiles, 128).transpose(0, 3, 1, 2, 4)
        scores = pl.pallas_call(
            score_kernel,
            out_shape=jax.ShapeDtypeStruct((n, 8, 128), jnp.float32),
            in_specs=[hbm, hbm, hbm],
            out_specs=vmem,
            scratch_shapes=[
                *[pltpu.VMEM((SLOTS // 4, tiles, 8, 128), jnp.bfloat16)] * DEPTH,
                pltpu.SMEM((n, per, 128), jnp.int32),
                pltpu.VMEM((chunks, SLOTS // CAP, width), jnp.bfloat16),
                pltpu.VMEM((SLOTS // CAP, width), jnp.float32),
                pltpu.SemaphoreType.DMA((DEPTH, WAITS)),
                pltpu.SemaphoreType.DMA((3,)),
            ],
            compiler_params=pltpu.CompilerParams(vmem_limit_bytes=67_000_000),
            name="score",
        )(tbl, pairs, hall.reshape(chunks, SLOTS // CAP, width))
        back = pl.pallas_call(
            functools.partial(return_kernel, n, n_vocab),
            out_shape=jax.ShapeDtypeStruct((n, 8, 128), jnp.float32),
            in_specs=[hbm],
            out_specs=hbm,
            scratch_shapes=[
                pltpu.VMEM((n, 8, 128), jnp.float32),
                pltpu.SemaphoreType.DMA((2,)),
                pltpu.SemaphoreType.DMA((n,)),
                pltpu.SemaphoreType.DMA((n,)),
            ],
            compiler_params=pltpu.CompilerParams(collective_id=1, has_side_effects=True),
            name="giveback",
        )(scores)
        return pl.pallas_call(
            softmax_kernel,
            out_shape=(jax.ShapeDtypeStruct((rows, length), jnp.float32), jax.ShapeDtypeStruct((rows,), jnp.float32)),
            in_specs=[vmem, vmem],
            out_specs=(vmem, vmem),
            scratch_shapes=[pltpu.VMEM((128, n * 8), jnp.float32)],
            name="finish",
        )(back, meta)

    return jax.shard_map(local_step, mesh=mesh, in_specs=(row_spec, P(axes, None), row_spec, row_spec, vec_spec),
                         out_specs=(row_spec, vec_spec), check_vma=False)
```

```python
import functools

import jax
import jax.numpy as jnp
from jax import lax
from jax.experimental import pallas as pl
from jax.experimental.pallas import tpu as pltpu
from jax.sharding import PartitionSpec as P

MESH = pl.DeviceIdType.MESH
TEMP = 0.5
CAP = 16
SLOTS = 128
DEPTH = 4
WAITS = 4


def flip_bits(a, k):
    for bit in (1, 2):
        if k & bit:
            a = a + bit - 2 * bit * lax.rem(lax.div(a, bit), 2)
    return a


def peer(m, v, k, n_vocab):
    return flip_bits(m, k // n_vocab), flip_bits(v, k % n_vocab)


def entry_barrier(n, n_vocab, m, v):
    barrier = pltpu.get_barrier_semaphore()
    for k in range(1, n):
        pm, pv = peer(m, v, k, n_vocab)
        pl.semaphore_signal(barrier, inc=1, device_id={"model": pm, "vocab": pv}, device_id_type=MESH)
    return barrier


def route_kernel(shard_len, n, n_vocab, ids_hbm, valid_hbm, tgt_hbm, h_hbm, tbl_out, meta_out, hall_out,
                 ids_ref, valid_ref, tgt_ref, meta_ref, t_ref, send_ref, tin_ref, hbuf, tsend, trecv, hsend, hrecv, lsem, osem):
    rows, length = ids_ref.shape
    m, v = lax.axis_index("model"), lax.axis_index("vocab")
    me = m * n_vocab + v
    barrier = entry_barrier(n, n_vocab, m, v)
    loads = [pltpu.make_async_copy(src, dst, lsem.at[i]) for i, (src, dst) in enumerate(
        ((h_hbm, hbuf.at[0]), (ids_hbm, ids_ref), (valid_hbm, valid_ref), (tgt_hbm, tgt_ref)))]
    for c in loads:
        c.start()

    half = rows // 2
    lo, hi, every = pl.ds(0, half), pl.ds(half, half), pl.ds(0, rows)
    sends = []

    def send(src, dst, part, to):
        pm, pv = peer(m, v, to, n_vocab)
        i = len(sends)
        sends.append(pltpu.make_async_remote_copy(
            src_ref=hbuf.at[src, part], dst_ref=(hall_out if to == 1 else hbuf).at[dst, part], send_sem=hsend.at[i], recv_sem=hrecv.at[i],
            device_id={"model": pm, "vocab": pv}, device_id_type=MESH))
        return sends[-1]

    own_x = [send(0, 2, lo, 2), send(0, 2, hi, 2)]
    own_y = [send(0, 4, lo, 4), send(0, 4, hi, 4)]
    own_p = send(0, 1, every, 1)
    x_to_y, y_to_x = send(2, 6, lo, 4), send(4, 6, hi, 2)
    x_p = [send(2, 3, lo, 1), send(2, 3, hi, 1)]
    y_p = [send(4, 5, lo, 1), send(4, 5, hi, 1)]
    d_p = [send(6, 7, lo, 1), send(6, 7, hi, 1)]

    loads[0].wait()
    pl.semaphore_wait(barrier, n - 1)
    for c in (own_x[0], own_y[1], own_p, own_x[1], own_y[0]):
        c.start()
    outs = []

    def keep(src, dst):
        outs.append(pltpu.make_async_copy(src, dst, osem.at[len(outs)]))
        outs[-1].start()

    keep(hbuf.at[0], hall_out.at[0])
    for c in loads[1:]:
        c.wait()

    ids = ids_ref[...]
    ok = valid_ref[...] > 0
    owner = jnp.where(ok, lax.div(ids, shard_len), n)
    off = lax.rem(ids, shard_len)
    tri = (lax.broadcasted_iota(jnp.int32, (length, length), 0)
           < lax.broadcasted_iota(jnp.int32, (length, length), 1)).astype(jnp.bfloat16)
    rank = jnp.zeros((rows, length), jnp.float32)
    for s in range(n):
        hit = owner == s
        count = jnp.dot(jnp.where(hit, 1.0, 0.0).astype(jnp.bfloat16), tri, preferred_element_type=jnp.float32)
        rank = rank + jnp.where(hit, count, 0.0)
    rank = rank.astype(jnp.int32)
    slot = jnp.where(ok, owner * CAP + rank, n * CAP)
    pair = off - lax.rem(off, 2)

    lane = lax.broadcasted_iota(jnp.int32, (rows, n * CAP), 1)
    row = lax.broadcasted_iota(jnp.int32, (rows, n * CAP), 0)
    spread = lax.rem(((me * rows + row) * CAP + lax.rem(lane, CAP)) * 4, shard_len)
    table = spread
    for j in range(length):
        table = jnp.where(lane == slot[:, j:j + 1], pair[:, j:j + 1], table)
    t_ref[...] = table

    groups = 128 // CAP
    per = rows // groups
    lane4 = lax.broadcasted_iota(jnp.int32, (per, 128), 1)
    parts = [jnp.zeros((per, 128), jnp.int32) for _ in range(n)]
    for q in range(groups):
        tq = t_ref[pl.ds(q, per, stride=groups), :]
        inside = lax.div(lane4, CAP) == q
        for s in range(n):
            moved = tq if q == s else pltpu.roll(tq, ((q - s) * CAP) % 128, axis=1)
            parts[s] = jnp.where(inside, moved, parts[s])
    for s in range(n):
        send_ref[s] = parts[s]

    code = lax.div(rank, 4) * (n * 8) + owner * 8 + lax.rem(rank, 4) * 2 + lax.rem(off, 2)
    diag = (lax.broadcasted_iota(jnp.int32, (rows, rows), 0) == lax.broadcasted_iota(jnp.int32, (rows, rows), 1))
    tcol = jnp.sum(jnp.where(diag, tgt_ref[...].reshape(1, rows), 0).astype(jnp.float32), axis=1, keepdims=True)
    meta_ref[:, :length] = jnp.where(ok, code, -1)
    meta_ref[:, length:] = jnp.broadcast_to(tcol.astype(jnp.int32), (rows, length))

    tin_ref[0] = send_ref[me]
    copies = []
    for k in range(1, n):
        pm, pv = peer(m, v, k, n_vocab)
        c = pltpu.make_async_remote_copy(
            src_ref=send_ref.at[pm * n_vocab + pv], dst_ref=tin_ref.at[k], send_sem=tsend.at[k], recv_sem=trecv.at[k],
            device_id={"model": pm, "vocab": pv}, device_id_type=MESH)
        c.start()
        copies.append(c)

    own_x[0].wait_recv()
    x_to_y.start()
    x_p[0].start()
    own_y[1].wait_recv()
    y_to_x.start()
    y_p[1].start()
    keep(meta_ref, meta_out)
    own_x[1].wait_recv()
    x_p[1].start()
    keep(hbuf.at[2], hall_out.at[2])
    own_y[0].wait_recv()
    y_p[0].start()
    keep(hbuf.at[4], hall_out.at[4])
    for c in copies:
        c.wait_recv()
    keep(tin_ref, tbl_out)
    x_to_y.wait_recv()
    d_p[0].start()
    keep(hbuf.at[6, lo], hall_out.at[6, lo])
    y_to_x.wait_recv()
    d_p[1].start()
    keep(hbuf.at[6, hi], hall_out.at[6, hi])
    for c in [own_p] + x_p + y_p + d_p:
        c.wait_recv()
    for c in sends + copies:
        c.wait_send()
    for c in outs:
        c.wait()


def score_kernel(tbl_hbm, w_hbm, h_hbm, out_ref, *scratch):
    bufs = scratch[:DEPTH]
    tbl_ref, tbl_vmem, h_ref, hf_ref, sems, lsem = scratch[DEPTH:]
    tiles = w_hbm.shape[1]
    nrow = SLOTS // CAP
    quads = CAP // 4
    blocks, per, _ = tbl_ref.shape
    chunks = blocks * per

    tload, hload = pltpu.make_async_copy(tbl_hbm, tbl_vmem, lsem.at[0]), pltpu.make_async_copy(h_hbm, h_ref, lsem.at[1])
    tload.start()
    hload.start()
    first = pltpu.make_async_copy(tbl_vmem.at[0], tbl_ref.at[0], lsem.at[2])
    rest = pltpu.make_async_copy(tbl_vmem.at[pl.ds(1, blocks - 1)], tbl_ref.at[pl.ds(1, blocks - 1)], lsem.at[3])

    def issue(r, b, k, parts=1):
        at = tbl_ref[r // per, r % per, k] if isinstance(r, int) else tbl_ref[lax.div(r, per), lax.rem(r, per), k]
        t, p = lax.shift_right_logical(at, 3), lax.bitwise_and(lax.shift_right_logical(at, 1), 3)
        pltpu.make_async_copy(
            w_hbm.at[t, :, p], bufs[b].at[k // 4, :, pl.ds(2 * (k % 4), 2), :], sems.at[b, k * parts // SLOTS]).start(priority=k % 2)

    lane = lax.broadcasted_iota(jnp.int32, (8, 128), 1)

    def work(c, b, more, parts=1, ahead_parts=1):
        ahead = c + DEPTH - 1
        flat = bufs[b].reshape(SLOTS // 4 * tiles * 8, 128)
        blk, part = lax.div(c, per), lax.rem(c, per)
        hf_ref[...] = h_ref[c].astype(jnp.float32)
        got = jnp.zeros((8, 128), jnp.float32)
        base = part * (SLOTS // 4)
        for i in range(nrow):
            if i % (nrow // parts) == 0:
                w = i // (nrow // parts)
                piece = bufs[b].at[pl.ds(w * (SLOTS // 4 // parts), SLOTS // 4 // parts)]
                pltpu.make_async_copy(piece, piece, sems.at[b, w]).wait()
            acc = [[jnp.zeros((8, 128), jnp.float32)] * 2 for _ in range(quads)]
            for kk in range(0, tiles, 2):
                if more:
                    for k in range(-(-kk * CAP // tiles), -(-(kk + 2) * CAP // tiles)):
                        issue(ahead, (b + DEPTH - 1) % DEPTH, i * CAP + k, ahead_parts)
                hb = [jnp.broadcast_to(hf_ref[i:i + 1, (kk + z) * 128:(kk + z + 1) * 128], (8, 128)) for z in (0, 1)]
                for g in range(quads):
                    at = ((i * quads + g) * tiles + kk) * 8
                    x = flat[at:at + 16, :].astype(jnp.float32)
                    acc[g] = [acc[g][0] + x[:8] * hb[0], acc[g][1] + x[8:] * hb[1]]
            for g in range(quads):
                total = jnp.sum(acc[g][0] + acc[g][1], axis=1, keepdims=True)
                got = jnp.where(lane == base + (i * quads + g), total, got)
        fresh = (lane >= base) & (lane < base + SLOTS // 4)
        out_ref[blk] = jnp.where(fresh, got, out_ref[blk])

    tload.wait()
    first.start()
    rest.start()
    first.wait()
    for c in range(DEPTH - 1):
        for k in range(SLOTS):
            issue(c, c, k)
    rest.wait()
    hload.wait()

    def step(g, _):
        for b in range(DEPTH):
            work(g * DEPTH + b, b, True)
        return 0

    lax.fori_loop(0, chunks // DEPTH - 1, step, 0)
    for b in range(DEPTH):
        work(jnp.int32(chunks - DEPTH + b), b, b == 0, WAITS if b == DEPTH - 1 else 1, WAITS)


def return_kernel(n, n_vocab, sc_hbm, out_hbm, sc_ref, lsem, ssend, srecv):
    m, v = lax.axis_index("model"), lax.axis_index("vocab")
    me = m * n_vocab + v
    barrier = entry_barrier(n, n_vocab, m, v)
    load = pltpu.make_async_copy(sc_hbm, sc_ref, lsem.at[0])
    load.start()
    load.wait()
    pl.semaphore_wait(barrier, n - 1)
    copies = []
    for k in range(1, n):
        pm, pv = peer(m, v, k, n_vocab)
        c = pltpu.make_async_remote_copy(
            src_ref=sc_ref.at[k], dst_ref=out_hbm.at[me], send_sem=ssend.at[k], recv_sem=srecv.at[k],
            device_id={"model": pm, "vocab": pv}, device_id_type=MESH)
        c.start()
        copies.append(c)
    own = pltpu.make_async_copy(sc_ref.at[0], out_hbm.at[me], lsem.at[1])
    own.start()
    for c in copies:
        c.wait_recv()
    for c in copies:
        c.wait_send()
    own.wait()


def softmax_kernel(sc_ref, meta_ref, p_ref, lp_ref, flip):
    n = sc_ref.shape[0]
    rows, length = p_ref.shape
    flip[...] = sc_ref[...].reshape(n * 8, 128).T
    wide = [jnp.concatenate([flip[pl.ds(q, rows, stride=4), :] for q in (2 * hb, 2 * hb + 1)], axis=1) for hb in (0, 1)]
    meta = meta_ref[...]
    code = meta[:, :length]
    ok = code >= 0
    full = jnp.concatenate([jnp.where(ok, code, 0), jnp.zeros((rows, 128 - length), jnp.int32)], axis=1)
    low = jnp.take_along_axis(wide[0], lax.rem(full, 128), axis=1)
    high = jnp.take_along_axis(wide[1], lax.rem(full, 128), axis=1)
    scores = jnp.where(full < 128, low, high)[:, :length] / TEMP
    scores = jnp.where(ok, scores, -jnp.inf)
    top = jnp.max(scores, axis=1, keepdims=True)
    log_norm = top + jnp.log(jnp.sum(jnp.exp(scores - top), axis=1, keepdims=True))
    p_ref[...] = jnp.where(ok, jnp.exp(scores - log_norm), 0.0)
    at = lax.broadcasted_iota(jnp.int32, (rows, length), 1)
    picked = jnp.sum(jnp.where(at == meta[:, length:], scores, 0.0), axis=1, keepdims=True)
    diag = (lax.broadcasted_iota(jnp.int32, (rows, rows), 0) == lax.broadcasted_iota(jnp.int32, (rows, rows), 1))
    lp_ref[...] = jnp.sum(jnp.where(diag, picked - log_norm, 0.0), axis=0)


def solution(mesh):
    axes = ("model", "vocab")
    n_model, n_vocab = mesh.shape["model"], mesh.shape["vocab"]
    n = n_model * n_vocab
    row_spec = P(("rep",) + axes, None)
    vec_spec = P(("rep",) + axes)
    vmem = pl.BlockSpec(memory_space=pltpu.VMEM)
    hbm = pl.BlockSpec(memory_space=pl.ANY)

    def local_step(hidden, head_rows, allowed_ids, valid_mask, target_pos):
        rows, length = allowed_ids.shape
        shard_len, width = head_rows.shape
        per = rows * CAP // 128
        tiles = width // 128

        chunks = n * rows * CAP // SLOTS
        tbl, meta, hall = pl.pallas_call(
            functools.partial(route_kernel, shard_len, n, n_vocab),
            out_shape=(jax.ShapeDtypeStruct((n, per, 128), jnp.int32),
                       jax.ShapeDtypeStruct((rows, 2 * length), jnp.int32),
                       jax.ShapeDtypeStruct((n, rows, width), jnp.bfloat16)),
            in_specs=[hbm] * 4,
            out_specs=(hbm, hbm, hbm),
            scratch_shapes=[
                pltpu.VMEM((rows, length), jnp.int32),
                pltpu.VMEM((rows, length), jnp.int32),
                pltpu.VMEM((rows,), jnp.int32),
                pltpu.VMEM((rows, 2 * length), jnp.int32),
                pltpu.VMEM((rows, n * CAP), jnp.int32),
                pltpu.VMEM((n, per, 128), jnp.int32),
                pltpu.VMEM((n, per, 128), jnp.int32),
                pltpu.VMEM((n, rows, width), jnp.bfloat16),
                pltpu.SemaphoreType.DMA((n,)),
                pltpu.SemaphoreType.DMA((n,)),
                pltpu.SemaphoreType.DMA((13,)),
                pltpu.SemaphoreType.DMA((13,)),
                pltpu.SemaphoreType.DMA((4,)),
                pltpu.SemaphoreType.DMA((12,)),
            ],
            compiler_params=pltpu.CompilerParams(collective_id=0, has_side_effects=True),
            name="route",
        )(allowed_ids, valid_mask, target_pos, hidden)
        pairs = head_rows.reshape(shard_len // 8, 4, 2, tiles, 128).transpose(0, 3, 1, 2, 4)
        scores = pl.pallas_call(
            score_kernel,
            out_shape=jax.ShapeDtypeStruct((n, 8, 128), jnp.float32),
            in_specs=[hbm, hbm, hbm],
            out_specs=vmem,
            scratch_shapes=[
                *[pltpu.VMEM((SLOTS // 4, tiles, 8, 128), jnp.bfloat16)] * DEPTH,
                pltpu.SMEM((n, per, 128), jnp.int32),
                pltpu.VMEM((n, per, 128), jnp.int32),
                pltpu.VMEM((chunks, SLOTS // CAP, width), jnp.bfloat16),
                pltpu.VMEM((SLOTS // CAP, width), jnp.float32),
                pltpu.SemaphoreType.DMA((DEPTH, WAITS)),
                pltpu.SemaphoreType.DMA((4,)),
            ],
            compiler_params=pltpu.CompilerParams(vmem_limit_bytes=67_000_000),
            name="score",
        )(tbl, pairs, hall.reshape(chunks, SLOTS // CAP, width))
        back = pl.pallas_call(
            functools.partial(return_kernel, n, n_vocab),
            out_shape=jax.ShapeDtypeStruct((n, 8, 128), jnp.float32),
            in_specs=[hbm],
            out_specs=hbm,
            scratch_shapes=[
                pltpu.VMEM((n, 8, 128), jnp.float32),
                pltpu.SemaphoreType.DMA((2,)),
                pltpu.SemaphoreType.DMA((n,)),
                pltpu.SemaphoreType.DMA((n,)),
            ],
            compiler_params=pltpu.CompilerParams(collective_id=1, has_side_effects=True),
            name="giveback",
        )(scores)
        return pl.pallas_call(
            softmax_kernel,
            out_shape=(jax.ShapeDtypeStruct((rows, length), jnp.float32), jax.ShapeDtypeStruct((rows,), jnp.float32)),
            in_specs=[vmem, vmem],
            out_specs=(vmem, vmem),
            scratch_shapes=[pltpu.VMEM((128, n * 8), jnp.float32)],
            name="finish",
        )(back, meta)

    return jax.shard_map(local_step, mesh=mesh, in_specs=(row_spec, P(axes, None), row_spec, row_spec, vec_spec),
                         out_specs=(row_spec, vec_spec), check_vma=False)
```

```python
import functools

import jax
import jax.numpy as jnp
from jax import lax
from jax.experimental import pallas as pl
from jax.experimental.pallas import tpu as pltpu
from jax.sharding import PartitionSpec as P

MESH = pl.DeviceIdType.MESH
TEMP = 0.5
CAP = 16
SLOTS = 128
DEPTH = 4
WAITS = 4


def flip_bits(a, k):
    for bit in (1, 2):
        if k & bit:
            a = a + bit - 2 * bit * lax.rem(lax.div(a, bit), 2)
    return a


def peer(m, v, k, n_vocab):
    return flip_bits(m, k // n_vocab), flip_bits(v, k % n_vocab)


def entry_barrier(n, n_vocab, m, v):
    barrier = pltpu.get_barrier_semaphore()
    for k in range(1, n):
        pm, pv = peer(m, v, k, n_vocab)
        pl.semaphore_signal(barrier, inc=1, device_id={"model": pm, "vocab": pv}, device_id_type=MESH)
    return barrier


def route_kernel(shard_len, n, n_vocab, ids_hbm, valid_hbm, tgt_hbm, h_hbm, tbl_out, meta_out, hall_out,
                 ids_ref, valid_ref, tgt_ref, meta_ref, t_ref, send_ref, tin_ref, hbuf, tsend, trecv, hsend, hrecv, lsem, osem):
    rows, length = ids_ref.shape
    m, v = lax.axis_index("model"), lax.axis_index("vocab")
    me = m * n_vocab + v
    barrier = entry_barrier(n, n_vocab, m, v)
    loads = [pltpu.make_async_copy(src, dst, lsem.at[i]) for i, (src, dst) in enumerate(
        ((h_hbm, hbuf.at[0]), (ids_hbm, ids_ref), (valid_hbm, valid_ref), (tgt_hbm, tgt_ref)))]
    for c in loads:
        c.start()

    half = rows // 2
    lo, hi, every = pl.ds(0, half), pl.ds(half, half), pl.ds(0, rows)
    sends = []

    def send(src, dst, part, to):
        pm, pv = peer(m, v, to, n_vocab)
        i = len(sends)
        sends.append(pltpu.make_async_remote_copy(
            src_ref=hbuf.at[src, part], dst_ref=(hall_out if to == 1 else hbuf).at[dst, part], send_sem=hsend.at[i], recv_sem=hrecv.at[i],
            device_id={"model": pm, "vocab": pv}, device_id_type=MESH))
        return sends[-1]

    own_x = [send(0, 2, lo, 2), send(0, 2, hi, 2)]
    own_y = [send(0, 4, lo, 4), send(0, 4, hi, 4)]
    own_p = send(0, 1, every, 1)
    x_to_y, y_to_x = send(2, 6, lo, 4), send(4, 6, hi, 2)
    x_p = [send(2, 3, lo, 1), send(2, 3, hi, 1)]
    y_p = [send(4, 5, lo, 1), send(4, 5, hi, 1)]
    d_p = [send(6, 7, lo, 1), send(6, 7, hi, 1)]

    loads[0].wait()
    pl.semaphore_wait(barrier, n - 1)
    for c in (own_x[0], own_y[1], own_p, own_x[1], own_y[0]):
        c.start()
    outs = []

    def keep(src, dst):
        outs.append(pltpu.make_async_copy(src, dst, osem.at[len(outs)]))
        outs[-1].start()

    keep(hbuf.at[0], hall_out.at[0])
    for c in loads[1:]:
        c.wait()

    ids = ids_ref[...]
    ok = valid_ref[...] > 0
    owner = jnp.where(ok, lax.div(ids, shard_len), n)
    off = lax.rem(ids, shard_len)
    tri = (lax.broadcasted_iota(jnp.int32, (length, length), 0)
           < lax.broadcasted_iota(jnp.int32, (length, length), 1)).astype(jnp.bfloat16)
    rank = jnp.zeros((rows, length), jnp.float32)
    for s in range(n):
        hit = owner == s
        count = jnp.dot(jnp.where(hit, 1.0, 0.0).astype(jnp.bfloat16), tri, preferred_element_type=jnp.float32)
        rank = rank + jnp.where(hit, count, 0.0)
    rank = rank.astype(jnp.int32)
    slot = jnp.where(ok, owner * CAP + rank, n * CAP)
    pair = off - lax.rem(off, 2)

    lane = lax.broadcasted_iota(jnp.int32, (rows, n * CAP), 1)
    row = lax.broadcasted_iota(jnp.int32, (rows, n * CAP), 0)
    spread = lax.rem(((me * rows + row) * CAP + lax.rem(lane, CAP)) * 4, shard_len)
    table = spread
    for j in range(length):
        table = jnp.where(lane == slot[:, j:j + 1], pair[:, j:j + 1], table)
    t_ref[...] = table

    groups = 128 // CAP
    per = rows // groups
    lane4 = lax.broadcasted_iota(jnp.int32, (per, 128), 1)
    parts = [jnp.zeros((per, 128), jnp.int32) for _ in range(n)]
    for q in range(groups):
        tq = t_ref[pl.ds(q, per, stride=groups), :]
        inside = lax.div(lane4, CAP) == q
        for s in range(n):
            moved = tq if q == s else pltpu.roll(tq, ((q - s) * CAP) % 128, axis=1)
            parts[s] = jnp.where(inside, moved, parts[s])
    for s in range(n):
        send_ref[s] = parts[s]

    code = lax.div(rank, 4) * (n * 8) + owner * 8 + lax.rem(rank, 4) * 2 + lax.rem(off, 2)
    diag = (lax.broadcasted_iota(jnp.int32, (rows, rows), 0) == lax.broadcasted_iota(jnp.int32, (rows, rows), 1))
    tcol = jnp.sum(jnp.where(diag, tgt_ref[...].reshape(1, rows), 0).astype(jnp.float32), axis=1, keepdims=True)
    meta_ref[:, :length] = jnp.where(ok, code, -1)
    meta_ref[:, length:] = jnp.broadcast_to(tcol.astype(jnp.int32), (rows, length))

    tin_ref[0] = send_ref[me]
    copies = []
    for k in range(1, n):
        pm, pv = peer(m, v, k, n_vocab)
        c = pltpu.make_async_remote_copy(
            src_ref=send_ref.at[pm * n_vocab + pv], dst_ref=tin_ref.at[k], send_sem=tsend.at[k], recv_sem=trecv.at[k],
            device_id={"model": pm, "vocab": pv}, device_id_type=MESH)
        c.start()
        copies.append(c)

    own_x[0].wait_recv()
    x_to_y.start()
    x_p[0].start()
    own_y[1].wait_recv()
    y_to_x.start()
    y_p[1].start()
    keep(meta_ref, meta_out)
    own_x[1].wait_recv()
    x_p[1].start()
    keep(hbuf.at[2], hall_out.at[2])
    own_y[0].wait_recv()
    y_p[0].start()
    keep(hbuf.at[4], hall_out.at[4])
    for c in copies:
        c.wait_recv()
    keep(tin_ref, tbl_out)
    x_to_y.wait_recv()
    d_p[0].start()
    keep(hbuf.at[6, lo], hall_out.at[6, lo])
    y_to_x.wait_recv()
    d_p[1].start()
    keep(hbuf.at[6, hi], hall_out.at[6, hi])
    for c in [own_p] + x_p + y_p + d_p:
        c.wait_recv()
    for c in sends + copies:
        c.wait_send()
    for c in outs:
        c.wait()


def score_kernel(tbl_hbm, w_hbm, h_hbm, out_ref, *scratch):
    bufs = scratch[:DEPTH]
    tbl_ref, tbl_vmem, h_ref, hf_ref, sems, lsem = scratch[DEPTH:]
    tiles = w_hbm.shape[1]
    nrow = SLOTS // CAP
    quads = CAP // 4
    blocks, per, _ = tbl_ref.shape
    chunks = blocks * per

    tload, hload = pltpu.make_async_copy(tbl_hbm, tbl_vmem, lsem.at[0]), pltpu.make_async_copy(h_hbm, h_ref, lsem.at[1])
    first = pltpu.make_async_copy(tbl_hbm.at[0], tbl_ref.at[0], lsem.at[2])
    first.start()
    tload.start()
    hload.start()
    rest = pltpu.make_async_copy(tbl_vmem.at[pl.ds(1, blocks - 1)], tbl_ref.at[pl.ds(1, blocks - 1)], lsem.at[3])

    def issue(r, b, k, parts=1):
        at = tbl_ref[r // per, r % per, k] if isinstance(r, int) else tbl_ref[lax.div(r, per), lax.rem(r, per), k]
        t, p = lax.shift_right_logical(at, 3), lax.bitwise_and(lax.shift_right_logical(at, 1), 3)
        pltpu.make_async_copy(
            w_hbm.at[t, :, p], bufs[b].at[k // 4, :, pl.ds(2 * (k % 4), 2), :], sems.at[b, k * parts // SLOTS]).start()

    lane = lax.broadcasted_iota(jnp.int32, (8, 128), 1)

    def work(c, b, more, parts=1, ahead_parts=1):
        ahead = c + DEPTH - 1
        flat = bufs[b].reshape(SLOTS // 4 * tiles * 8, 128)
        blk, part = lax.div(c, per), lax.rem(c, per)
        hf_ref[...] = h_ref[c].astype(jnp.float32)
        got = jnp.zeros((8, 128), jnp.float32)
        base = part * (SLOTS // 4)
        for i in range(nrow):
            if i % (nrow // parts) == 0:
                w = i // (nrow // parts)
                piece = bufs[b].at[pl.ds(w * (SLOTS // 4 // parts), SLOTS // 4 // parts)]
                pltpu.make_async_copy(piece, piece, sems.at[b, w]).wait()
            acc = [[jnp.zeros((8, 128), jnp.float32)] * 2 for _ in range(quads)]
            for kk in range(0, tiles, 2):
                if more:
                    for k in range(-(-kk * CAP // tiles), -(-(kk + 2) * CAP // tiles)):
                        issue(ahead, (b + DEPTH - 1) % DEPTH, i * CAP + k, ahead_parts)
                hb = [jnp.broadcast_to(hf_ref[i:i + 1, (kk + z) * 128:(kk + z + 1) * 128], (8, 128)) for z in (0, 1)]
                for g in range(quads):
                    at = ((i * quads + g) * tiles + kk) * 8
                    x = flat[at:at + 16, :].astype(jnp.float32)
                    acc[g] = [acc[g][0] + x[:8] * hb[0], acc[g][1] + x[8:] * hb[1]]
            for g in range(quads):
                total = jnp.sum(acc[g][0] + acc[g][1], axis=1, keepdims=True)
                got = jnp.where(lane == base + (i * quads + g), total, got)
        fresh = (lane >= base) & (lane < base + SLOTS // 4)
        out_ref[blk] = jnp.where(fresh, got, out_ref[blk])

    first.wait()
    for c in range(DEPTH - 1):
        for k in range(SLOTS):
            issue(c, c, k)
    tload.wait()
    rest.start()
    rest.wait()
    hload.wait()

    def step(g, _):
        for b in range(DEPTH):
            work(g * DEPTH + b, b, True)
        return 0

    lax.fori_loop(0, chunks // DEPTH - 1, step, 0)
    for b in range(DEPTH):
        work(jnp.int32(chunks - DEPTH + b), b, b == 0, WAITS if b == DEPTH - 1 else 1, WAITS)


def return_kernel(n, n_vocab, sc_hbm, out_hbm, sc_ref, lsem, ssend, srecv):
    m, v = lax.axis_index("model"), lax.axis_index("vocab")
    me = m * n_vocab + v
    barrier = entry_barrier(n, n_vocab, m, v)
    load = pltpu.make_async_copy(sc_hbm, sc_ref, lsem.at[0])
    load.start()
    load.wait()
    pl.semaphore_wait(barrier, n - 1)
    copies = []
    for k in range(1, n):
        pm, pv = peer(m, v, k, n_vocab)
        c = pltpu.make_async_remote_copy(
            src_ref=sc_ref.at[k], dst_ref=out_hbm.at[me], send_sem=ssend.at[k], recv_sem=srecv.at[k],
            device_id={"model": pm, "vocab": pv}, device_id_type=MESH)
        c.start()
        copies.append(c)
    own = pltpu.make_async_copy(sc_ref.at[0], out_hbm.at[me], lsem.at[1])
    own.start()
    for c in copies:
        c.wait_recv()
    for c in copies:
        c.wait_send()
    own.wait()


def softmax_kernel(sc_ref, meta_ref, p_ref, lp_ref, flip):
    n = sc_ref.shape[0]
    rows, length = p_ref.shape
    flip[...] = sc_ref[...].reshape(n * 8, 128).T
    wide = [jnp.concatenate([flip[pl.ds(q, rows, stride=4), :] for q in (2 * hb, 2 * hb + 1)], axis=1) for hb in (0, 1)]
    meta = meta_ref[...]
    code = meta[:, :length]
    ok = code >= 0
    full = jnp.concatenate([jnp.where(ok, code, 0), jnp.zeros((rows, 128 - length), jnp.int32)], axis=1)
    low = jnp.take_along_axis(wide[0], lax.rem(full, 128), axis=1)
    high = jnp.take_along_axis(wide[1], lax.rem(full, 128), axis=1)
    scores = jnp.where(full < 128, low, high)[:, :length] / TEMP
    scores = jnp.where(ok, scores, -jnp.inf)
    top = jnp.max(scores, axis=1, keepdims=True)
    log_norm = top + jnp.log(jnp.sum(jnp.exp(scores - top), axis=1, keepdims=True))
    p_ref[...] = jnp.where(ok, jnp.exp(scores - log_norm), 0.0)
    at = lax.broadcasted_iota(jnp.int32, (rows, length), 1)
    picked = jnp.sum(jnp.where(at == meta[:, length:], scores, 0.0), axis=1, keepdims=True)
    diag = (lax.broadcasted_iota(jnp.int32, (rows, rows), 0) == lax.broadcasted_iota(jnp.int32, (rows, rows), 1))
    lp_ref[...] = jnp.sum(jnp.where(diag, picked - log_norm, 0.0), axis=0)


def solution(mesh):
    axes = ("model", "vocab")
    n_model, n_vocab = mesh.shape["model"], mesh.shape["vocab"]
    n = n_model * n_vocab
    row_spec = P(("rep",) + axes, None)
    vec_spec = P(("rep",) + axes)
    vmem = pl.BlockSpec(memory_space=pltpu.VMEM)
    hbm = pl.BlockSpec(memory_space=pl.ANY)

    def local_step(hidden, head_rows, allowed_ids, valid_mask, target_pos):
        rows, length = allowed_ids.shape
        shard_len, width = head_rows.shape
        per = rows * CAP // 128
        tiles = width // 128

        chunks = n * rows * CAP // SLOTS
        tbl, meta, hall = pl.pallas_call(
            functools.partial(route_kernel, shard_len, n, n_vocab),
            out_shape=(jax.ShapeDtypeStruct((n, per, 128), jnp.int32),
                       jax.ShapeDtypeStruct((rows, 2 * length), jnp.int32),
                       jax.ShapeDtypeStruct((n, rows, width), jnp.bfloat16)),
            in_specs=[hbm] * 4,
            out_specs=(hbm, hbm, hbm),
            scratch_shapes=[
                pltpu.VMEM((rows, length), jnp.int32),
                pltpu.VMEM((rows, length), jnp.int32),
                pltpu.VMEM((rows,), jnp.int32),
                pltpu.VMEM((rows, 2 * length), jnp.int32),
                pltpu.VMEM((rows, n * CAP), jnp.int32),
                pltpu.VMEM((n, per, 128), jnp.int32),
                pltpu.VMEM((n, per, 128), jnp.int32),
                pltpu.VMEM((n, rows, width), jnp.bfloat16),
                pltpu.SemaphoreType.DMA((n,)),
                pltpu.SemaphoreType.DMA((n,)),
                pltpu.SemaphoreType.DMA((13,)),
                pltpu.SemaphoreType.DMA((13,)),
                pltpu.SemaphoreType.DMA((4,)),
                pltpu.SemaphoreType.DMA((12,)),
            ],
            compiler_params=pltpu.CompilerParams(collective_id=0, has_side_effects=True),
            name="route",
        )(allowed_ids, valid_mask, target_pos, hidden)
        pairs = head_rows.reshape(shard_len // 8, 4, 2, tiles, 128).transpose(0, 3, 1, 2, 4)
        scores = pl.pallas_call(
            score_kernel,
            out_shape=jax.ShapeDtypeStruct((n, 8, 128), jnp.float32),
            in_specs=[hbm, hbm, hbm],
            out_specs=vmem,
            scratch_shapes=[
                *[pltpu.VMEM((SLOTS // 4, tiles, 8, 128), jnp.bfloat16)] * DEPTH,
                pltpu.SMEM((n, per, 128), jnp.int32),
                pltpu.VMEM((n, per, 128), jnp.int32),
                pltpu.VMEM((chunks, SLOTS // CAP, width), jnp.bfloat16),
                pltpu.VMEM((SLOTS // CAP, width), jnp.float32),
                pltpu.SemaphoreType.DMA((DEPTH, WAITS)),
                pltpu.SemaphoreType.DMA((4,)),
            ],
            compiler_params=pltpu.CompilerParams(vmem_limit_bytes=67_000_000),
            name="score",
        )(tbl, pairs, hall.reshape(chunks, SLOTS // CAP, width))
        back = pl.pallas_call(
            functools.partial(return_kernel, n, n_vocab),
            out_shape=jax.ShapeDtypeStruct((n, 8, 128), jnp.float32),
            in_specs=[hbm],
            out_specs=hbm,
            scratch_shapes=[
                pltpu.VMEM((n, 8, 128), jnp.float32),
                pltpu.SemaphoreType.DMA((2,)),
                pltpu.SemaphoreType.DMA((n,)),
                pltpu.SemaphoreType.DMA((n,)),
            ],
            compiler_params=pltpu.CompilerParams(collective_id=1, has_side_effects=True),
            name="giveback",
        )(scores)
        return pl.pallas_call(
            softmax_kernel,
            out_shape=(jax.ShapeDtypeStruct((rows, length), jnp.float32), jax.ShapeDtypeStruct((rows,), jnp.float32)),
            in_specs=[vmem, vmem],
            out_specs=(vmem, vmem),
            scratch_shapes=[pltpu.VMEM((128, n * 8), jnp.float32)],
            name="finish",
        )(back, meta)

    return jax.shard_map(local_step, mesh=mesh, in_specs=(row_spec, P(axes, None), row_spec, row_spec, vec_spec),
                         out_specs=(row_spec, vec_spec), check_vma=False)
```

```python
import functools

import jax
import jax.numpy as jnp
from jax import lax
from jax.experimental import pallas as pl
from jax.experimental.pallas import tpu as pltpu
from jax.sharding import PartitionSpec as P

MESH = pl.DeviceIdType.MESH
TEMP = 0.5
CAP = 16
SLOTS = 128
DEPTH = 4
WAITS = 4


def flip_bits(a, k):
    for bit in (1, 2):
        if k & bit:
            a = a + bit - 2 * bit * lax.rem(lax.div(a, bit), 2)
    return a


def peer(m, v, k, n_vocab):
    return flip_bits(m, k // n_vocab), flip_bits(v, k % n_vocab)


def entry_barrier(n, n_vocab, m, v):
    barrier = pltpu.get_barrier_semaphore()
    for k in range(1, n):
        pm, pv = peer(m, v, k, n_vocab)
        pl.semaphore_signal(barrier, inc=1, device_id={"model": pm, "vocab": pv}, device_id_type=MESH)
    return barrier


def route_kernel(shard_len, n, n_vocab, ids_hbm, valid_hbm, tgt_hbm, h_hbm, tbl_out, meta_out, hall_out,
                 ids_ref, valid_ref, tgt_ref, meta_ref, t_ref, send_ref, tin_ref, hbuf, tsend, trecv, hsend, hrecv, lsem, osem):
    rows, length = ids_ref.shape
    m, v = lax.axis_index("model"), lax.axis_index("vocab")
    me = m * n_vocab + v
    barrier = entry_barrier(n, n_vocab, m, v)
    loads = [pltpu.make_async_copy(src, dst, lsem.at[i]) for i, (src, dst) in enumerate(
        ((h_hbm, hbuf.at[0]), (ids_hbm, ids_ref), (valid_hbm, valid_ref), (tgt_hbm, tgt_ref)))]
    for c in loads:
        c.start()

    half = rows // 2
    lo, hi, every = pl.ds(0, half), pl.ds(half, half), pl.ds(0, rows)
    sends = []

    def send(src, dst, part, to):
        pm, pv = peer(m, v, to, n_vocab)
        i = len(sends)
        sends.append(pltpu.make_async_remote_copy(
            src_ref=hbuf.at[src, part], dst_ref=(hall_out if to == 1 else hbuf).at[dst, part], send_sem=hsend.at[i], recv_sem=hrecv.at[i],
            device_id={"model": pm, "vocab": pv}, device_id_type=MESH))
        return sends[-1]

    own_x = [send(0, 2, lo, 2), send(0, 2, hi, 2)]
    own_y = [send(0, 4, lo, 4), send(0, 4, hi, 4)]
    own_p = send(0, 1, every, 1)
    quarter = [pl.ds(i * half // 2, half // 2) for i in range(4)]
    x_to_y, y_to_x = [send(2, 6, q, 4) for q in quarter[:2]], [send(4, 6, q, 2) for q in quarter[2:]]
    x_p = [send(2, 3, lo, 1), send(2, 3, hi, 1)]
    y_p = [send(4, 5, lo, 1), send(4, 5, hi, 1)]
    d_p = [send(6, 7, q, 1) for q in quarter]

    loads[0].wait()
    pl.semaphore_wait(barrier, n - 1)
    for c in (own_x[0], own_y[1], own_p, own_x[1], own_y[0]):
        c.start()
    outs = []

    def keep(src, dst):
        outs.append(pltpu.make_async_copy(src, dst, osem.at[len(outs)]))
        outs[-1].start()

    keep(hbuf.at[0], hall_out.at[0])
    for c in loads[1:]:
        c.wait()

    ids = ids_ref[...]
    ok = valid_ref[...] > 0
    owner = jnp.where(ok, lax.div(ids, shard_len), n)
    off = lax.rem(ids, shard_len)
    tri = (lax.broadcasted_iota(jnp.int32, (length, length), 0)
           < lax.broadcasted_iota(jnp.int32, (length, length), 1)).astype(jnp.bfloat16)
    rank = jnp.zeros((rows, length), jnp.float32)
    for s in range(n):
        hit = owner == s
        count = jnp.dot(jnp.where(hit, 1.0, 0.0).astype(jnp.bfloat16), tri, preferred_element_type=jnp.float32)
        rank = rank + jnp.where(hit, count, 0.0)
    rank = rank.astype(jnp.int32)
    slot = jnp.where(ok, owner * CAP + rank, n * CAP)
    pair = off - lax.rem(off, 2)

    lane = lax.broadcasted_iota(jnp.int32, (rows, n * CAP), 1)
    row = lax.broadcasted_iota(jnp.int32, (rows, n * CAP), 0)
    spread = lax.rem(((me * rows + row) * CAP + lax.rem(lane, CAP)) * 4, shard_len)
    table = spread
    for j in range(length):
        table = jnp.where(lane == slot[:, j:j + 1], pair[:, j:j + 1], table)
    t_ref[...] = table

    groups = 128 // CAP
    per = rows // groups
    lane4 = lax.broadcasted_iota(jnp.int32, (per, 128), 1)
    parts = [jnp.zeros((per, 128), jnp.int32) for _ in range(n)]
    for q in range(groups):
        tq = t_ref[pl.ds(q, per, stride=groups), :]
        inside = lax.div(lane4, CAP) == q
        for s in range(n):
            moved = tq if q == s else pltpu.roll(tq, ((q - s) * CAP) % 128, axis=1)
            parts[s] = jnp.where(inside, moved, parts[s])
    for s in range(n):
        send_ref[s] = parts[s]

    code = lax.div(rank, 4) * (n * 8) + owner * 8 + lax.rem(rank, 4) * 2 + lax.rem(off, 2)
    diag = (lax.broadcasted_iota(jnp.int32, (rows, rows), 0) == lax.broadcasted_iota(jnp.int32, (rows, rows), 1))
    tcol = jnp.sum(jnp.where(diag, tgt_ref[...].reshape(1, rows), 0).astype(jnp.float32), axis=1, keepdims=True)
    meta_ref[:, :length] = jnp.where(ok, code, -1)
    meta_ref[:, length:] = jnp.broadcast_to(tcol.astype(jnp.int32), (rows, length))

    tin_ref[0] = send_ref[me]
    copies = []
    for k in range(1, n):
        pm, pv = peer(m, v, k, n_vocab)
        copies.append(pltpu.make_async_remote_copy(
            src_ref=send_ref.at[pm * n_vocab + pv], dst_ref=tin_ref.at[k], send_sem=tsend.at[k], recv_sem=trecv.at[k],
            device_id={"model": pm, "vocab": pv}, device_id_type=MESH))

    own_x[0].wait_recv()
    for c in copies:
        c.start()
    for c in x_to_y:
        c.start()
    x_p[0].start()
    own_y[1].wait_recv()
    for c in y_to_x:
        c.start()
    y_p[1].start()
    keep(meta_ref, meta_out)
    own_x[1].wait_recv()
    x_p[1].start()
    keep(hbuf.at[2], hall_out.at[2])
    own_y[0].wait_recv()
    y_p[0].start()
    keep(hbuf.at[4], hall_out.at[4])
    for c in copies:
        c.wait_recv()
    keep(tin_ref, tbl_out)
    for i in range(2):
        x_to_y[i].wait_recv()
        d_p[i].start()
        y_to_x[i].wait_recv()
        d_p[2 + i].start()
    keep(hbuf.at[6], hall_out.at[6])
    for c in [own_p] + x_p + y_p + d_p:
        c.wait_recv()
    for c in sends + copies:
        c.wait_send()
    for c in outs:
        c.wait()


def score_kernel(tbl_hbm, w_hbm, h_hbm, out_ref, *scratch):
    bufs = scratch[:DEPTH]
    tbl_ref, tbl_vmem, h_ref, hf_ref, sems, lsem = scratch[DEPTH:]
    tiles = w_hbm.shape[1]
    nrow = SLOTS // CAP
    quads = CAP // 4
    blocks, per, _ = tbl_ref.shape
    chunks = blocks * per

    tload, hload = pltpu.make_async_copy(tbl_hbm, tbl_vmem, lsem.at[0]), pltpu.make_async_copy(h_hbm, h_ref, lsem.at[1])
    first = pltpu.make_async_copy(tbl_hbm.at[0], tbl_ref.at[0], lsem.at[2])
    first.start()
    tload.start()
    hload.start()
    rest = pltpu.make_async_copy(tbl_vmem.at[pl.ds(1, blocks - 1)], tbl_ref.at[pl.ds(1, blocks - 1)], lsem.at[3])

    def issue(r, b, k, parts=1):
        at = tbl_ref[r // per, r % per, k] if isinstance(r, int) else tbl_ref[lax.div(r, per), lax.rem(r, per), k]
        t, p = lax.shift_right_logical(at, 3), lax.bitwise_and(lax.shift_right_logical(at, 1), 3)
        pltpu.make_async_copy(
            w_hbm.at[t, :, p], bufs[b].at[k // 4, :, pl.ds(2 * (k % 4), 2), :], sems.at[b, k * parts // SLOTS]).start()

    lane = lax.broadcasted_iota(jnp.int32, (8, 128), 1)

    def work(c, b, more, parts=1, ahead_parts=1):
        ahead = c + DEPTH - 1
        flat = bufs[b].reshape(SLOTS // 4 * tiles * 8, 128)
        blk, part = lax.div(c, per), lax.rem(c, per)
        hf_ref[...] = h_ref[c].astype(jnp.float32)
        got = jnp.zeros((8, 128), jnp.float32)
        base = part * (SLOTS // 4)
        for i in range(nrow):
            if i % (nrow // parts) == 0:
                w = i // (nrow // parts)
                piece = bufs[b].at[pl.ds(w * (SLOTS // 4 // parts), SLOTS // 4 // parts)]
                pltpu.make_async_copy(piece, piece, sems.at[b, w]).wait()
            acc = [[jnp.zeros((8, 128), jnp.float32)] * 2 for _ in range(quads)]
            for kk in range(0, tiles, 2):
                if more:
                    for k in range(-(-kk * CAP // tiles), -(-(kk + 2) * CAP // tiles)):
                        issue(ahead, (b + DEPTH - 1) % DEPTH, i * CAP + k, ahead_parts)
                hb = [jnp.broadcast_to(hf_ref[i:i + 1, (kk + z) * 128:(kk + z + 1) * 128], (8, 128)) for z in (0, 1)]
                for g in range(quads):
                    at = ((i * quads + g) * tiles + kk) * 8
                    x = flat[at:at + 16, :].astype(jnp.float32)
                    acc[g] = [acc[g][0] + x[:8] * hb[0], acc[g][1] + x[8:] * hb[1]]
            for g in range(quads):
                total = jnp.sum(acc[g][0] + acc[g][1], axis=1, keepdims=True)
                got = jnp.where(lane == base + (i * quads + g), total, got)
        fresh = (lane >= base) & (lane < base + SLOTS // 4)
        out_ref[blk] = jnp.where(fresh, got, out_ref[blk])

    first.wait()
    for c in range(DEPTH - 1):
        for k in range(SLOTS):
            issue(c, c, k)
    tload.wait()
    rest.start()
    rest.wait()
    hload.wait()

    def step(g, _):
        for b in range(DEPTH):
            work(g * DEPTH + b, b, True)
        return 0

    lax.fori_loop(0, chunks // DEPTH - 1, step, 0)
    for b in range(DEPTH):
        work(jnp.int32(chunks - DEPTH + b), b, b == 0, WAITS if b == DEPTH - 1 else 1, WAITS)


def return_kernel(n, n_vocab, sc_hbm, out_hbm, sc_ref, lsem, ssend, srecv):
    m, v = lax.axis_index("model"), lax.axis_index("vocab")
    me = m * n_vocab + v
    barrier = entry_barrier(n, n_vocab, m, v)
    load = pltpu.make_async_copy(sc_hbm, sc_ref, lsem.at[0])
    load.start()
    load.wait()
    pl.semaphore_wait(barrier, n - 1)
    copies = []
    for k in range(1, n):
        pm, pv = peer(m, v, k, n_vocab)
        c = pltpu.make_async_remote_copy(
            src_ref=sc_ref.at[k], dst_ref=out_hbm.at[me], send_sem=ssend.at[k], recv_sem=srecv.at[k],
            device_id={"model": pm, "vocab": pv}, device_id_type=MESH)
        c.start()
        copies.append(c)
    own = pltpu.make_async_copy(sc_ref.at[0], out_hbm.at[me], lsem.at[1])
    own.start()
    for c in copies:
        c.wait_recv()
    for c in copies:
        c.wait_send()
    own.wait()


def softmax_kernel(sc_ref, meta_ref, p_ref, lp_ref, flip):
    n = sc_ref.shape[0]
    rows, length = p_ref.shape
    flip[...] = sc_ref[...].reshape(n * 8, 128).T
    wide = [jnp.concatenate([flip[pl.ds(q, rows, stride=4), :] for q in (2 * hb, 2 * hb + 1)], axis=1) for hb in (0, 1)]
    meta = meta_ref[...]
    code = meta[:, :length]
    ok = code >= 0
    full = jnp.concatenate([jnp.where(ok, code, 0), jnp.zeros((rows, 128 - length), jnp.int32)], axis=1)
    low = jnp.take_along_axis(wide[0], lax.rem(full, 128), axis=1)
    high = jnp.take_along_axis(wide[1], lax.rem(full, 128), axis=1)
    scores = jnp.where(full < 128, low, high)[:, :length] / TEMP
    scores = jnp.where(ok, scores, -jnp.inf)
    top = jnp.max(scores, axis=1, keepdims=True)
    log_norm = top + jnp.log(jnp.sum(jnp.exp(scores - top), axis=1, keepdims=True))
    p_ref[...] = jnp.where(ok, jnp.exp(scores - log_norm), 0.0)
    at = lax.broadcasted_iota(jnp.int32, (rows, length), 1)
    picked = jnp.sum(jnp.where(at == meta[:, length:], scores, 0.0), axis=1, keepdims=True)
    diag = (lax.broadcasted_iota(jnp.int32, (rows, rows), 0) == lax.broadcasted_iota(jnp.int32, (rows, rows), 1))
    lp_ref[...] = jnp.sum(jnp.where(diag, picked - log_norm, 0.0), axis=0)


def solution(mesh):
    axes = ("model", "vocab")
    n_model, n_vocab = mesh.shape["model"], mesh.shape["vocab"]
    n = n_model * n_vocab
    row_spec = P(("rep",) + axes, None)
    vec_spec = P(("rep",) + axes)
    vmem = pl.BlockSpec(memory_space=pltpu.VMEM)
    hbm = pl.BlockSpec(memory_space=pl.ANY)

    def local_step(hidden, head_rows, allowed_ids, valid_mask, target_pos):
        rows, length = allowed_ids.shape
        shard_len, width = head_rows.shape
        per = rows * CAP // 128
        tiles = width // 128

        chunks = n * rows * CAP // SLOTS
        tbl, meta, hall = pl.pallas_call(
            functools.partial(route_kernel, shard_len, n, n_vocab),
            out_shape=(jax.ShapeDtypeStruct((n, per, 128), jnp.int32),
                       jax.ShapeDtypeStruct((rows, 2 * length), jnp.int32),
                       jax.ShapeDtypeStruct((n, rows, width), jnp.bfloat16)),
            in_specs=[hbm] * 4,
            out_specs=(hbm, hbm, hbm),
            scratch_shapes=[
                pltpu.VMEM((rows, length), jnp.int32),
                pltpu.VMEM((rows, length), jnp.int32),
                pltpu.VMEM((rows,), jnp.int32),
                pltpu.VMEM((rows, 2 * length), jnp.int32),
                pltpu.VMEM((rows, n * CAP), jnp.int32),
                pltpu.VMEM((n, per, 128), jnp.int32),
                pltpu.VMEM((n, per, 128), jnp.int32),
                pltpu.VMEM((n, rows, width), jnp.bfloat16),
                pltpu.SemaphoreType.DMA((n,)),
                pltpu.SemaphoreType.DMA((n,)),
                pltpu.SemaphoreType.DMA((17,)),
                pltpu.SemaphoreType.DMA((17,)),
                pltpu.SemaphoreType.DMA((4,)),
                pltpu.SemaphoreType.DMA((12,)),
            ],
            compiler_params=pltpu.CompilerParams(collective_id=0, has_side_effects=True),
            name="route",
        )(allowed_ids, valid_mask, target_pos, hidden)
        pairs = head_rows.reshape(shard_len // 8, 4, 2, tiles, 128).transpose(0, 3, 1, 2, 4)
        scores = pl.pallas_call(
            score_kernel,
            out_shape=jax.ShapeDtypeStruct((n, 8, 128), jnp.float32),
            in_specs=[hbm, hbm, hbm],
            out_specs=vmem,
            scratch_shapes=[
                *[pltpu.VMEM((SLOTS // 4, tiles, 8, 128), jnp.bfloat16)] * DEPTH,
                pltpu.SMEM((n, per, 128), jnp.int32),
                pltpu.VMEM((n, per, 128), jnp.int32),
                pltpu.VMEM((chunks, SLOTS // CAP, width), jnp.bfloat16),
                pltpu.VMEM((SLOTS // CAP, width), jnp.float32),
                pltpu.SemaphoreType.DMA((DEPTH, WAITS)),
                pltpu.SemaphoreType.DMA((4,)),
            ],
            compiler_params=pltpu.CompilerParams(vmem_limit_bytes=67_000_000),
            name="score",
        )(tbl, pairs, hall.reshape(chunks, SLOTS // CAP, width))
        back = pl.pallas_call(
            functools.partial(return_kernel, n, n_vocab),
            out_shape=jax.ShapeDtypeStruct((n, 8, 128), jnp.float32),
            in_specs=[hbm],
            out_specs=hbm,
            scratch_shapes=[
                pltpu.VMEM((n, 8, 128), jnp.float32),
                pltpu.SemaphoreType.DMA((2,)),
                pltpu.SemaphoreType.DMA((n,)),
                pltpu.SemaphoreType.DMA((n,)),
            ],
            compiler_params=pltpu.CompilerParams(collective_id=1, has_side_effects=True),
            name="giveback",
        )(scores)
        return pl.pallas_call(
            softmax_kernel,
            out_shape=(jax.ShapeDtypeStruct((rows, length), jnp.float32), jax.ShapeDtypeStruct((rows,), jnp.float32)),
            in_specs=[vmem, vmem],
            out_specs=(vmem, vmem),
            scratch_shapes=[pltpu.VMEM((128, n * 8), jnp.float32)],
            name="finish",
        )(back, meta)

    return jax.shard_map(local_step, mesh=mesh, in_specs=(row_spec, P(axes, None), row_spec, row_spec, vec_spec),
                         out_specs=(row_spec, vec_spec), check_vma=False)
```

```python
import functools

import jax
import jax.numpy as jnp
from jax import lax
from jax.experimental import pallas as pl
from jax.experimental.pallas import tpu as pltpu
from jax.sharding import PartitionSpec as P

MESH = pl.DeviceIdType.MESH
TEMP = 0.5
CAP = 16
SLOTS = 128
DEPTH = 4
WAITS = 4


def flip_bits(a, k):
    for bit in (1, 2):
        if k & bit:
            a = a + bit - 2 * bit * lax.rem(lax.div(a, bit), 2)
    return a


def peer(m, v, k, n_vocab):
    return flip_bits(m, k // n_vocab), flip_bits(v, k % n_vocab)


def signal_peers(sem, ks, n_vocab, m, v):
    for k in ks:
        pm, pv = peer(m, v, k, n_vocab)
        pl.semaphore_signal(sem, inc=1, device_id={"model": pm, "vocab": pv}, device_id_type=MESH)


NEAR = (1, 2, 4)


def route_kernel(shard_len, n, n_vocab, ids_hbm, valid_hbm, tgt_hbm, h_hbm, tbl_out, meta_out, hall_out,
                 ids_ref, valid_ref, tgt_ref, meta_ref, t_ref, send_ref, tin_ref, hbuf, tsend, trecv, hsend, hrecv, lsem, osem, round_sem):
    rows, length = ids_ref.shape
    m, v = lax.axis_index("model"), lax.axis_index("vocab")
    me = m * n_vocab + v
    barrier = pltpu.get_barrier_semaphore()
    signal_peers(barrier, NEAR, n_vocab, m, v)
    loads = [pltpu.make_async_copy(src, dst, lsem.at[i]) for i, (src, dst) in enumerate(
        ((h_hbm, hbuf.at[0]), (ids_hbm, ids_ref), (valid_hbm, valid_ref), (tgt_hbm, tgt_ref)))]
    for c in loads:
        c.start()

    half = rows // 2
    lo, hi, every = pl.ds(0, half), pl.ds(half, half), pl.ds(0, rows)
    sends = []

    def send(src, dst, part, to):
        pm, pv = peer(m, v, to, n_vocab)
        i = len(sends)
        sends.append(pltpu.make_async_remote_copy(
            src_ref=hbuf.at[src, part], dst_ref=(hall_out if to == 1 else hbuf).at[dst, part], send_sem=hsend.at[i], recv_sem=hrecv.at[i],
            device_id={"model": pm, "vocab": pv}, device_id_type=MESH))
        return sends[-1]

    own_x = [send(0, 2, lo, 2), send(0, 2, hi, 2)]
    own_y = [send(0, 4, lo, 4), send(0, 4, hi, 4)]
    own_p = send(0, 1, every, 1)
    quarter = [pl.ds(i * half // 2, half // 2) for i in range(4)]
    x_to_y, y_to_x = [send(2, 6, q, 4) for q in quarter[:2]], [send(4, 6, q, 2) for q in quarter[2:]]
    x_p = [send(2, 3, lo, 1), send(2, 3, hi, 1)]
    y_p = [send(4, 5, lo, 1), send(4, 5, hi, 1)]
    d_p = [send(6, 7, q, 1) for q in quarter]

    loads[0].wait()
    pl.semaphore_wait(barrier, len(NEAR))
    for c in (own_x[0], own_y[1], own_p, own_x[1], own_y[0]):
        c.start()
    signal_peers(round_sem.at[0], NEAR, n_vocab, m, v)
    outs = []

    def keep(src, dst):
        outs.append(pltpu.make_async_copy(src, dst, osem.at[len(outs)]))
        outs[-1].start()

    keep(hbuf.at[0], hall_out.at[0])
    for c in loads[1:]:
        c.wait()

    ids = ids_ref[...]
    ok = valid_ref[...] > 0
    owner = jnp.where(ok, lax.div(ids, shard_len), n)
    off = lax.rem(ids, shard_len)
    tri = (lax.broadcasted_iota(jnp.int32, (length, length), 0)
           < lax.broadcasted_iota(jnp.int32, (length, length), 1)).astype(jnp.bfloat16)
    rank = jnp.zeros((rows, length), jnp.float32)
    for s in range(n):
        hit = owner == s
        count = jnp.dot(jnp.where(hit, 1.0, 0.0).astype(jnp.bfloat16), tri, preferred_element_type=jnp.float32)
        rank = rank + jnp.where(hit, count, 0.0)
    rank = rank.astype(jnp.int32)
    slot = jnp.where(ok, owner * CAP + rank, n * CAP)
    pair = off - lax.rem(off, 2)

    lane = lax.broadcasted_iota(jnp.int32, (rows, n * CAP), 1)
    row = lax.broadcasted_iota(jnp.int32, (rows, n * CAP), 0)
    spread = lax.rem(((me * rows + row) * CAP + lax.rem(lane, CAP)) * 4, shard_len)
    table = spread
    for j in range(length):
        table = jnp.where(lane == slot[:, j:j + 1], pair[:, j:j + 1], table)
    t_ref[...] = table

    groups = 128 // CAP
    per = rows // groups
    lane4 = lax.broadcasted_iota(jnp.int32, (per, 128), 1)
    parts = [jnp.zeros((per, 128), jnp.int32) for _ in range(n)]
    for q in range(groups):
        tq = t_ref[pl.ds(q, per, stride=groups), :]
        inside = lax.div(lane4, CAP) == q
        for s in range(n):
            moved = tq if q == s else pltpu.roll(tq, ((q - s) * CAP) % 128, axis=1)
            parts[s] = jnp.where(inside, moved, parts[s])
    for s in range(n):
        send_ref[s] = parts[s]

    code = lax.div(rank, 4) * (n * 8) + owner * 8 + lax.rem(rank, 4) * 2 + lax.rem(off, 2)
    diag = (lax.broadcasted_iota(jnp.int32, (rows, rows), 0) == lax.broadcasted_iota(jnp.int32, (rows, rows), 1))
    tcol = jnp.sum(jnp.where(diag, tgt_ref[...].reshape(1, rows), 0).astype(jnp.float32), axis=1, keepdims=True)
    meta_ref[:, :length] = jnp.where(ok, code, -1)
    meta_ref[:, length:] = jnp.broadcast_to(tcol.astype(jnp.int32), (rows, length))

    tin_ref[0] = send_ref[me]
    copies = []
    for k in range(1, n):
        pm, pv = peer(m, v, k, n_vocab)
        copies.append(pltpu.make_async_remote_copy(
            src_ref=send_ref.at[pm * n_vocab + pv], dst_ref=tin_ref.at[k], send_sem=tsend.at[k], recv_sem=trecv.at[k],
            device_id={"model": pm, "vocab": pv}, device_id_type=MESH))

    pl.semaphore_wait(round_sem.at[0], len(NEAR))
    signal_peers(round_sem.at[1], NEAR, n_vocab, m, v)
    own_x[0].wait_recv()
    pl.semaphore_wait(round_sem.at[1], len(NEAR))
    for c in copies:
        c.start()
    for c in x_to_y:
        c.start()
    x_p[0].start()
    own_y[1].wait_recv()
    for c in y_to_x:
        c.start()
    y_p[1].start()
    keep(meta_ref, meta_out)
    own_x[1].wait_recv()
    x_p[1].start()
    keep(hbuf.at[2], hall_out.at[2])
    own_y[0].wait_recv()
    y_p[0].start()
    keep(hbuf.at[4], hall_out.at[4])
    for c in copies:
        c.wait_recv()
    keep(tin_ref, tbl_out)
    for i in range(2):
        x_to_y[i].wait_recv()
        d_p[i].start()
        y_to_x[i].wait_recv()
        d_p[2 + i].start()
    keep(hbuf.at[6], hall_out.at[6])
    for c in [own_p] + x_p + y_p + d_p:
        c.wait_recv()
    for c in sends + copies:
        c.wait_send()
    for c in outs:
        c.wait()


def score_kernel(tbl_hbm, w_hbm, h_hbm, out_ref, *scratch):
    bufs = scratch[:DEPTH]
    tbl_ref, tbl_vmem, h_ref, hf_ref, sems, lsem = scratch[DEPTH:]
    tiles = w_hbm.shape[1]
    nrow = SLOTS // CAP
    quads = CAP // 4
    blocks, per, _ = tbl_ref.shape
    chunks = blocks * per

    tload, hload = pltpu.make_async_copy(tbl_hbm, tbl_vmem, lsem.at[0]), pltpu.make_async_copy(h_hbm, h_ref, lsem.at[1])
    first = pltpu.make_async_copy(tbl_hbm.at[0], tbl_ref.at[0], lsem.at[2])
    first.start()
    tload.start()
    hload.start()
    rest = pltpu.make_async_copy(tbl_vmem.at[pl.ds(1, blocks - 1)], tbl_ref.at[pl.ds(1, blocks - 1)], lsem.at[3])

    def issue(r, b, k, parts=1):
        at = tbl_ref[r // per, r % per, k] if isinstance(r, int) else tbl_ref[lax.div(r, per), lax.rem(r, per), k]
        t, p = lax.shift_right_logical(at, 3), lax.bitwise_and(lax.shift_right_logical(at, 1), 3)
        pltpu.make_async_copy(
            w_hbm.at[t, :, p], bufs[b].at[k // 4, :, pl.ds(2 * (k % 4), 2), :], sems.at[b, k * parts // SLOTS]).start()

    lane = lax.broadcasted_iota(jnp.int32, (8, 128), 1)

    def work(c, b, more, parts=1, ahead_parts=1):
        ahead = c + DEPTH - 1
        flat = bufs[b].reshape(SLOTS // 4 * tiles * 8, 128)
        blk, part = lax.div(c, per), lax.rem(c, per)
        hf_ref[...] = h_ref[c].astype(jnp.float32)
        got = jnp.zeros((8, 128), jnp.float32)
        base = part * (SLOTS // 4)
        for i in range(nrow):
            if i % (nrow // parts) == 0:
                w = i // (nrow // parts)
                piece = bufs[b].at[pl.ds(w * (SLOTS // 4 // parts), SLOTS // 4 // parts)]
                pltpu.make_async_copy(piece, piece, sems.at[b, w]).wait()
            acc = [[jnp.zeros((8, 128), jnp.float32)] * 2 for _ in range(quads)]
            for kk in range(0, tiles, 2):
                if more:
                    for k in range(-(-kk * CAP // tiles), -(-(kk + 2) * CAP // tiles)):
                        issue(ahead, (b + DEPTH - 1) % DEPTH, i * CAP + k, ahead_parts)
                hb = [jnp.broadcast_to(hf_ref[i:i + 1, (kk + z) * 128:(kk + z + 1) * 128], (8, 128)) for z in (0, 1)]
                for g in range(quads):
                    at = ((i * quads + g) * tiles + kk) * 8
                    x = flat[at:at + 16, :].astype(jnp.float32)
                    acc[g] = [acc[g][0] + x[:8] * hb[0], acc[g][1] + x[8:] * hb[1]]
            for g in range(quads):
                total = jnp.sum(acc[g][0] + acc[g][1], axis=1, keepdims=True)
                got = jnp.where(lane == base + (i * quads + g), total, got)
        fresh = (lane >= base) & (lane < base + SLOTS // 4)
        out_ref[blk] = jnp.where(fresh, got, out_ref[blk])

    first.wait()
    for c in range(DEPTH - 1):
        for k in range(SLOTS):
            issue(c, c, k)
    tload.wait()
    rest.start()
    rest.wait()
    hload.wait()

    def step(g, _):
        for b in range(DEPTH):
            work(g * DEPTH + b, b, True)
        return 0

    lax.fori_loop(0, chunks // DEPTH - 1, step, 0)
    for b in range(DEPTH):
        work(jnp.int32(chunks - DEPTH + b), b, b == 0, WAITS if b == DEPTH - 1 else 1, WAITS)


def return_kernel(n, n_vocab, sc_hbm, out_hbm, sc_ref, lsem, ssend, srecv):
    m, v = lax.axis_index("model"), lax.axis_index("vocab")
    me = m * n_vocab + v
    barrier = pltpu.get_barrier_semaphore()
    signal_peers(barrier, range(1, n), n_vocab, m, v)
    load = pltpu.make_async_copy(sc_hbm, sc_ref, lsem.at[0])
    load.start()
    load.wait()
    pl.semaphore_wait(barrier, n - 1)
    copies = []
    for k in range(1, n):
        pm, pv = peer(m, v, k, n_vocab)
        c = pltpu.make_async_remote_copy(
            src_ref=sc_ref.at[k], dst_ref=out_hbm.at[me], send_sem=ssend.at[k], recv_sem=srecv.at[k],
            device_id={"model": pm, "vocab": pv}, device_id_type=MESH)
        c.start()
        copies.append(c)
    own = pltpu.make_async_copy(sc_ref.at[0], out_hbm.at[me], lsem.at[1])
    own.start()
    for c in copies:
        c.wait_recv()
    for c in copies:
        c.wait_send()
    own.wait()


def softmax_kernel(sc_ref, meta_ref, p_ref, lp_ref, flip):
    n = sc_ref.shape[0]
    rows, length = p_ref.shape
    flip[...] = sc_ref[...].reshape(n * 8, 128).T
    wide = [jnp.concatenate([flip[pl.ds(q, rows, stride=4), :] for q in (2 * hb, 2 * hb + 1)], axis=1) for hb in (0, 1)]
    meta = meta_ref[...]
    code = meta[:, :length]
    ok = code >= 0
    full = jnp.concatenate([jnp.where(ok, code, 0), jnp.zeros((rows, 128 - length), jnp.int32)], axis=1)
    low = jnp.take_along_axis(wide[0], lax.rem(full, 128), axis=1)
    high = jnp.take_along_axis(wide[1], lax.rem(full, 128), axis=1)
    scores = jnp.where(full < 128, low, high)[:, :length] / TEMP
    scores = jnp.where(ok, scores, -jnp.inf)
    top = jnp.max(scores, axis=1, keepdims=True)
    log_norm = top + jnp.log(jnp.sum(jnp.exp(scores - top), axis=1, keepdims=True))
    p_ref[...] = jnp.where(ok, jnp.exp(scores - log_norm), 0.0)
    at = lax.broadcasted_iota(jnp.int32, (rows, length), 1)
    picked = jnp.sum(jnp.where(at == meta[:, length:], scores, 0.0), axis=1, keepdims=True)
    diag = (lax.broadcasted_iota(jnp.int32, (rows, rows), 0) == lax.broadcasted_iota(jnp.int32, (rows, rows), 1))
    lp_ref[...] = jnp.sum(jnp.where(diag, picked - log_norm, 0.0), axis=0)


def solution(mesh):
    axes = ("model", "vocab")
    n_model, n_vocab = mesh.shape["model"], mesh.shape["vocab"]
    n = n_model * n_vocab
    row_spec = P(("rep",) + axes, None)
    vec_spec = P(("rep",) + axes)
    vmem = pl.BlockSpec(memory_space=pltpu.VMEM)
    hbm = pl.BlockSpec(memory_space=pl.ANY)

    def local_step(hidden, head_rows, allowed_ids, valid_mask, target_pos):
        rows, length = allowed_ids.shape
        shard_len, width = head_rows.shape
        per = rows * CAP // 128
        tiles = width // 128

        chunks = n * rows * CAP // SLOTS
        tbl, meta, hall = pl.pallas_call(
            functools.partial(route_kernel, shard_len, n, n_vocab),
            out_shape=(jax.ShapeDtypeStruct((n, per, 128), jnp.int32),
                       jax.ShapeDtypeStruct((rows, 2 * length), jnp.int32),
                       jax.ShapeDtypeStruct((n, rows, width), jnp.bfloat16)),
            in_specs=[hbm] * 4,
            out_specs=(hbm, hbm, hbm),
            scratch_shapes=[
                pltpu.VMEM((rows, length), jnp.int32),
                pltpu.VMEM((rows, length), jnp.int32),
                pltpu.VMEM((rows,), jnp.int32),
                pltpu.VMEM((rows, 2 * length), jnp.int32),
                pltpu.VMEM((rows, n * CAP), jnp.int32),
                pltpu.VMEM((n, per, 128), jnp.int32),
                pltpu.VMEM((n, per, 128), jnp.int32),
                pltpu.VMEM((n, rows, width), jnp.bfloat16),
                pltpu.SemaphoreType.DMA((n,)),
                pltpu.SemaphoreType.DMA((n,)),
                pltpu.SemaphoreType.DMA((17,)),
                pltpu.SemaphoreType.DMA((17,)),
                pltpu.SemaphoreType.DMA((4,)),
                pltpu.SemaphoreType.DMA((12,)),
                pltpu.SemaphoreType.REGULAR((2,)),
            ],
            compiler_params=pltpu.CompilerParams(collective_id=0, has_side_effects=True),
            name="route",
        )(allowed_ids, valid_mask, target_pos, hidden)
        pairs = head_rows.reshape(shard_len // 8, 4, 2, tiles, 128).transpose(0, 3, 1, 2, 4)
        scores = pl.pallas_call(
            score_kernel,
            out_shape=jax.ShapeDtypeStruct((n, 8, 128), jnp.float32),
            in_specs=[hbm, hbm, hbm],
            out_specs=vmem,
            scratch_shapes=[
                *[pltpu.VMEM((SLOTS // 4, tiles, 8, 128), jnp.bfloat16)] * DEPTH,
                pltpu.SMEM((n, per, 128), jnp.int32),
                pltpu.VMEM((n, per, 128), jnp.int32),
                pltpu.VMEM((chunks, SLOTS // CAP, width), jnp.bfloat16),
                pltpu.VMEM((SLOTS // CAP, width), jnp.float32),
                pltpu.SemaphoreType.DMA((DEPTH, WAITS)),
                pltpu.SemaphoreType.DMA((4,)),
            ],
            compiler_params=pltpu.CompilerParams(vmem_limit_bytes=67_000_000),
            name="score",
        )(tbl, pairs, hall.reshape(chunks, SLOTS // CAP, width))
        back = pl.pallas_call(
            functools.partial(return_kernel, n, n_vocab),
            out_shape=jax.ShapeDtypeStruct((n, 8, 128), jnp.float32),
            in_specs=[hbm],
            out_specs=hbm,
            scratch_shapes=[
                pltpu.VMEM((n, 8, 128), jnp.float32),
                pltpu.SemaphoreType.DMA((2,)),
                pltpu.SemaphoreType.DMA((n,)),
                pltpu.SemaphoreType.DMA((n,)),
            ],
            compiler_params=pltpu.CompilerParams(collective_id=1, has_side_effects=True),
            name="giveback",
        )(scores)
        return pl.pallas_call(
            softmax_kernel,
            out_shape=(jax.ShapeDtypeStruct((rows, length), jnp.float32), jax.ShapeDtypeStruct((rows,), jnp.float32)),
            in_specs=[vmem, vmem],
            out_specs=(vmem, vmem),
            scratch_shapes=[pltpu.VMEM((128, n * 8), jnp.float32)],
            name="finish",
        )(back, meta)

    return jax.shard_map(local_step, mesh=mesh, in_specs=(row_spec, P(axes, None), row_spec, row_spec, vec_spec),
                         out_specs=(row_spec, vec_spec), check_vma=False)
```

```python
import functools

import jax
import jax.numpy as jnp
from jax import lax
from jax.experimental import pallas as pl
from jax.experimental.pallas import tpu as pltpu
from jax.sharding import PartitionSpec as P

MESH = pl.DeviceIdType.MESH
TEMP = 0.5
CAP = 16
SLOTS = 128
DEPTH = 4
WAITS = 4


def flip_bits(a, k):
    for bit in (1, 2):
        if k & bit:
            a = a + bit - 2 * bit * lax.rem(lax.div(a, bit), 2)
    return a


def peer(m, v, k, n_vocab):
    return flip_bits(m, k // n_vocab), flip_bits(v, k % n_vocab)


def signal_peers(sem, ks, n_vocab, m, v):
    for k in ks:
        pm, pv = peer(m, v, k, n_vocab)
        pl.semaphore_signal(sem, inc=1, device_id={"model": pm, "vocab": pv}, device_id_type=MESH)


NEAR = (1, 2, 4)


def route_kernel(shard_len, n, n_vocab, ids_hbm, valid_hbm, tgt_hbm, h_hbm, tbl_out, meta_out, hall_out,
                 ids_ref, valid_ref, tgt_ref, meta_ref, t_ref, send_ref, tin_ref, hbuf, tsend, trecv, hsend, hrecv, lsem, osem, round_sem):
    rows, length = ids_ref.shape
    m, v = lax.axis_index("model"), lax.axis_index("vocab")
    me = m * n_vocab + v
    barrier = pltpu.get_barrier_semaphore()
    signal_peers(barrier, NEAR, n_vocab, m, v)
    half = rows // 2
    lo, hi, every = pl.ds(0, half), pl.ds(half, half), pl.ds(0, rows)
    loads = [pltpu.make_async_copy(src, dst, lsem.at[i]) for i, (src, dst) in enumerate(
        ((h_hbm.at[lo], hbuf.at[0, lo]), (h_hbm.at[hi], hbuf.at[0, hi]), (ids_hbm, ids_ref), (valid_hbm, valid_ref),
         (tgt_hbm, tgt_ref)))]
    for c in loads:
        c.start()

    sends = []

    def send(src, dst, part, to):
        pm, pv = peer(m, v, to, n_vocab)
        i = len(sends)
        sends.append(pltpu.make_async_remote_copy(
            src_ref=hbuf.at[src, part], dst_ref=(hall_out if to == 1 else hbuf).at[dst, part], send_sem=hsend.at[i], recv_sem=hrecv.at[i],
            device_id={"model": pm, "vocab": pv}, device_id_type=MESH))
        return sends[-1]

    own_x = [send(0, 2, lo, 2), send(0, 2, hi, 2)]
    own_y = [send(0, 4, lo, 4), send(0, 4, hi, 4)]
    own_p = send(0, 1, every, 1)
    quarter = [pl.ds(i * half // 2, half // 2) for i in range(4)]
    x_to_y, y_to_x = [send(2, 6, q, 4) for q in quarter[:2]], [send(4, 6, q, 2) for q in quarter[2:]]
    x_p = [send(2, 3, lo, 1), send(2, 3, hi, 1)]
    y_p = [send(4, 5, lo, 1), send(4, 5, hi, 1)]
    d_p = [send(6, 7, q, 1) for q in quarter]

    pl.semaphore_wait(barrier, len(NEAR))
    loads[0].wait()
    own_x[0].start()
    loads[1].wait()
    for c in (own_y[1], own_p, own_x[1], own_y[0]):
        c.start()
    signal_peers(round_sem.at[0], NEAR, n_vocab, m, v)
    outs = []

    def keep(src, dst):
        outs.append(pltpu.make_async_copy(src, dst, osem.at[len(outs)]))
        outs[-1].start()

    keep(hbuf.at[0], hall_out.at[0])
    for c in loads[2:]:
        c.wait()

    ids = ids_ref[...]
    ok = valid_ref[...] > 0
    owner = jnp.where(ok, lax.div(ids, shard_len), n)
    off = lax.rem(ids, shard_len)
    tri = (lax.broadcasted_iota(jnp.int32, (length, length), 0)
           < lax.broadcasted_iota(jnp.int32, (length, length), 1)).astype(jnp.bfloat16)
    rank = jnp.zeros((rows, length), jnp.float32)
    for s in range(n):
        hit = owner == s
        count = jnp.dot(jnp.where(hit, 1.0, 0.0).astype(jnp.bfloat16), tri, preferred_element_type=jnp.float32)
        rank = rank + jnp.where(hit, count, 0.0)
    rank = rank.astype(jnp.int32)
    slot = jnp.where(ok, owner * CAP + rank, n * CAP)
    pair = off - lax.rem(off, 2)

    lane = lax.broadcasted_iota(jnp.int32, (rows, n * CAP), 1)
    row = lax.broadcasted_iota(jnp.int32, (rows, n * CAP), 0)
    spread = lax.rem(((me * rows + row) * CAP + lax.rem(lane, CAP)) * 4, shard_len)
    table = spread
    for j in range(length):
        table = jnp.where(lane == slot[:, j:j + 1], pair[:, j:j + 1], table)
    t_ref[...] = table

    groups = 128 // CAP
    per = rows // groups
    lane4 = lax.broadcasted_iota(jnp.int32, (per, 128), 1)
    parts = [jnp.zeros((per, 128), jnp.int32) for _ in range(n)]
    for q in range(groups):
        tq = t_ref[pl.ds(q, per, stride=groups), :]
        inside = lax.div(lane4, CAP) == q
        for s in range(n):
            moved = tq if q == s else pltpu.roll(tq, ((q - s) * CAP) % 128, axis=1)
            parts[s] = jnp.where(inside, moved, parts[s])
    for s in range(n):
        send_ref[s] = parts[s]

    code = lax.div(rank, 4) * (n * 8) + owner * 8 + lax.rem(rank, 4) * 2 + lax.rem(off, 2)
    diag = (lax.broadcasted_iota(jnp.int32, (rows, rows), 0) == lax.broadcasted_iota(jnp.int32, (rows, rows), 1))
    tcol = jnp.sum(jnp.where(diag, tgt_ref[...].reshape(1, rows), 0).astype(jnp.float32), axis=1, keepdims=True)
    meta_ref[:, :length] = jnp.where(ok, code, -1)
    meta_ref[:, length:] = jnp.broadcast_to(tcol.astype(jnp.int32), (rows, length))

    tin_ref[0] = send_ref[me]
    copies = []
    for k in range(1, n):
        pm, pv = peer(m, v, k, n_vocab)
        copies.append(pltpu.make_async_remote_copy(
            src_ref=send_ref.at[pm * n_vocab + pv], dst_ref=tin_ref.at[k], send_sem=tsend.at[k], recv_sem=trecv.at[k],
            device_id={"model": pm, "vocab": pv}, device_id_type=MESH))

    pl.semaphore_wait(round_sem.at[0], len(NEAR))
    signal_peers(round_sem.at[1], NEAR, n_vocab, m, v)
    own_x[0].wait_recv()
    pl.semaphore_wait(round_sem.at[1], len(NEAR))
    for c in copies:
        c.start()
    for c in x_to_y:
        c.start()
    x_p[0].start()
    own_y[1].wait_recv()
    for c in y_to_x:
        c.start()
    y_p[1].start()
    keep(meta_ref, meta_out)
    own_x[1].wait_recv()
    x_p[1].start()
    keep(hbuf.at[2], hall_out.at[2])
    own_y[0].wait_recv()
    y_p[0].start()
    keep(hbuf.at[4], hall_out.at[4])
    for c in copies:
        c.wait_recv()
    keep(tin_ref, tbl_out)
    for i in range(2):
        x_to_y[i].wait_recv()
        d_p[i].start()
        y_to_x[i].wait_recv()
        d_p[2 + i].start()
    keep(hbuf.at[6], hall_out.at[6])
    for c in [own_p] + x_p + y_p + d_p:
        c.wait_recv()
    for c in sends + copies:
        c.wait_send()
    for c in outs:
        c.wait()


def score_kernel(tbl_hbm, w_hbm, h_hbm, out_ref, *scratch):
    bufs = scratch[:DEPTH]
    tbl_ref, tbl_vmem, h_ref, hf_ref, sems, lsem = scratch[DEPTH:]
    tiles = w_hbm.shape[1]
    nrow = SLOTS // CAP
    quads = CAP // 4
    blocks, per, _ = tbl_ref.shape
    chunks = blocks * per

    tload, hload = pltpu.make_async_copy(tbl_hbm, tbl_vmem, lsem.at[0]), pltpu.make_async_copy(h_hbm, h_ref, lsem.at[1])
    first = pltpu.make_async_copy(tbl_hbm.at[0], tbl_ref.at[0], lsem.at[2])
    first.start()
    tload.start()
    hload.start()
    rest = pltpu.make_async_copy(tbl_vmem.at[pl.ds(1, blocks - 1)], tbl_ref.at[pl.ds(1, blocks - 1)], lsem.at[3])

    def issue(r, b, k, parts=1):
        at = tbl_ref[r // per, r % per, k] if isinstance(r, int) else tbl_ref[lax.div(r, per), lax.rem(r, per), k]
        t, p = lax.shift_right_logical(at, 3), lax.bitwise_and(lax.shift_right_logical(at, 1), 3)
        pltpu.make_async_copy(
            w_hbm.at[t, :, p], bufs[b].at[k // 4, :, pl.ds(2 * (k % 4), 2), :], sems.at[b, k * parts // SLOTS]).start()

    lane = lax.broadcasted_iota(jnp.int32, (8, 128), 1)

    def work(c, b, more, parts=1, ahead_parts=1):
        ahead = c + DEPTH - 1
        flat = bufs[b].reshape(SLOTS // 4 * tiles * 8, 128)
        blk, part = lax.div(c, per), lax.rem(c, per)
        hf_ref[...] = h_ref[c].astype(jnp.float32)
        got = jnp.zeros((8, 128), jnp.float32)
        base = part * (SLOTS // 4)
        for i in range(nrow):
            if i % (nrow // parts) == 0:
                w = i // (nrow // parts)
                piece = bufs[b].at[pl.ds(w * (SLOTS // 4 // parts), SLOTS // 4 // parts)]
                pltpu.make_async_copy(piece, piece, sems.at[b, w]).wait()
            acc = [[jnp.zeros((8, 128), jnp.float32)] * 2 for _ in range(quads)]
            for kk in range(0, tiles, 2):
                if more:
                    for k in range(-(-kk * CAP // tiles), -(-(kk + 2) * CAP // tiles)):
                        issue(ahead, (b + DEPTH - 1) % DEPTH, i * CAP + k, ahead_parts)
                hb = [jnp.broadcast_to(hf_ref[i:i + 1, (kk + z) * 128:(kk + z + 1) * 128], (8, 128)) for z in (0, 1)]
                for g in range(quads):
                    at = ((i * quads + g) * tiles + kk) * 8
                    x = flat[at:at + 16, :].astype(jnp.float32)
                    acc[g] = [acc[g][0] + x[:8] * hb[0], acc[g][1] + x[8:] * hb[1]]
            for g in range(quads):
                total = jnp.sum(acc[g][0] + acc[g][1], axis=1, keepdims=True)
                got = jnp.where(lane == base + (i * quads + g), total, got)
        fresh = (lane >= base) & (lane < base + SLOTS // 4)
        out_ref[blk] = jnp.where(fresh, got, out_ref[blk])

    first.wait()
    for c in range(DEPTH - 1):
        for k in range(SLOTS):
            issue(c, c, k)
    tload.wait()
    rest.start()
    rest.wait()
    hload.wait()

    def step(g, _):
        for b in range(DEPTH):
            work(g * DEPTH + b, b, True)
        return 0

    lax.fori_loop(0, chunks // DEPTH - 1, step, 0)
    for b in range(DEPTH):
        work(jnp.int32(chunks - DEPTH + b), b, b == 0, WAITS if b == DEPTH - 1 else 1, WAITS)


def return_kernel(n, n_vocab, sc_hbm, out_hbm, sc_ref, lsem, ssend, srecv):
    m, v = lax.axis_index("model"), lax.axis_index("vocab")
    me = m * n_vocab + v
    barrier = pltpu.get_barrier_semaphore()
    signal_peers(barrier, range(1, n), n_vocab, m, v)
    load = pltpu.make_async_copy(sc_hbm, sc_ref, lsem.at[0])
    load.start()
    load.wait()
    pl.semaphore_wait(barrier, n - 1)
    copies = []
    for k in reversed(range(1, n)):
        pm, pv = peer(m, v, k, n_vocab)
        c = pltpu.make_async_remote_copy(
            src_ref=sc_ref.at[k], dst_ref=out_hbm.at[me], send_sem=ssend.at[k], recv_sem=srecv.at[k],
            device_id={"model": pm, "vocab": pv}, device_id_type=MESH)
        c.start()
        copies.append(c)
    own = pltpu.make_async_copy(sc_ref.at[0], out_hbm.at[me], lsem.at[1])
    own.start()
    for c in copies:
        c.wait_recv()
    for c in copies:
        c.wait_send()
    own.wait()


def softmax_kernel(sc_ref, meta_ref, p_ref, lp_ref, flip):
    n = sc_ref.shape[0]
    rows, length = p_ref.shape
    flip[...] = sc_ref[...].reshape(n * 8, 128).T
    wide = [jnp.concatenate([flip[pl.ds(q, rows, stride=4), :] for q in (2 * hb, 2 * hb + 1)], axis=1) for hb in (0, 1)]
    meta = meta_ref[...]
    code = meta[:, :length]
    ok = code >= 0
    full = jnp.concatenate([jnp.where(ok, code, 0), jnp.zeros((rows, 128 - length), jnp.int32)], axis=1)
    low = jnp.take_along_axis(wide[0], lax.rem(full, 128), axis=1)
    high = jnp.take_along_axis(wide[1], lax.rem(full, 128), axis=1)
    scores = jnp.where(full < 128, low, high)[:, :length] / TEMP
    scores = jnp.where(ok, scores, -jnp.inf)
    top = jnp.max(scores, axis=1, keepdims=True)
    log_norm = top + jnp.log(jnp.sum(jnp.exp(scores - top), axis=1, keepdims=True))
    p_ref[...] = jnp.where(ok, jnp.exp(scores - log_norm), 0.0)
    at = lax.broadcasted_iota(jnp.int32, (rows, length), 1)
    picked = jnp.sum(jnp.where(at == meta[:, length:], scores, 0.0), axis=1, keepdims=True)
    diag = (lax.broadcasted_iota(jnp.int32, (rows, rows), 0) == lax.broadcasted_iota(jnp.int32, (rows, rows), 1))
    lp_ref[...] = jnp.sum(jnp.where(diag, picked - log_norm, 0.0), axis=0)


def solution(mesh):
    axes = ("model", "vocab")
    n_model, n_vocab = mesh.shape["model"], mesh.shape["vocab"]
    n = n_model * n_vocab
    row_spec = P(("rep",) + axes, None)
    vec_spec = P(("rep",) + axes)
    vmem = pl.BlockSpec(memory_space=pltpu.VMEM)
    hbm = pl.BlockSpec(memory_space=pl.ANY)

    def local_step(hidden, head_rows, allowed_ids, valid_mask, target_pos):
        rows, length = allowed_ids.shape
        shard_len, width = head_rows.shape
        per = rows * CAP // 128
        tiles = width // 128

        chunks = n * rows * CAP // SLOTS
        tbl, meta, hall = pl.pallas_call(
            functools.partial(route_kernel, shard_len, n, n_vocab),
            out_shape=(jax.ShapeDtypeStruct((n, per, 128), jnp.int32),
                       jax.ShapeDtypeStruct((rows, 2 * length), jnp.int32),
                       jax.ShapeDtypeStruct((n, rows, width), jnp.bfloat16)),
            in_specs=[hbm] * 4,
            out_specs=(hbm, hbm, hbm),
            scratch_shapes=[
                pltpu.VMEM((rows, length), jnp.int32),
                pltpu.VMEM((rows, length), jnp.int32),
                pltpu.VMEM((rows,), jnp.int32),
                pltpu.VMEM((rows, 2 * length), jnp.int32),
                pltpu.VMEM((rows, n * CAP), jnp.int32),
                pltpu.VMEM((n, per, 128), jnp.int32),
                pltpu.VMEM((n, per, 128), jnp.int32),
                pltpu.VMEM((n, rows, width), jnp.bfloat16),
                pltpu.SemaphoreType.DMA((n,)),
                pltpu.SemaphoreType.DMA((n,)),
                pltpu.SemaphoreType.DMA((17,)),
                pltpu.SemaphoreType.DMA((17,)),
                pltpu.SemaphoreType.DMA((5,)),
                pltpu.SemaphoreType.DMA((12,)),
                pltpu.SemaphoreType.REGULAR((2,)),
            ],
            compiler_params=pltpu.CompilerParams(collective_id=0, has_side_effects=True),
            name="route",
        )(allowed_ids, valid_mask, target_pos, hidden)
        pairs = head_rows.reshape(shard_len // 8, 4, 2, tiles, 128).transpose(0, 3, 1, 2, 4)
        scores = pl.pallas_call(
            score_kernel,
            out_shape=jax.ShapeDtypeStruct((n, 8, 128), jnp.float32),
            in_specs=[hbm, hbm, hbm],
            out_specs=vmem,
            scratch_shapes=[
                *[pltpu.VMEM((SLOTS // 4, tiles, 8, 128), jnp.bfloat16)] * DEPTH,
                pltpu.SMEM((n, per, 128), jnp.int32),
                pltpu.VMEM((n, per, 128), jnp.int32),
                pltpu.VMEM((chunks, SLOTS // CAP, width), jnp.bfloat16),
                pltpu.VMEM((SLOTS // CAP, width), jnp.float32),
                pltpu.SemaphoreType.DMA((DEPTH, WAITS)),
                pltpu.SemaphoreType.DMA((4,)),
            ],
            compiler_params=pltpu.CompilerParams(vmem_limit_bytes=67_000_000),
            name="score",
        )(tbl, pairs, hall.reshape(chunks, SLOTS // CAP, width))
        back = pl.pallas_call(
            functools.partial(return_kernel, n, n_vocab),
            out_shape=jax.ShapeDtypeStruct((n, 8, 128), jnp.float32),
            in_specs=[hbm],
            out_specs=hbm,
            scratch_shapes=[
                pltpu.VMEM((n, 8, 128), jnp.float32),
                pltpu.SemaphoreType.DMA((2,)),
                pltpu.SemaphoreType.DMA((n,)),
                pltpu.SemaphoreType.DMA((n,)),
            ],
            compiler_params=pltpu.CompilerParams(collective_id=1, has_side_effects=True),
            name="giveback",
        )(scores)
        return pl.pallas_call(
            softmax_kernel,
            out_shape=(jax.ShapeDtypeStruct((rows, length), jnp.float32), jax.ShapeDtypeStruct((rows,), jnp.float32)),
            in_specs=[vmem, vmem],
            out_specs=(vmem, vmem),
            scratch_shapes=[pltpu.VMEM((128, n * 8), jnp.float32)],
            name="finish",
        )(back, meta)

    return jax.shard_map(local_step, mesh=mesh, in_specs=(row_spec, P(axes, None), row_spec, row_spec, vec_spec),
                         out_specs=(row_spec, vec_spec), check_vma=False)
```
